128 devices in a mesh: col: 2 (over core), row: 64 (over z, y, x).
Axes of the slice: x: 4, y: 4, z: 4, core: 2. Of those that a mesh axis runs over, the one named last changes fastest.
Arguments:
- img_emb: bfloat16 [32768, 768], P(('row', 'col'))
- txt_emb: bfloat16 [32768, 768], P(('row', 'col'))
- log_scale: float32 [], replicated
Outputs:
- output 1: float32 [], replicated
- output 2: bfloat16 [32768, 768], P(('row', 'col'))
- output 3: bfloat16 [32768, 768], P(('row', 'col'))
- output 4: float32 [], replicated
All inputs are finite; a program needn't handle non-finite values.
Results may differ from the reference program's by a relative error of at most 0.001.
Values are sent between devices in bfloat16 or wider.
A program may use at most 1 GiB of HBM per device.

```python
import jax
import jax.numpy as jnp
from jax import lax

ROWS_DEV = 256
SHARDS = 128
EMBED_DIM = 768
BATCH = ROWS_DEV * SHARDS


def unit_rows(values):
    return values / jnp.sqrt(jnp.sum(values * values, axis=-1, keepdims=True))


def setup_inputs(seed: int = 0) -> dict:
    keys = jax.random.split(jax.random.key(seed), 5)
    shared_dir = unit_rows(jax.random.normal(keys[0], (EMBED_DIM,), jnp.float32))
    spread = (1.0 / EMBED_DIM) ** 0.5
    pair_part = jax.random.normal(keys[1], (BATCH, EMBED_DIM), jnp.float32) * spread
    noise_img = jax.random.normal(keys[2], (BATCH, EMBED_DIM), jnp.float32) * spread
    noise_txt = jax.random.normal(keys[3], (BATCH, EMBED_DIM), jnp.float32) * spread
    img_emb = unit_rows(0.7 * shared_dir + 0.5 * pair_part + 0.5 * noise_img)
    txt_emb = unit_rows(0.7 * shared_dir + 0.5 * pair_part + 0.5 * noise_txt)
    log_scale = jnp.log(jax.random.uniform(keys[4], (), jnp.float32, 10.0, 30.0))
    return {"img_emb": img_emb.astype(jnp.bfloat16), "txt_emb": txt_emb.astype(jnp.bfloat16), "log_scale": log_scale}


def reference(img_emb, txt_emb, log_scale):
    logit_scale = jnp.exp(log_scale)
    img_blocks = img_emb.reshape(SHARDS, ROWS_DEV, EMBED_DIM)
    txt_blocks = txt_emb.reshape(SHARDS, ROWS_DEV, EMBED_DIM)
    block_ids = jnp.arange(SHARDS)
    positions = jnp.arange(BATCH)
    inv_count = 1.0 / (2 * BATCH)

    def row_lse_of(img_block):
        logits = logit_scale * jnp.dot(img_block, txt_emb.T, preferred_element_type=jnp.float32)
        return jax.nn.logsumexp(logits, axis=1)

    def col_lse_of(txt_block):
        logits_t = logit_scale * jnp.dot(txt_block, img_emb.T, preferred_element_type=jnp.float32)
        return jax.nn.logsumexp(logits_t, axis=1)

    row_lse = lax.map(row_lse_of, img_blocks).reshape(BATCH)
    col_lse = lax.map(col_lse_of, txt_blocks).reshape(BATCH)
    pos_logits = logit_scale * jnp.sum(img_emb.astype(jnp.float32) * txt_emb.astype(jnp.float32), axis=1)
    total_loss = (jnp.sum(row_lse - pos_logits) + jnp.sum(col_lse - pos_logits)) * inv_count

    def img_grad_of(block_args):
        block_id, img_block, row_lse_blk = block_args
        logits = logit_scale * jnp.dot(img_block, txt_emb.T, preferred_element_type=jnp.float32)
        diag_mask = (block_id * ROWS_DEV + jnp.arange(ROWS_DEV))[:, None] == positions[None, :]
        grad_tile = (jnp.exp(logits - row_lse_blk[:, None]) + jnp.exp(logits - col_lse[None, :]) - jnp.where(diag_mask, 2.0, 0.0)) * inv_count
        d_block = logit_scale * jnp.dot(grad_tile.astype(jnp.bfloat16), txt_emb, preferred_element_type=jnp.float32)
        return d_block.astype(jnp.bfloat16), jnp.sum(grad_tile * logits)

    def txt_grad_of(block_args):
        block_id, txt_block, col_lse_blk = block_args
        logits_t = logit_scale * jnp.dot(txt_block, img_emb.T, preferred_element_type=jnp.float32)
        diag_mask = (block_id * ROWS_DEV + jnp.arange(ROWS_DEV))[:, None] == positions[None, :]
        grad_t = (jnp.exp(logits_t - row_lse[None, :]) + jnp.exp(logits_t - col_lse_blk[:, None]) - jnp.where(diag_mask, 2.0, 0.0)) * inv_count
        d_block = logit_scale * jnp.dot(grad_t.astype(jnp.bfloat16), img_emb, preferred_element_type=jnp.float32)
        return d_block.astype(jnp.bfloat16)

    d_img, dt_parts = lax.map(img_grad_of, (block_ids, img_blocks, row_lse.reshape(SHARDS, ROWS_DEV)))
    d_txt = lax.map(txt_grad_of, (block_ids, txt_blocks, col_lse.reshape(SHARDS, ROWS_DEV)))
    return total_loss, d_img.reshape(BATCH, EMBED_DIM), d_txt.reshape(BATCH, EMBED_DIM), jnp.sum(dt_parts)
```

```python
import functools

import jax
import jax.numpy as jnp
from jax import lax
from jax.experimental import pallas as pl
from jax.experimental.pallas import tpu as pltpu
from jax.sharding import PartitionSpec as P

MESH = pl.DeviceIdType.MESH
F32 = jnp.float32
BF16 = jnp.bfloat16
VMEM_LIMIT = 64_000_000


class Grid:
    def __init__(self):
        row = lax.axis_index("row")
        self.c = lax.axis_index("col")
        self.z = row // 16
        self.y = (row // 4) % 4
        self.x = row % 4

    def dev(self, z, y, x, c):
        return {"row": (z * 4 + y) * 4 + x, "col": c}

    def y_a(self):
        return self.y + 1 - 2 * (self.y % 2)

    def y_b(self):
        return 3 - self.y

    def img_peer(self, dy, dz):
        y = self.y_a() if dy else self.y
        return self.dev((self.z + dz) % 4, y, self.x, self.c)

    def txt_peer(self, dc, dy, dx):
        y = self.y_b() if dy else self.y
        c = 1 - self.c if dc else self.c
        return self.dev(self.z, y, (self.x + dx) % 4, c)


class Net:
    def __init__(self, send_sems, recv_sems):
        self.send_sems, self.recv_sems, self.copies = send_sems, recv_sems, []

    def send(self, src, dst, peer):
        i = len(self.copies)
        copy = pltpu.make_async_remote_copy(
            src_ref=src, dst_ref=dst, send_sem=self.send_sems.at[i], recv_sem=self.recv_sems.at[i],
            device_id=peer, device_id_type=MESH)
        copy.start()
        self.copies.append(copy)
        return copy

    def finish(self):
        for copy in self.copies:
            copy.wait_send()


def greet(peers):
    barrier = pltpu.get_barrier_semaphore()
    for peer in peers:
        pl.semaphore_signal(barrier, inc=1, device_id=peer, device_id_type=MESH)
    pl.semaphore_wait(barrier, len(peers))


def neighbours(g):
    return [g.img_peer(0, 1), g.img_peer(0, 3), g.img_peer(1, 0), g.txt_peer(0, 0, 1), g.txt_peer(0, 0, 3),
            g.txt_peer(0, 1, 0), g.txt_peer(1, 0, 0)]


N_GATHER = 9 + 9 + 10


def gather_kernel(n, img_ref, txt_ref, img_all, txt_all, local_sems, send_sems, recv_sems):
    g = Grid()
    own = [pltpu.make_async_copy(img_ref, img_all.at[pl.ds(0, n)], local_sems.at[0]),
           pltpu.make_async_copy(txt_ref, txt_all.at[pl.ds(0, n)], local_sems.at[1])]
    for copy in own:
        copy.start()
    greet(neighbours(g))
    net = Net(send_sems, recv_sems)
    h = n // 2

    def slot(ref, k, lo=0, size=n):
        return ref.at[pl.ds(k * n + lo, size)]

    def ring(ref, peer_plus, peer_minus, peer_y):
        return dict(ref=ref, plus=peer_plus, minus=peer_minus, y=peer_y)

    img = ring(img_all, g.img_peer(0, 1), g.img_peer(0, 3), g.img_peer(1, 0))
    txt = ring(txt_all, g.txt_peer(0, 0, 1), g.txt_peer(0, 0, 3), g.txt_peer(0, 1, 0))
    core = g.txt_peer(1, 0, 0)
    for r, src in ((img, img_ref), (txt, txt_ref)):
        r["y0"] = net.send(src, slot(r["ref"], 4), r["y"])
        r["p0"] = net.send(src, slot(r["ref"], 3), r["plus"])
        r["m0"] = net.send(src, slot(r["ref"], 1), r["minus"])
    cross = [net.send(txt_ref, slot(txt_all, 8), core)]
    for r in (img, txt):
        r["y0"].wait_recv()
        r["p1"] = net.send(slot(r["ref"], 4), slot(r["ref"], 7), r["plus"])
        r["m1"] = net.send(slot(r["ref"], 4), slot(r["ref"], 5), r["minus"])
    cross.append(net.send(slot(txt_all, 4), slot(txt_all, 12), core))
    for dy in (0, 1):
        for r in (img, txt):
            ref, b = r["ref"], 4 * dy
            r["p%d" % dy].wait_recv()
            r["fp%d" % dy] = net.send(slot(ref, b + 3, 0, h), slot(ref, b + 2, 0, h), r["plus"])
            r["m%d" % dy].wait_recv()
            r["fm%d" % dy] = net.send(slot(ref, b + 1, h, h), slot(ref, b + 2, h, h), r["minus"])
        cross.append(net.send(slot(txt_all, 4 * dy + 3), slot(txt_all, 8 + 4 * dy + 3), core))
        cross.append(net.send(slot(txt_all, 4 * dy + 1), slot(txt_all, 8 + 4 * dy + 1), core))
    for dy in (0, 1):
        for r in (txt, img):
            r["fp%d" % dy].wait_recv()
            if r is txt:
                cross.append(net.send(slot(txt_all, 4 * dy + 2, 0, h), slot(txt_all, 8 + 4 * dy + 2, 0, h), core))
            r["fm%d" % dy].wait_recv()
            if r is txt:
                cross.append(net.send(slot(txt_all, 4 * dy + 2, h, h), slot(txt_all, 8 + 4 * dy + 2, h, h), core))
    for copy in cross:
        copy.wait_recv()
    for copy in own:
        copy.wait()
    net.finish()


def gather(img, txt):
    n, d = img.shape
    return pl.pallas_call(
        functools.partial(gather_kernel, n),
        out_shape=[jax.ShapeDtypeStruct((8 * n, d), BF16), jax.ShapeDtypeStruct((16 * n, d), BF16)],
        in_specs=[pl.BlockSpec(memory_space=pltpu.VMEM)] * 2,
        out_specs=[pl.BlockSpec(memory_space=pl.ANY)] * 2,
        scratch_shapes=[pltpu.SemaphoreType.DMA((2,)), pltpu.SemaphoreType.DMA((N_GATHER,)),
                        pltpu.SemaphoreType.DMA((N_GATHER,))],
        compiler_params=pltpu.CompilerParams(collective_id=0, has_side_effects=True, vmem_limit_bytes=VMEM_LIMIT),
        name="gather_blocks")(img, txt)


BN = 512
CM = 256


def pass1_kernel(scale_ref, img_ref, txt_ref, e_ref, rs_ref, rl_ref, cs_ref, cl_ref):
    j = pl.program_id(0)
    scale = scale_ref[0]
    rows = img_ref.shape[0]

    @pl.when(j == 0)
    def _():
        rs_ref[...] = jnp.zeros_like(rs_ref)
        rl_ref[...] = jnp.zeros_like(rl_ref)

    cs_ref[...] = jnp.zeros_like(cs_ref)
    cl_ref[...] = jnp.zeros_like(cl_ref)

    def step(i, carry):
        at = pl.ds(pl.multiple_of(i * CM, CM), CM)
        dots = lax.dot_general(img_ref[at, :], txt_ref[...], (((1,), (1,)), ((), ())), preferred_element_type=F32)
        logits = scale * dots
        e = jnp.exp(logits)
        el = e * logits
        e_ref[at, :] = e
        rs, rl = rs_ref[at, :], rl_ref[at, :]
        for q in range(BN // 128):
            lanes = slice(q * 128, (q + 1) * 128)
            rs += e[:, lanes]
            rl += el[:, lanes]
        rs_ref[at, :] = rs
        rl_ref[at, :] = rl
        cs_ref[...] += jnp.sum(e.reshape(CM // 8, 8, BN), axis=0)
        cl_ref[...] += jnp.sum(el.reshape(CM // 8, 8, BN), axis=0)
        return carry

    lax.fori_loop(0, rows // CM, step, 0)


def pass1(scale, img_all, txt_all):
    m, d = img_all.shape
    n = txt_all.shape[0]
    whole = lambda j: (0, 0)
    return pl.pallas_call(
        pass1_kernel,
        grid=(n // BN,),
        out_shape=[jax.ShapeDtypeStruct((m, n), F32), jax.ShapeDtypeStruct((m, 128), F32),
                   jax.ShapeDtypeStruct((m, 128), F32), jax.ShapeDtypeStruct((8, n), F32),
                   jax.ShapeDtypeStruct((8, n), F32)],
        in_specs=[pl.BlockSpec(memory_space=pltpu.SMEM), pl.BlockSpec((m, d), whole),
                  pl.BlockSpec((BN, d), lambda j: (j, 0))],
        out_specs=[pl.BlockSpec((m, BN), lambda j: (0, j)), pl.BlockSpec((m, 128), whole),
                   pl.BlockSpec((m, 128), whole), pl.BlockSpec((8, BN), lambda j: (0, j)),
                   pl.BlockSpec((8, BN), lambda j: (0, j))],
        compiler_params=pltpu.CompilerParams(dimension_semantics=("arbitrary",), vmem_limit_bytes=VMEM_LIMIT),
        cost_estimate=pl.CostEstimate(flops=2 * m * n * d, bytes_accessed=4 * m * n, transcendentals=m * n),
        name="logits_pass")(scale, img_all, txt_all)


N_SUMS = 7 + 15


def sums_kernel(inv, rs_ref, rl_ref, cs_ref, cl_ref, pos_ref, a_ref, b_ref, part_ref, rbuf, cbuf, send_sems, recv_sems):
    g = Grid()
    img_offs = [(dy, dz) for dy in (0, 1) for dz in range(4) if (dy, dz) != (0, 0)]
    txt_offs = [(dc, dy, dx) for dc in (0, 1) for dy in (0, 1) for dx in range(4) if (dc, dy, dx) != (0, 0, 0)]
    greet([g.img_peer(*o) for o in img_offs] + [g.txt_peer(*o) for o in txt_offs])
    net = Net(send_sems, recv_sems)
    for dc, dy, dx in txt_offs:
        net.send(cs_ref, cbuf.at[dc * 8 + dy * 4 + (4 - dx) % 4], g.txt_peer(dc, dy, dx))
    for dy, dz in img_offs:
        net.send(rs_ref, rbuf.at[dy * 4 + (4 - dz) % 4], g.img_peer(dy, dz))
    for copy in net.copies:
        copy.wait_recv()
    a, b, rtot, ctot = [], [], [], []
    for dy, dz in [(0, 0)] + img_offs:
        k = 2 * (dy * 4 + dz)
        tot = rs_ref[k:k + 2, :]
        for oy, oz in img_offs:
            q = 2 * ((dy ^ oy) * 4 + (dz - oz) % 4)
            tot += rbuf[oy * 4 + oz, q:q + 2, :]
        rtot.append(tot)
        a.append(inv / tot)
        a_ref[k:k + 2, :] = a[-1]
    for dc, dy, dx in [(0, 0, 0)] + txt_offs:
        k = 2 * (dc * 8 + dy * 4 + dx)
        tot = cs_ref[k:k + 2, :]
        for oc, oy, ox in txt_offs:
            q = 2 * ((dc ^ oc) * 8 + (dy ^ oy) * 4 + (dx - ox) % 4)
            tot += cbuf[oc * 8 + oy * 4 + ox, q:q + 2, :]
        ctot.append(tot)
        b.append(inv / tot)
        b_ref[k:k + 2, :] = b[-1]
    pos = pos_ref[...]
    loss = jnp.log(rtot[0]) + jnp.log(ctot[0]) - 2.0 * pos
    dt = -2.0 * pos
    for k in range(8):
        dt += a[k] * (1.0 / inv) * rl_ref[2 * k:2 * k + 2, :]
    for k in range(16):
        dt += b[k] * (1.0 / inv) * cl_ref[2 * k:2 * k + 2, :]
    loss = jnp.sum(loss, axis=0, keepdims=True) * inv
    dt = jnp.sum(dt, axis=0, keepdims=True) * inv
    part_ref[...] = jnp.zeros_like(part_ref)
    part_ref[0:1, :] = loss
    part_ref[1:2, :] = dt
    net.finish()


def exchange_sums(inv, rs, rl, cs, cl, pos):
    vmem = pl.BlockSpec(memory_space=pltpu.VMEM)
    return pl.pallas_call(
        functools.partial(sums_kernel, inv),
        out_shape=[jax.ShapeDtypeStruct(rs.shape, F32), jax.ShapeDtypeStruct(cs.shape, F32),
                   jax.ShapeDtypeStruct((8, 128), F32)],
        in_specs=[vmem] * 5,
        out_specs=[vmem] * 3,
        scratch_shapes=[pltpu.VMEM((8,) + rs.shape, F32), pltpu.VMEM((16,) + cs.shape, F32),
                        pltpu.SemaphoreType.DMA((N_SUMS,)), pltpu.SemaphoreType.DMA((N_SUMS,))],
        compiler_params=pltpu.CompilerParams(collective_id=1, has_side_effects=True),
        name="exchange_sums")(rs, rl, cs, cl, pos)


CI = 512


def pass2_kernel(inv, n, img_ref, txt_ref, e_ref, a_ref, b_ref, dimg_ref, dtxt_ref, gb_ref, imgt_ref):
    j = pl.program_id(0)
    rows, d = img_ref.shape

    @pl.when(j == 0)
    def _():
        for i in range(rows // 256):
            imgt_ref[:, i * 256:(i + 1) * 256] = img_ref[i * 256:(i + 1) * 256, :].T

    b = b_ref[...]

    def grad_step(i, carry):
        at = pl.ds(pl.multiple_of(i * CM, CM), CM)
        a = a_ref[at, :]
        for q in range(BN // 128):
            lanes = slice(q * 128, (q + 1) * 128)
            gb_ref[at, lanes] = (e_ref[at, lanes] * (a + b[:, lanes])).astype(BF16)
        return carry

    lax.fori_loop(0, rows // CM, grad_step, 0)

    @pl.when(j == 0)
    def _():
        diag = lax.broadcasted_iota(jnp.int32, (n, n), 0) == lax.broadcasted_iota(jnp.int32, (n, n), 1)
        for q in range(n // 128):
            lanes = slice(q * 128, (q + 1) * 128)
            grad = e_ref[0:n, lanes] * (a_ref[0:n, :] + b[:, lanes])
            gb_ref[0:n, lanes] = (grad - jnp.where(diag[:, lanes], 2.0 * inv, 0.0)).astype(BF16)

    def txt_step(i, carry):
        at = pl.ds(pl.multiple_of(i * 256, 256), 256)
        part = jnp.dot(imgt_ref[at, :], gb_ref[...], preferred_element_type=F32)
        for q in range(BN // n):
            dtxt_ref[q, at, :] = part[:, q * n:(q + 1) * n]
        return carry

    lax.fori_loop(0, d // 256, txt_step, 0)

    def img_step(first, i, carry):
        at = pl.ds(pl.multiple_of(i * CI, CI), CI)
        part = jnp.dot(gb_ref[at, :], txt_ref[...], preferred_element_type=F32)
        dimg_ref[at, :] = part if first else dimg_ref[at, :] + part
        return carry

    @pl.when(j == 0)
    def _():
        lax.fori_loop(0, rows // CI, functools.partial(img_step, True), 0)

    @pl.when(j > 0)
    def _():
        lax.fori_loop(0, rows // CI, functools.partial(img_step, False), 0)


def pass2(inv, n, img_all, txt_all, e, a, b):
    m, d = img_all.shape
    nt = txt_all.shape[0]
    whole = lambda j: (0, 0)
    return pl.pallas_call(
        functools.partial(pass2_kernel, inv, n),
        grid=(nt // BN,),
        out_shape=[jax.ShapeDtypeStruct((m, d), F32), jax.ShapeDtypeStruct((nt // n, d, n), F32)],
        in_specs=[pl.BlockSpec((m, d), whole), pl.BlockSpec((BN, d), lambda j: (j, 0)),
                  pl.BlockSpec((m, BN), lambda j: (0, j)), pl.BlockSpec((m, 128), whole),
                  pl.BlockSpec((1, BN), lambda j: (0, j))],
        out_specs=[pl.BlockSpec((m, d), whole), pl.BlockSpec((BN // n, d, n), lambda j: (j, 0, 0))],
        scratch_shapes=[pltpu.VMEM((m, BN), BF16), pltpu.VMEM((d, m), BF16)],
        compiler_params=pltpu.CompilerParams(dimension_semantics=("arbitrary",), vmem_limit_bytes=VMEM_LIMIT),
        cost_estimate=pl.CostEstimate(flops=4 * m * nt * d, bytes_accessed=4 * m * nt, transcendentals=0),
        name="grad_pass")(img_all, txt_all, e, a, b)


N_REDUCE = 8 + 2 * (4 + 18 + 1) + 22


class Ring:
    def __init__(self, net, acc, buf, ybuf, rows, cut, plus, minus, pair):
        self.net, self.acc, self.buf, self.ybuf = net, acc, buf, ybuf
        self.cut, self.rows = cut, rows
        self.plus, self.minus, self.pair = plus, minus, pair
        self.streams = {}

    def pair_first(self):
        lo, size = self.cut, self.rows - self.cut
        self.early = {d: self.net.send(self.acc.at[4 + d, pl.ds(lo, size)], self.ybuf.at[d, pl.ds(lo, size)], self.pair)
                      for d in (2, 1, 3, 0)}

    def pair_add(self):
        lo, size = self.cut, self.rows - self.cut
        for d in (2, 1, 3, 0):
            self.early[d].wait_recv()
            self.acc[d, lo:lo + size] += self.ybuf[d, lo:lo + size]

    def start(self, name, dy, lo, size):
        h, b = size // 2, 4 * dy
        acc, buf, send = self.acc, self.buf, self.net.send
        s = dict(lo=lo, h=h, b=b)
        h0, h1 = pl.ds(lo, h), pl.ds(lo + h, h)
        s["a_plus"] = send(acc.at[b + 2, h0], buf.at[b + 2, h0], self.plus)
        s["a_minus"] = send(acc.at[b + 2, h1], buf.at[b + 2, h1], self.minus)
        s["b_plus_h1"] = send(acc.at[b + 1, h1], buf.at[b + 3, h1], self.plus)
        s["b_minus_h0"] = send(acc.at[b + 3, h0], buf.at[b + 1, h0], self.minus)
        self.streams[name] = s

    def middle(self, name):
        s = self.streams[name]
        acc, buf, send = self.acc, self.buf, self.net.send
        lo, h, b = s["lo"], s["h"], s["b"]
        h0, h1 = pl.ds(lo, h), pl.ds(lo + h, h)
        s["a_plus"].wait_recv()
        acc[b + 1, lo:lo + h] += buf[b + 2, lo:lo + h]
        s["b_plus_h0"] = send(acc.at[b + 1, h0], buf.at[b + 3, h0], self.plus)
        s["a_minus"].wait_recv()
        acc[b + 3, lo + h:lo + 2 * h] += buf[b + 2, lo + h:lo + 2 * h]
        s["b_minus_h1"] = send(acc.at[b + 3, h1], buf.at[b + 1, h1], self.minus)

    def end(self, name):
        s = self.streams[name]
        lo, h, b = s["lo"], s["h"], s["b"]
        for key in ("b_plus_h1", "b_minus_h0", "b_plus_h0", "b_minus_h1"):
            s[key].wait_recv()
        self.acc[b, lo:lo + 2 * h] += self.buf[b + 1, lo:lo + 2 * h] + self.buf[b + 3, lo:lo + 2 * h]

    def pair_last(self):
        at = pl.ds(0, self.cut)
        self.late = self.net.send(self.acc.at[4, at], self.buf.at[0, at], self.pair)

    def pair_end(self):
        self.late.wait_recv()
        self.acc[0, 0:self.cut] += self.buf[0, 0:self.cut]


def reduce_kernel(dimg_ref, dtxt_ref, part_ref, img_out, txt_out, part_out, iacc, tacc, ibuf, tbuf, iy, ty, dbuf, pa, pb,
                  psum, local_sems, send_sems, recv_sems):
    g = Grid()
    img_offs = [(dy, dz) for dy in (0, 1) for dz in range(4) if (dy, dz) != (0, 0)]
    txt_offs = [(dc, dy, dx) for dc in (0, 1) for dy in (0, 1) for dx in range(4) if (dc, dy, dx) != (0, 0, 0)]
    loads = {}
    for k in (6, 2, 5, 1, 7, 3, 4, 0):
        loads["t", k] = pltpu.make_async_copy(dtxt_ref.at[k], tacc.at[k], local_sems.at[k])
        loads["i", k] = pltpu.make_async_copy(dimg_ref.at[k], iacc.at[k], local_sems.at[8 + k])
        loads["t", k].start()
        loads["i", k].start()
    greet([g.img_peer(*o) for o in img_offs] + [g.txt_peer(*o) for o in txt_offs])
    net = Net(send_sems, recv_sems)
    core = g.txt_peer(1, 0, 0)
    cross = {k: net.send(dtxt_ref.at[8 + k], dbuf.at[k], core) for k in (6, 5, 7, 4, 2, 1, 3, 0)}
    ia = g.z * 2 + g.y % 2
    ib = (g.x * 2 + g.y // 2) * 2 + g.c
    scal_a = [net.send(part_ref, pa.at[ia], g.img_peer(*o)) for o in img_offs]
    pa[ia] = part_ref[...]

    img = Ring(net, iacc, ibuf, iy, iacc.shape[1], ICUT, g.img_peer(0, 1), g.img_peer(0, 3), g.img_peer(1, 0))
    txt = Ring(net, tacc, tbuf, ty, tacc.shape[1], TCUT, g.txt_peer(0, 0, 1), g.txt_peer(0, 0, 3), g.txt_peer(0, 1, 0))
    for k in (6, 5, 7, 4):
        loads["i", k].wait()
    img.pair_first()
    img.start("1", 1, 0, img.cut)
    for k in (2, 1, 3, 0):
        loads["i", k].wait()
    img.start("0", 0, 0, img.cut)
    for k in (6, 5, 7, 4):
        loads["t", k].wait()
        cross[k].wait_recv()
        tacc[k] += dbuf[k]
    txt.pair_first()
    txt.start("1", 1, 0, txt.cut)
    for k in (2, 1, 3, 0):
        loads["t", k].wait()
        cross[k].wait_recv()
        tacc[k] += dbuf[k]
    txt.start("0", 0, 0, txt.cut)
    for copy in scal_a:
        copy.wait_recv()
    total = pa[0]
    for k in range(1, 8):
        total += pa[k]
    psum[...] = total
    scal_b = [net.send(psum, pb.at[ib], g.txt_peer(*o)) for o in txt_offs]
    pb[ib] = total
    for r in (img, txt):
        r.middle("1")
    for r in (img, txt):
        r.end("1")
        r.pair_last()
        r.middle("0")
    for r in (img, txt):
        r.pair_add()
        r.start("2", 0, r.cut, r.rows - r.cut)
    for copy in scal_b:
        copy.wait_recv()
    total = pb[0]
    for k in range(1, 16):
        total += pb[k]
    part_out[...] = total
    for r in (img, txt):
        r.end("0")
    for r in (img, txt):
        r.middle("2")
    for r in (img, txt):
        r.pair_end()
    for r in (img, txt):
        r.end("2")
    img_out[...] = iacc[0]
    txt_out[...] = tacc[0]
    net.finish()


ICUT = 144
TCUT = 432


def reduce_scatter(dimg, dtxt, part):
    _, n, d = dimg.shape
    vmem = pl.BlockSpec(memory_space=pltpu.VMEM)
    hbm = pl.BlockSpec(memory_space=pl.ANY)
    return pl.pallas_call(
        reduce_kernel,
        out_shape=[jax.ShapeDtypeStruct((n, d), F32), jax.ShapeDtypeStruct((d, n), F32),
                   jax.ShapeDtypeStruct((8, 128), F32)],
        in_specs=[hbm, hbm, vmem],
        out_specs=[vmem] * 3,
        scratch_shapes=[pltpu.VMEM((8, n, d), F32), pltpu.VMEM((8, d, n), F32), pltpu.VMEM((8, n, d), F32),
                        pltpu.VMEM((8, d, n), F32), pltpu.VMEM((4, n, d), F32), pltpu.VMEM((4, d, n), F32),
                        pltpu.VMEM((8, d, n), F32), pltpu.VMEM((8, 8, 128), F32), pltpu.VMEM((16, 8, 128), F32),
                        pltpu.VMEM((8, 128), F32), pltpu.SemaphoreType.DMA((16,)),
                        pltpu.SemaphoreType.DMA((N_REDUCE,)), pltpu.SemaphoreType.DMA((N_REDUCE,))],
        compiler_params=pltpu.CompilerParams(collective_id=2, has_side_effects=True, vmem_limit_bytes=VMEM_LIMIT),
        name="reduce_blocks")(dimg, dtxt, part)


def solution(mesh):
    batch_spec = P(("row", "col"), None)
    shards = mesh.shape["row"] * mesh.shape["col"]

    def local_tile(img_loc, txt_loc, log_scale):
        n, d = img_loc.shape
        inv = 1.0 / (2 * n * shards)
        scale = jnp.exp(log_scale)
        pos = scale * jnp.sum(img_loc.astype(F32) * txt_loc.astype(F32), axis=1)
        img_all, txt_all = gather(img_loc, txt_loc)
        e, rs, rl, cs, cl = pass1(scale.reshape(1), img_all, txt_all)
        rows = lambda v: jnp.sum(v, axis=1).reshape(-1, 128)
        cols = lambda v: jnp.sum(v, axis=0).reshape(-1, 128)
        a, b, part = exchange_sums(inv, rows(rs), rows(rl), cols(cs), cols(cl), pos.reshape(-1, 128))
        a_rows = jnp.broadcast_to(a.reshape(-1, 1), (8 * n, 128))
        dimg, dtxt = pass2(inv, n, img_all, txt_all, e, a_rows, b.reshape(1, -1))
        img_sum, txt_sum, tot = reduce_scatter(dimg.reshape(8, n, d), dtxt, part)
        d_img = (scale * img_sum).astype(BF16)
        d_txt = (scale * txt_sum).T.astype(BF16)
        tot = jnp.sum(tot[0:2], axis=1)
        return tot[0], d_img, d_txt, tot[1]

    return jax.shard_map(local_tile, mesh=mesh, in_specs=(batch_spec, batch_spec, P()),
                         out_specs=(P(), batch_spec, batch_spec, P()), check_vma=False)
```

```python
import functools

import jax
import jax.numpy as jnp
from jax import lax
from jax.experimental import pallas as pl
from jax.experimental.pallas import tpu as pltpu
from jax.sharding import PartitionSpec as P

MESH = pl.DeviceIdType.MESH
F32 = jnp.float32
BF16 = jnp.bfloat16
VMEM_LIMIT = 64_000_000


class Grid:
    def __init__(self):
        row = lax.axis_index("row")
        self.c = lax.axis_index("col")
        self.z = row // 16
        self.y = (row // 4) % 4
        self.x = row % 4

    def dev(self, z, y, x, c):
        return {"row": (z * 4 + y) * 4 + x, "col": c}

    def y_a(self):
        return self.y + 1 - 2 * (self.y % 2)

    def y_b(self):
        return 3 - self.y

    def img_peer(self, dy, dz):
        y = self.y_a() if dy else self.y
        return self.dev((self.z + dz) % 4, y, self.x, self.c)

    def txt_peer(self, dc, dy, dx):
        y = self.y_b() if dy else self.y
        c = 1 - self.c if dc else self.c
        return self.dev(self.z, y, (self.x + dx) % 4, c)


class Net:
    def __init__(self, send_sems, recv_sems):
        self.send_sems, self.recv_sems, self.copies = send_sems, recv_sems, []

    def send(self, src, dst, peer):
        i = len(self.copies)
        copy = pltpu.make_async_remote_copy(
            src_ref=src, dst_ref=dst, send_sem=self.send_sems.at[i], recv_sem=self.recv_sems.at[i],
            device_id=peer, device_id_type=MESH)
        copy.start()
        self.copies.append(copy)
        return copy

    def finish(self, skip=()):
        for copy in self.copies:
            if not any(copy is other for other in skip):
                copy.wait_send()


def greet(peers):
    barrier = pltpu.get_barrier_semaphore()
    for peer in peers:
        pl.semaphore_signal(barrier, inc=1, device_id=peer, device_id_type=MESH)
    pl.semaphore_wait(barrier, len(peers))


def neighbours(g):
    return [g.img_peer(0, 1), g.img_peer(0, 3), g.img_peer(1, 0), g.txt_peer(0, 0, 1), g.txt_peer(0, 0, 3),
            g.txt_peer(0, 1, 0), g.txt_peer(1, 0, 0)]


N_GATHER = 9 + 9 + 10


def gather_kernel(n, img_ref, txt_ref, img_all, txt_all, local_sems, send_sems, recv_sems):
    g = Grid()
    own = [pltpu.make_async_copy(img_ref, img_all.at[pl.ds(0, n)], local_sems.at[0]),
           pltpu.make_async_copy(txt_ref, txt_all.at[pl.ds(0, n)], local_sems.at[1])]
    for copy in own:
        copy.start()
    greet(neighbours(g))
    net = Net(send_sems, recv_sems)
    h = n // 2

    def slot(ref, k, lo=0, size=n):
        return ref.at[pl.ds(k * n + lo, size)]

    def ring(ref, peer_plus, peer_minus, peer_y):
        return dict(ref=ref, plus=peer_plus, minus=peer_minus, y=peer_y)

    img = ring(img_all, g.img_peer(0, 1), g.img_peer(0, 3), g.img_peer(1, 0))
    txt = ring(txt_all, g.txt_peer(0, 0, 1), g.txt_peer(0, 0, 3), g.txt_peer(0, 1, 0))
    core = g.txt_peer(1, 0, 0)
    for r, src in ((img, img_ref), (txt, txt_ref)):
        r["y0"] = net.send(src, slot(r["ref"], 4), r["y"])
        r["p0"] = net.send(src, slot(r["ref"], 3), r["plus"])
        r["m0"] = net.send(src, slot(r["ref"], 1), r["minus"])
    cross = [net.send(txt_ref, slot(txt_all, 8), core)]
    for r in (img, txt):
        r["y0"].wait_recv()
        r["p1"] = net.send(slot(r["ref"], 4), slot(r["ref"], 7), r["plus"])
        r["m1"] = net.send(slot(r["ref"], 4), slot(r["ref"], 5), r["minus"])
    cross.append(net.send(slot(txt_all, 4), slot(txt_all, 12), core))
    for dy in (0, 1):
        for r in (img, txt):
            ref, b = r["ref"], 4 * dy
            r["p%d" % dy].wait_recv()
            r["fp%d" % dy] = net.send(slot(ref, b + 3, 0, h), slot(ref, b + 2, 0, h), r["plus"])
            r["m%d" % dy].wait_recv()
            r["fm%d" % dy] = net.send(slot(ref, b + 1, h, h), slot(ref, b + 2, h, h), r["minus"])
        cross.append(net.send(slot(txt_all, 4 * dy + 3), slot(txt_all, 8 + 4 * dy + 3), core))
        cross.append(net.send(slot(txt_all, 4 * dy + 1), slot(txt_all, 8 + 4 * dy + 1), core))
    for dy in (0, 1):
        for r in (txt, img):
            r["fp%d" % dy].wait_recv()
            if r is txt:
                cross.append(net.send(slot(txt_all, 4 * dy + 2, 0, h), slot(txt_all, 8 + 4 * dy + 2, 0, h), core))
            r["fm%d" % dy].wait_recv()
            if r is txt:
                cross.append(net.send(slot(txt_all, 4 * dy + 2, h, h), slot(txt_all, 8 + 4 * dy + 2, h, h), core))
    for copy in cross:
        copy.wait_recv()
    for copy in own:
        copy.wait()
    net.finish()


def gather(img, txt):
    n, d = img.shape
    return pl.pallas_call(
        functools.partial(gather_kernel, n),
        out_shape=[jax.ShapeDtypeStruct((8 * n, d), BF16), jax.ShapeDtypeStruct((16 * n, d), BF16)],
        in_specs=[pl.BlockSpec(memory_space=pltpu.VMEM)] * 2,
        out_specs=[pl.BlockSpec(memory_space=pl.ANY)] * 2,
        scratch_shapes=[pltpu.SemaphoreType.DMA((2,)), pltpu.SemaphoreType.DMA((N_GATHER,)),
                        pltpu.SemaphoreType.DMA((N_GATHER,))],
        compiler_params=pltpu.CompilerParams(collective_id=0, has_side_effects=True, vmem_limit_bytes=VMEM_LIMIT),
        name="gather_blocks")(img, txt)


BN = 512
CM = 256


def pass1_kernel(scale_ref, img_ref, txt_ref, e_ref, rs_ref, rl_ref, cs_ref, cl_ref, imgt_ref):
    j = pl.program_id(0)
    scale = scale_ref[0]
    rows = img_ref.shape[0]

    @pl.when(j == 0)
    def _():
        rs_ref[...] = jnp.zeros_like(rs_ref)
        rl_ref[...] = jnp.zeros_like(rl_ref)
        for i in range(rows // 256):
            imgt_ref[:, i * 256:(i + 1) * 256] = img_ref[i * 256:(i + 1) * 256, :].T

    cs_ref[...] = jnp.zeros_like(cs_ref)
    cl_ref[...] = jnp.zeros_like(cl_ref)

    def step(i, carry):
        at = pl.ds(pl.multiple_of(i * CM, CM), CM)
        dots = lax.dot_general(img_ref[at, :], txt_ref[...], (((1,), (1,)), ((), ())), preferred_element_type=F32)
        logits = scale * dots
        e = jnp.exp(logits)
        el = e * logits
        e_ref[at, :] = e
        rs, rl = rs_ref[at, :], rl_ref[at, :]
        for q in range(BN // 128):
            lanes = slice(q * 128, (q + 1) * 128)
            rs += e[:, lanes]
            rl += el[:, lanes]
        rs_ref[at, :] = rs
        rl_ref[at, :] = rl
        cs_ref[...] += jnp.sum(e.reshape(CM // 8, 8, BN), axis=0)
        cl_ref[...] += jnp.sum(el.reshape(CM // 8, 8, BN), axis=0)
        return carry

    lax.fori_loop(0, rows // CM, step, 0)


def pass1(scale, img_all, txt_all):
    m, d = img_all.shape
    n = txt_all.shape[0]
    whole = lambda j: (0, 0)
    return pl.pallas_call(
        pass1_kernel,
        grid=(n // BN,),
        out_shape=[jax.ShapeDtypeStruct((m, n), F32), jax.ShapeDtypeStruct((m, 128), F32),
                   jax.ShapeDtypeStruct((m, 128), F32), jax.ShapeDtypeStruct((8, n), F32),
                   jax.ShapeDtypeStruct((8, n), F32), jax.ShapeDtypeStruct((d, m), BF16)],
        in_specs=[pl.BlockSpec(memory_space=pltpu.SMEM), pl.BlockSpec((m, d), whole),
                  pl.BlockSpec((BN, d), lambda j: (j, 0))],
        out_specs=[pl.BlockSpec((m, BN), lambda j: (0, j)), pl.BlockSpec((m, 128), whole),
                   pl.BlockSpec((m, 128), whole), pl.BlockSpec((8, BN), lambda j: (0, j)),
                   pl.BlockSpec((8, BN), lambda j: (0, j)), pl.BlockSpec((d, m), whole)],
        compiler_params=pltpu.CompilerParams(dimension_semantics=("arbitrary",), vmem_limit_bytes=VMEM_LIMIT),
        cost_estimate=pl.CostEstimate(flops=2 * m * n * d, bytes_accessed=4 * m * n, transcendentals=m * n),
        name="logits_pass")(scale, img_all, txt_all)


N_SUMS = 7 + 15


def sums_kernel(inv, rs_ref, rl_ref, cs_ref, cl_ref, pos_ref, a_ref, b_ref, part_ref, rbuf, cbuf, send_sems, recv_sems):
    g = Grid()
    img_offs = [(dy, dz) for dy in (0, 1) for dz in range(4) if (dy, dz) != (0, 0)]
    txt_offs = [(dc, dy, dx) for dc in (0, 1) for dy in (0, 1) for dx in range(4) if (dc, dy, dx) != (0, 0, 0)]
    greet([g.img_peer(*o) for o in img_offs] + [g.txt_peer(*o) for o in txt_offs])
    net = Net(send_sems, recv_sems)
    for dc, dy, dx in txt_offs:
        net.send(cs_ref, cbuf.at[dc * 8 + dy * 4 + (4 - dx) % 4], g.txt_peer(dc, dy, dx))
    for dy, dz in img_offs:
        net.send(rs_ref, rbuf.at[dy * 4 + (4 - dz) % 4], g.img_peer(dy, dz))
    for copy in net.copies:
        copy.wait_recv()
    a, b, rtot, ctot = [], [], [], []
    for dy, dz in [(0, 0)] + img_offs:
        k = 2 * (dy * 4 + dz)
        tot = rs_ref[k:k + 2, :]
        for oy, oz in img_offs:
            q = 2 * ((dy ^ oy) * 4 + (dz - oz) % 4)
            tot += rbuf[oy * 4 + oz, q:q + 2, :]
        rtot.append(tot)
        a.append(inv / tot)
        a_ref[k:k + 2, :] = a[-1]
    for dc, dy, dx in [(0, 0, 0)] + txt_offs:
        k = 2 * (dc * 8 + dy * 4 + dx)
        tot = cs_ref[k:k + 2, :]
        for oc, oy, ox in txt_offs:
            q = 2 * ((dc ^ oc) * 8 + (dy ^ oy) * 4 + (dx - ox) % 4)
            tot += cbuf[oc * 8 + oy * 4 + ox, q:q + 2, :]
        ctot.append(tot)
        b.append(inv / tot)
        b_ref[k:k + 2, :] = b[-1]
    pos = pos_ref[...]
    loss = jnp.log(rtot[0]) + jnp.log(ctot[0]) - 2.0 * pos
    dt = -2.0 * pos
    for k in range(8):
        dt += a[k] * (1.0 / inv) * rl_ref[2 * k:2 * k + 2, :]
    for k in range(16):
        dt += b[k] * (1.0 / inv) * cl_ref[2 * k:2 * k + 2, :]
    loss = jnp.sum(loss, axis=0, keepdims=True) * inv
    dt = jnp.sum(dt, axis=0, keepdims=True) * inv
    part_ref[...] = jnp.zeros_like(part_ref)
    part_ref[0:1, :] = loss
    part_ref[1:2, :] = dt
    net.finish()


def exchange_sums(inv, rs, rl, cs, cl, pos):
    vmem = pl.BlockSpec(memory_space=pltpu.VMEM)
    return pl.pallas_call(
        functools.partial(sums_kernel, inv),
        out_shape=[jax.ShapeDtypeStruct(rs.shape, F32), jax.ShapeDtypeStruct(cs.shape, F32),
                   jax.ShapeDtypeStruct((8, 128), F32)],
        in_specs=[vmem] * 5,
        out_specs=[vmem] * 3,
        scratch_shapes=[pltpu.VMEM((8,) + rs.shape, F32), pltpu.VMEM((16,) + cs.shape, F32),
                        pltpu.SemaphoreType.DMA((N_SUMS,)), pltpu.SemaphoreType.DMA((N_SUMS,))],
        compiler_params=pltpu.CompilerParams(collective_id=1, has_side_effects=True),
        name="exchange_sums")(rs, rl, cs, cl, pos)


ICUT = 144
TCUT = 432
ORDER = (6, 5, 7, 2, 1, 4, 3, 0)
KC = 512
N_REDUCE = 8 + 2 * (4 + 18 + 1) + 22


class Ring:
    def __init__(self, net, acc, buf, cut, plus, minus, pair):
        self.net, self.acc, self.buf = net, acc, buf
        self.cut, self.rows = cut, acc.shape[1]
        self.plus, self.minus, self.pair = plus, minus, pair
        self.early, self.streams = {}, {}

    def pair_send(self, d):
        at = pl.ds(self.cut, self.rows - self.cut)
        self.early[d] = self.net.send(self.acc.at[4 + d, at], self.buf.at[4 + d, at], self.pair)

    def pair_add(self, d):
        self.early[d].wait_recv()
        self.acc[d, self.cut:] += self.buf[4 + d, self.cut:]

    def where(self, name):
        if name == 2:
            return 0, self.cut, (self.rows - self.cut) // 2
        return 4 * name, 0, self.cut // 2

    def send(self, name, key, slot, half, to_slot, peer):
        _, lo, h = self.where(name)
        at = pl.ds(lo + half * h, h)
        self.streams[name, key] = self.net.send(self.acc.at[slot, at], self.buf.at[to_slot, at], peer)

    def far(self, name):
        b, _, _ = self.where(name)
        self.send(name, "a+", b + 2, 0, b + 2, self.plus)
        self.send(name, "a-", b + 2, 1, b + 2, self.minus)

    def plain_plus(self, name):
        b, _, _ = self.where(name)
        self.send(name, "b+1", b + 1, 1, b + 3, self.plus)

    def plain_minus(self, name):
        b, _, _ = self.where(name)
        self.send(name, "b-0", b + 3, 0, b + 1, self.minus)

    def mid(self, name):
        b, lo, h = self.where(name)
        self.streams[name, "a+"].wait_recv()
        self.acc[b + 1, lo:lo + h] += self.buf[b + 2, lo:lo + h]
        self.send(name, "b+0", b + 1, 0, b + 3, self.plus)
        self.streams[name, "a-"].wait_recv()
        self.acc[b + 3, lo + h:lo + 2 * h] += self.buf[b + 2, lo + h:lo + 2 * h]
        self.send(name, "b-1", b + 3, 1, b + 1, self.minus)

    def end(self, name):
        b, lo, h = self.where(name)
        for key in ("b+1", "b-0", "b+0", "b-1"):
            self.streams[name, key].wait_recv()
        self.acc[b, lo:lo + 2 * h] += self.buf[b + 1, lo:lo + 2 * h] + self.buf[b + 3, lo:lo + 2 * h]

    def pair_last(self):
        at = pl.ds(0, self.cut)
        self.late = self.net.send(self.acc.at[4, at], self.buf.at[0, at], self.pair)

    def pair_end(self):
        self.late.wait_recv()
        self.acc[0, 0:self.cut] += self.buf[0, 0:self.cut]

    def ready(self, step):
        if step == 0:
            self.pair_send(2)
            self.far(1)
        elif step == 1:
            self.pair_send(1)
            self.plain_plus(1)
        elif step == 2:
            self.pair_send(3)
            self.plain_minus(1)
            self.mid(1)
        elif step == 3:
            self.far(0)
            self.pair_add(2)
            self.far(2)
        elif step == 4:
            self.plain_plus(0)
            self.pair_add(1)
            self.plain_plus(2)
        elif step == 5:
            self.pair_send(0)
            self.end(1)
            self.pair_last()
        elif step == 6:
            self.plain_minus(0)
            self.pair_add(3)
            self.plain_minus(2)
            self.mid(0)

    def close(self):
        self.pair_add(0)
        self.end(0)
        self.pair_end()
        self.end(2)


def grads_kernel(inv, imgt_hbm, txt_hbm, e_hbm, a_ref, b_ref, part_ref, img_out, txt_out, part_out,
                 imgt, txt, erow, ecol, gb0, gb1, arow, stage, iacc, tacc, ibuf, tbuf, dbuf, pa, pb, psum,
                 local_sems, row_sems, col_sems, send_sems, recv_sems):
    g = Grid()
    n = iacc.shape[1]
    d = iacc.shape[2]
    m = imgt.shape[1]
    nt = txt.shape[0]
    img_offs = [(dy, dz) for dy in (0, 1) for dz in range(4) if (dy, dz) != (0, 0)]
    txt_offs = [(dc, dy, dx) for dc in (0, 1) for dy in (0, 1) for dx in range(4) if (dc, dy, dx) != (0, 0, 0)]

    def row_load(step):
        k = ORDER[step]
        return pltpu.make_async_copy(e_hbm.at[pl.ds(k * n, n)], erow.at[step % 2], row_sems.at[step % 2])

    def col_load(step, side):
        k = ORDER[step] + 8 * side
        return pltpu.make_async_copy(e_hbm.at[:, pl.ds(k * n, n)], ecol.at[side], col_sems.at[side])

    load_imgt = pltpu.make_async_copy(imgt_hbm, imgt, local_sems.at[0])
    load_txt = pltpu.make_async_copy(txt_hbm, txt, local_sems.at[1])
    cols = {}
    cols[0, 1] = col_load(0, 1)
    cols[0, 1].start()
    load_imgt.start()
    rows = {0: row_load(0)}
    rows[0].start()
    load_txt.start()
    cols[0, 0] = col_load(0, 0)
    cols[0, 0].start()
    for i in range(m // 128):
        arow[i * 128:(i + 1) * 128, :] = jnp.broadcast_to(a_ref[i:i + 1, :], (128, 128)).T
    greet([g.img_peer(*o) for o in img_offs] + [g.txt_peer(*o) for o in txt_offs])
    net = Net(send_sems, recv_sems)
    core = g.txt_peer(1, 0, 0)
    ia = g.z * 2 + g.y % 2
    ib = (g.x * 2 + g.y // 2) * 2 + g.c
    scal_a = [net.send(part_ref, pa.at[ia], g.img_peer(*o)) for o in img_offs]
    pa[ia] = part_ref[...]
    img = Ring(net, iacc, ibuf, ICUT, g.img_peer(0, 1), g.img_peer(0, 3), g.img_peer(1, 0))
    txr = Ring(net, tacc, tbuf, TCUT, g.txt_peer(0, 0, 1), g.txt_peer(0, 0, 3), g.txt_peer(0, 1, 0))

    def minus_diag(grad, q):
        r = lax.broadcasted_iota(jnp.int32, (n, 128), 0)
        c = lax.broadcasted_iota(jnp.int32, (n, 128), 1) + q * 128
        head = grad[:n] - jnp.where(r == c, 2.0 * inv, 0.0)
        return head if grad.shape[0] == n else jnp.concatenate([head, grad[n:]], axis=0)

    def col_slot(k, e_ref, out_ref):
        b = [b_ref[2 * k + q:2 * k + q + 1, :] for q in range(n // 128)]

        def grad(i, to, diag=False):
            at = pl.ds(i * KC, KC)
            a = arow[at, :]
            for q in range(n // 128):
                lanes = slice(q * 128, (q + 1) * 128)
                v = e_ref[at, lanes] * (a + b[q])
                if diag:
                    v = minus_diag(v, q)
                to[:, lanes] = v.astype(BF16)

        grad(0, gb0[0], diag=k == 0)
        out_ref[...] = jnp.zeros_like(out_ref)
        count = m // KC

        def body(it, carry):
            for half, (now, later) in enumerate(((gb0[0], gb0[1]), (gb0[1], gb0[0]))):
                i = 2 * it + half
                at = pl.ds(pl.multiple_of(i * KC, KC), KC)
                out_ref[...] += jnp.dot(imgt[:, at], now[...], preferred_element_type=F32)
                grad_dyn((i + 1) % count, later)
            return carry

        def grad_dyn(i, to):
            at = pl.ds(pl.multiple_of(i * KC, KC), KC)
            a = arow[at, :]
            for q in range(n // 128):
                lanes = slice(q * 128, (q + 1) * 128)
                to[:, lanes] = (e_ref[at, lanes] * (a + b[q])).astype(BF16)

        lax.fori_loop(0, count // 2, body, 0)

    def row_slot(k, e_ref, out_ref):
        count = nt // KC

        def grad(i, to, diag=False):
            for q in range(KC // 128):
                lanes = pl.ds(pl.multiple_of(i * KC + q * 128, 128), 128)
                v = e_ref[:, lanes] * (arow[k * n:(k + 1) * n, :] + b_ref[pl.ds(i * (KC // 128) + q, 1), :])
                if diag and q < n // 128:
                    v = minus_diag(v, q)
                to[:, q * 128:(q + 1) * 128] = v.astype(BF16)

        grad(0, gb1[0], diag=k == 0)
        out_ref[...] = jnp.zeros_like(out_ref)

        def body(it, carry):
            for half, (now, later) in enumerate(((gb1[0], gb1[1]), (gb1[1], gb1[0]))):
                i = 2 * it + half
                at = pl.ds(pl.multiple_of(i * KC, KC), KC)
                out_ref[...] += jnp.dot(now[...], txt[at, :], preferred_element_type=F32)
                grad((i + 1) % count, later)
            return carry

        lax.fori_loop(0, count // 2, body, 0)

    cross = {}
    for step, k in enumerate(ORDER):
        cols[step, 1].wait()
        if step == 0:
            load_imgt.wait()
        if step >= 2:
            cross[ORDER[step - 2]].wait_send()
        col_slot(8 + k, ecol.at[1], stage.at[step % 2])
        cross[k] = net.send(stage.at[step % 2], dbuf.at[k], core)
        if step + 1 < len(ORDER):
            cols[step + 1, 1] = col_load(step + 1, 1)
            cols[step + 1, 1].start()
            rows[step + 1] = row_load(step + 1)
            rows[step + 1].start()
        rows[step].wait()
        if step == 0:
            load_txt.wait()
        row_slot(k, erow.at[step % 2], iacc.at[k])
        img.ready(step)
        cols[step, 0].wait()
        col_slot(k, ecol.at[0], tacc.at[k])
        if step + 1 < len(ORDER):
            cols[step + 1, 0] = col_load(step + 1, 0)
            cols[step + 1, 0].start()
        cross[k].wait_recv()
        tacc[k] += dbuf[k]
        txr.ready(step)
        if step == 1:
            for copy in scal_a:
                copy.wait_recv()
            total = pa[0]
            for q in range(1, 8):
                total += pa[q]
            psum[...] = total
            scal_b = [net.send(psum, pb.at[ib], g.txt_peer(*o)) for o in txt_offs]
            pb[ib] = total
    for r in (img, txr):
        r.mid(2)
    for copy in scal_b:
        copy.wait_recv()
    total = pb[0]
    for k in range(1, 16):
        total += pb[k]
    part_out[...] = total
    for r in (img, txr):
        r.close()
    img_out[...] = iacc[0]
    txt_out[...] = tacc[0]
    net.finish(skip=[cross[k] for k in ORDER[:-2]])


def grads(inv, imgt, txt_all, e, a, b, part):
    d, m = imgt.shape
    nt = txt_all.shape[0]
    n = m // 8
    vmem = pl.BlockSpec(memory_space=pltpu.VMEM)
    hbm = pl.BlockSpec(memory_space=pl.ANY)
    dma = pltpu.SemaphoreType.DMA
    return pl.pallas_call(
        functools.partial(grads_kernel, inv),
        out_shape=[jax.ShapeDtypeStruct((n, d), F32), jax.ShapeDtypeStruct((d, n), F32),
                   jax.ShapeDtypeStruct((8, 128), F32)],
        in_specs=[hbm, hbm, hbm, vmem, vmem, vmem],
        out_specs=[vmem] * 3,
        scratch_shapes=[pltpu.VMEM((d, m), BF16), pltpu.VMEM((nt, d), BF16), pltpu.VMEM((2, n, nt), F32),
                        pltpu.VMEM((2, m, n), F32), [pltpu.VMEM((KC, n), BF16)] * 2, [pltpu.VMEM((n, KC), BF16)] * 2,
                        pltpu.VMEM((m, 128), F32), pltpu.VMEM((2, d, n), F32), pltpu.VMEM((8, n, d), F32),
                        pltpu.VMEM((8, d, n), F32), pltpu.VMEM((8, n, d), F32), pltpu.VMEM((8, d, n), F32),
                        pltpu.VMEM((8, d, n), F32), pltpu.VMEM((8, 8, 128), F32), pltpu.VMEM((16, 8, 128), F32),
                        pltpu.VMEM((8, 128), F32), dma((2,)), dma((2,)), dma((2,)), dma((N_REDUCE,)),
                        dma((N_REDUCE,))],
        compiler_params=pltpu.CompilerParams(collective_id=2, has_side_effects=True, vmem_limit_bytes=VMEM_LIMIT),
        cost_estimate=pl.CostEstimate(flops=4 * m * nt * d, bytes_accessed=8 * m * nt, transcendentals=0),
        name="grads_reduce")(imgt, txt_all, e, a, b, part)


def solution(mesh):
    batch_spec = P(("row", "col"), None)
    shards = mesh.shape["row"] * mesh.shape["col"]

    def local_tile(img_loc, txt_loc, log_scale):
        n, d = img_loc.shape
        inv = 1.0 / (2 * n * shards)
        scale = jnp.exp(log_scale)
        pos = scale * jnp.sum(img_loc.astype(F32) * txt_loc.astype(F32), axis=1)
        img_all, txt_all = gather(img_loc, txt_loc)
        e, rs, rl, cs, cl, imgt = pass1(scale.reshape(1), img_all, txt_all)
        rows = lambda v: jnp.sum(v, axis=1).reshape(-1, 128)
        cols = lambda v: jnp.sum(v, axis=0).reshape(-1, 128)
        a, b, part = exchange_sums(inv, rows(rs), rows(rl), cols(cs), cols(cl), pos.reshape(-1, 128))
        img_sum, txt_sum, tot = grads(inv, imgt, txt_all, e, a, b, part)
        d_img = (scale * img_sum).astype(BF16)
        d_txt = (scale * txt_sum).T.astype(BF16)
        tot = jnp.sum(tot[0:2], axis=1)
        return tot[0], d_img, d_txt, tot[1]

    return jax.shard_map(local_tile, mesh=mesh, in_specs=(batch_spec, batch_spec, P()),
                         out_specs=(P(), batch_spec, batch_spec, P()), check_vma=False)
```

```python
import functools

import jax
import jax.numpy as jnp
from jax import lax
from jax.experimental import pallas as pl
from jax.experimental.pallas import tpu as pltpu
from jax.sharding import PartitionSpec as P

MESH = pl.DeviceIdType.MESH
F32 = jnp.float32
BF16 = jnp.bfloat16
VMEM_LIMIT = 64_000_000


class Grid:
    def __init__(self):
        row = lax.axis_index("row")
        self.c = lax.axis_index("col")
        self.z = row // 16
        self.y = (row // 4) % 4
        self.x = row % 4

    def dev(self, z, y, x, c):
        return {"row": (z * 4 + y) * 4 + x, "col": c}

    def y_a(self):
        return self.y + 1 - 2 * (self.y % 2)

    def y_b(self):
        return 3 - self.y

    def img_peer(self, dy, dz):
        y = self.y_a() if dy else self.y
        return self.dev((self.z + dz) % 4, y, self.x, self.c)

    def txt_peer(self, dc, dy, dx):
        y = self.y_b() if dy else self.y
        c = 1 - self.c if dc else self.c
        return self.dev(self.z, y, (self.x + dx) % 4, c)


class Net:
    def __init__(self, send_sems, recv_sems):
        self.send_sems, self.recv_sems, self.copies = send_sems, recv_sems, []

    def send(self, src, dst, peer):
        i = len(self.copies)
        copy = pltpu.make_async_remote_copy(
            src_ref=src, dst_ref=dst, send_sem=self.send_sems.at[i], recv_sem=self.recv_sems.at[i],
            device_id=peer, device_id_type=MESH)
        copy.start()
        self.copies.append(copy)
        return copy

    def finish(self, skip=()):
        for copy in self.copies:
            if not any(copy is other for other in skip):
                copy.wait_send()


def greet(peers):
    barrier = pltpu.get_barrier_semaphore()
    for peer in peers:
        pl.semaphore_signal(barrier, inc=1, device_id=peer, device_id_type=MESH)
    pl.semaphore_wait(barrier, len(peers))


def neighbours(g):
    return [g.img_peer(0, 1), g.img_peer(0, 3), g.img_peer(1, 0), g.txt_peer(0, 0, 1), g.txt_peer(0, 0, 3),
            g.txt_peer(0, 1, 0), g.txt_peer(1, 0, 0)]


POS = {0: 0, 4: 1, 3: 2, 1: 3, 2: 4, 7: 5, 5: 6, 6: 7}
N_FORWARD = 2 * 18 + 9 + 22


class Gather:
    def __init__(self, net, own, dst, plus, minus, pair):
        self.net, self.own, self.dst = net, own, dst
        self.n = own.shape[0]
        self.plus, self.minus, self.pair = plus, minus, pair
        self.got = {}

    def half(self, k, side):
        h = self.n // 2
        return self.dst.at[POS[k], pl.ds(side * h, h)]

    def send(self, key, src, k, side, peer):
        self.got[key, side] = self.net.send(src, self.half(k, side), peer)

    def first(self):
        h = self.n // 2
        own = [self.own.at[pl.ds(side * h, h)] for side in (0, 1)]
        for side in (0, 1):
            self.send("p0", own[side], 3, side, self.plus)
            self.send("m0", own[1 - side], 1, 1 - side, self.minus)
            self.send("y0", own[side], 4, side, self.pair)

    def wait(self, *keys):
        for key in keys:
            self.got[key].wait_recv()

    def far(self, dy):
        self.wait(("p%d" % dy, 0))
        self.send("f%d" % dy, self.half(4 * dy + 3, 0), 4 * dy + 2, 0, self.plus)
        self.wait(("m%d" % dy, 1))
        self.send("f%d" % dy, self.half(4 * dy + 1, 1), 4 * dy + 2, 1, self.minus)

    def second(self):
        self.wait(("y0", 0), ("y0", 1))
        for side in (0, 1):
            self.send("p1", self.half(4, side), 7, side, self.plus)
            self.send("m1", self.half(4, 1 - side), 5, 1 - side, self.minus)


def forward_kernel(inv, scale_ref, img_ref, txt_ref, e_out, imgt_out, txt_out, a_ref, b_ref, part_ref,
                   img_all, txt_all, imgt, d0, d1, s0, s1, rs, rl, cs, cl, rsum, csum, rbuf, cbuf,
                   e_sems, t_sems, i_sems, own_sems, send_sems, recv_sems):
    g = Grid()
    n, d = img_ref.shape
    scale = scale_ref[0]
    img_offs = [(dy, dz) for dy in (0, 1) for dz in range(4) if (dy, dz) != (0, 0)]
    txt_offs = [(dc, dy, dx) for dc in (0, 1) for dy in (0, 1) for dx in range(4) if (dc, dy, dx) != (0, 0, 0)]
    own = [pltpu.make_async_copy(img_ref, img_all.at[0], own_sems.at[0]),
           pltpu.make_async_copy(txt_ref, txt_all.at[0], own_sems.at[1])]
    for copy in own:
        copy.start()
    greet([g.img_peer(*o) for o in img_offs] + [g.txt_peer(*o) for o in txt_offs])
    net = Net(send_sems, recv_sems)
    core = g.txt_peer(1, 0, 0)
    img = Gather(net, img_ref, img_all, g.img_peer(0, 1), g.img_peer(0, 3), g.img_peer(1, 0))
    txt = Gather(net, txt_ref, txt_all, g.txt_peer(0, 0, 1), g.txt_peer(0, 0, 3), g.txt_peer(0, 1, 0))
    img.first()
    txt.first()
    cross = {0: net.send(txt_ref, txt_all.at[8], core)}
    saves = []

    def save_txt(p):
        copy = pltpu.make_async_copy(txt_all.at[p], txt_out.at[pl.ds(p * n, n)], t_sems.at[p])
        copy.start()
        saves.append(copy)

    def got_txt(*slots):
        for k in slots:
            p = POS[k]
            cross[p] = net.send(txt_all.at[p], txt_all.at[8 + p], core)
            save_txt(p)

    def got_cross(*slots):
        for k in slots:
            cross[POS[k]].wait_recv()
            save_txt(8 + POS[k])

    def got_img(*slots):
        for k in slots:
            p = POS[k]
            imgt[p] = img_all[p].T
            copy = pltpu.make_async_copy(imgt.at[p], imgt_out.at[:, pl.ds(p * n, n)], i_sems.at[p])
            copy.start()
            saves.append(copy)

    dots, stage = (d0, d1), (s0, s1)

    def dot(i, k, buf):
        lhs = img_all[i]
        for side in (0, 1):
            dots[buf][side] = lax.dot_general(lhs, txt_all[8 * side + k], (((1,), (1,)), ((), ())),
                                              preferred_element_type=F32)

    def store(i, k, buf):
        return pltpu.make_async_copy(stage[buf], e_out.at[i, :, k], e_sems.at[buf])

    def finish_unit(i, k, buf, first=False):
        if not first:
            store(i, k, buf).wait()
        at = pl.ds(i * n, n) if isinstance(i, int) else pl.ds(pl.multiple_of(i * n, n), n)
        for blk in range(n // 32):
            lo = blk * 32
            rows = pl.ds(i * n + lo, 32) if isinstance(i, int) else pl.ds(pl.multiple_of(i * n + lo, 32), 32)
            racc, lacc = rs[rows, :], rl[rows, :]
            for side in (0, 1):
                logits = scale * dots[buf][side, lo:lo + 32, :]
                e = jnp.exp(logits)
                el = e * logits
                stage[buf][side, lo:lo + 32, :] = e
                for q in range(n // 128):
                    racc += e[:, q * 128:(q + 1) * 128]
                    lacc += el[:, q * 128:(q + 1) * 128]
                cs[8 * side + k] += jnp.sum(e.reshape(4, 8, n), axis=0)
                cl[8 * side + k] += jnp.sum(el.reshape(4, 8, n), axis=0)
            rs[rows, :] = racc
            rl[rows, :] = lacc
        store(i, k, buf).start()

    state = {"buf": 0, "unit": (0, 0)}

    def one(i, k, first=False):
        buf = state["buf"]
        dot(i, k, 1 - buf)
        finish_unit(*state["unit"], buf, first)
        state["buf"], state["unit"] = 1 - buf, (i, k)

    def run(i0, k0, width, start, count):
        buf = state["buf"]

        def unit(u):
            return i0 + u // width, k0 + u % width

        def body(it, carry):
            u = start + 2 * it
            dot(*unit(u), 1 - buf)
            finish_unit(carry[0], carry[1], buf)
            dot(*unit(u + 1), buf)
            finish_unit(*unit(u), 1 - buf)
            return unit(u + 1)

        last = tuple(jnp.int32(v) for v in state["unit"])
        state["unit"] = lax.fori_loop(0, count // 2, body, last)
        if count % 2:
            one(*unit(jnp.int32(start + count - 1)))

    rs[...] = jnp.zeros_like(rs)
    rl[...] = jnp.zeros_like(rl)
    cs[...] = jnp.zeros_like(cs)
    cl[...] = jnp.zeros_like(cl)
    for copy in own:
        copy.wait()
    save_txt(0)
    got_img(0)
    img.far(0)
    txt.far(0)
    img.second()
    txt.second()
    got_txt(4)
    txt.wait(("p0", 1), ("m0", 0))
    got_txt(3, 1)
    got_cross(0)
    dot(0, 0, 0)
    img.wait(("p0", 1), ("m0", 0))
    got_cross(4, 3, 1)
    one(0, 1, True)
    one(0, 2, True)
    run(0, 0, 4, 3, 13)
    got_img(4, 3, 1)
    for r in (txt, img):
        r.wait(("f0", 0), ("f0", 1))
    got_txt(2)
    run(4, 0, 4, 0, 4)
    got_cross(2)
    run(0, 4, 1, 0, 5)
    got_img(2)
    for r in (txt, img):
        r.far(1)
    txt.wait(("p1", 1), ("m1", 0))
    got_txt(7, 5)
    img.wait(("p1", 1), ("m1", 0))
    run(5, 0, 5, 0, 10)
    got_cross(7, 5)
    run(0, 5, 2, 0, 6)
    txt.wait(("f1", 0), ("f1", 1))
    got_txt(6)
    run(3, 5, 2, 0, 8)
    got_img(7, 5)
    img.wait(("f1", 0), ("f1", 1))
    got_cross(6)
    run(7, 0, 8, 0, 8)
    run(0, 7, 1, 0, 7)
    finish_unit(*state["unit"], state["buf"])

    for p in range(16):
        for q in range(n // 128):
            csum[2 * p + q:2 * p + q + 1, :] = jnp.sum(cs[p, :, q * 128:(q + 1) * 128], axis=0, keepdims=True)
    sums = []
    for dc, dy, dx in txt_offs:
        sums.append(net.send(csum, cbuf.at[dc * 8 + dy * 4 + (4 - dx) % 4], g.txt_peer(dc, dy, dx)))
    for i in range(8 * n // 128):
        rsum[i:i + 1, :] = jnp.sum(rs[i * 128:(i + 1) * 128, :].T, axis=0, keepdims=True)
    for dy, dz in img_offs:
        sums.append(net.send(rsum, rbuf.at[dy * 4 + (4 - dz) % 4], g.img_peer(dy, dz)))
    got_img(6)
    pos = jnp.sum(img_ref[...].astype(F32) * txt_ref[...].astype(F32), axis=1, keepdims=True) * scale
    rlsum = [jnp.sum(rl[i * 128:(i + 1) * 128, :].T, axis=0, keepdims=True) for i in range(8 * n // 128)]
    clsum = [jnp.sum(cl[p, :, q * 128:(q + 1) * 128], axis=0, keepdims=True) for p in range(16) for q in range(n // 128)]
    for copy in sums:
        copy.wait_recv()
    loss = jnp.zeros((2, 128), F32)
    dt = jnp.zeros((1, 128), F32)
    for dy, dz in [(0, 0)] + img_offs:
        k = 2 * POS[dy * 4 + dz]
        tot = rsum[k:k + 2, :]
        for oy, oz in img_offs:
            q = 2 * POS[(dy ^ oy) * 4 + (dz - oz) % 4]
            tot += rbuf[oy * 4 + oz, q:q + 2, :]
        a = 1.0 / tot
        a_ref[k:k + 2, :] = a * inv
        dt += a[0:1] * rlsum[k] + a[1:2] * rlsum[k + 1]
        if k == 0:
            loss += jnp.log(tot)
    for dc, dy, dx in [(0, 0, 0)] + txt_offs:
        k = 2 * (dc * 8 + POS[dy * 4 + dx])
        tot = csum[k:k + 2, :]
        for oc, oy, ox in txt_offs:
            q = 2 * ((dc ^ oc) * 8 + POS[(dy ^ oy) * 4 + (dx - ox) % 4])
            tot += cbuf[oc * 8 + oy * 4 + ox, q:q + 2, :]
        b = 1.0 / tot
        b_ref[k:k + 2, :] = b * inv
        dt += b[0:1] * clsum[k] + b[1:2] * clsum[k + 1]
        if k == 0:
            loss += jnp.log(tot)
    diag = jnp.sum(pos, axis=0, keepdims=True)
    first_lane = lax.broadcasted_iota(jnp.int32, (1, 128), 1) == 0
    diag = jnp.where(first_lane, 2.0 * diag, 0.0)
    part_ref[...] = jnp.zeros_like(part_ref)
    part_ref[0:1, :] = (jnp.sum(loss, axis=0, keepdims=True) - diag) * inv
    part_ref[1:2, :] = (dt - diag) * inv
    for buf in (0, 1):
        store(0, 0, buf).wait()
    for copy in saves:
        copy.wait()
    net.finish()


def forward(inv, scale, img, txt):
    n, d = img.shape
    vmem = pl.BlockSpec(memory_space=pltpu.VMEM)
    hbm = pl.BlockSpec(memory_space=pl.ANY)
    dma = pltpu.SemaphoreType.DMA
    return pl.pallas_call(
        functools.partial(forward_kernel, inv),
        out_shape=[jax.ShapeDtypeStruct((8, 2, 8, n, n), F32), jax.ShapeDtypeStruct((d, 8 * n), BF16),
                   jax.ShapeDtypeStruct((16 * n, d), BF16), jax.ShapeDtypeStruct((16, 128), F32),
                   jax.ShapeDtypeStruct((32, 128), F32), jax.ShapeDtypeStruct((8, 128), F32)],
        in_specs=[pl.BlockSpec(memory_space=pltpu.SMEM), vmem, vmem],
        out_specs=[hbm, hbm, hbm, vmem, vmem, vmem],
        scratch_shapes=[pltpu.VMEM((8, n, d), BF16), pltpu.VMEM((16, n, d), BF16), pltpu.VMEM((8, d, n), BF16),
                        pltpu.VMEM((2, n, n), F32), pltpu.VMEM((2, n, n), F32), pltpu.VMEM((2, n, n), F32),
                        pltpu.VMEM((2, n, n), F32), pltpu.VMEM((8 * n, 128), F32), pltpu.VMEM((8 * n, 128), F32),
                        pltpu.VMEM((16, 8, n), F32), pltpu.VMEM((16, 8, n), F32), pltpu.VMEM((16, 128), F32),
                        pltpu.VMEM((32, 128), F32), pltpu.VMEM((8, 16, 128), F32), pltpu.VMEM((16, 32, 128), F32),
                        dma((2,)), dma((16,)), dma((8,)), dma((2,)), dma((N_FORWARD,)), dma((N_FORWARD,))],
        compiler_params=pltpu.CompilerParams(collective_id=0, has_side_effects=True, vmem_limit_bytes=VMEM_LIMIT),
        name="forward_sums")(scale, img, txt)


ICUT = 144
TCUT = 432
ORDER = (6, 5, 7, 2, 1, 4, 3, 0)
KC = 512
N_REDUCE = 8 + 2 * (4 + 18 + 1) + 22


class Ring:
    def __init__(self, net, acc, buf, cut, plus, minus, pair):
        self.net, self.acc, self.buf = net, acc, buf
        self.cut, self.rows = cut, acc.shape[1]
        self.plus, self.minus, self.pair = plus, minus, pair
        self.early, self.streams = {}, {}

    def pair_send(self, d):
        at = pl.ds(self.cut, self.rows - self.cut)
        self.early[d] = self.net.send(self.acc.at[4 + d, at], self.buf.at[4 + d, at], self.pair)

    def pair_add(self, d):
        self.early[d].wait_recv()
        self.acc[d, self.cut:] += self.buf[4 + d, self.cut:]

    def where(self, name):
        if name == 2:
            return 0, self.cut, (self.rows - self.cut) // 2
        return 4 * name, 0, self.cut // 2

    def send(self, name, key, slot, half, to_slot, peer):
        _, lo, h = self.where(name)
        at = pl.ds(lo + half * h, h)
        self.streams[name, key] = self.net.send(self.acc.at[slot, at], self.buf.at[to_slot, at], peer)

    def far(self, name):
        b, _, _ = self.where(name)
        self.send(name, "a+", b + 2, 0, b + 2, self.plus)
        self.send(name, "a-", b + 2, 1, b + 2, self.minus)

    def plain_plus(self, name):
        b, _, _ = self.where(name)
        self.send(name, "b+1", b + 1, 1, b + 3, self.plus)

    def plain_minus(self, name):
        b, _, _ = self.where(name)
        self.send(name, "b-0", b + 3, 0, b + 1, self.minus)

    def mid(self, name):
        b, lo, h = self.where(name)
        self.streams[name, "a+"].wait_recv()
        self.acc[b + 1, lo:lo + h] += self.buf[b + 2, lo:lo + h]
        self.send(name, "b+0", b + 1, 0, b + 3, self.plus)
        self.streams[name, "a-"].wait_recv()
        self.acc[b + 3, lo + h:lo + 2 * h] += self.buf[b + 2, lo + h:lo + 2 * h]
        self.send(name, "b-1", b + 3, 1, b + 1, self.minus)

    def end(self, name):
        b, lo, h = self.where(name)
        for key in ("b+1", "b-0", "b+0", "b-1"):
            self.streams[name, key].wait_recv()
        self.acc[b, lo:lo + 2 * h] += self.buf[b + 1, lo:lo + 2 * h] + self.buf[b + 3, lo:lo + 2 * h]

    def pair_last(self):
        at = pl.ds(0, self.cut)
        self.late = self.net.send(self.acc.at[4, at], self.buf.at[0, at], self.pair)

    def pair_end(self):
        self.late.wait_recv()
        self.acc[0, 0:self.cut] += self.buf[0, 0:self.cut]

    def ready(self, step):
        if step == 0:
            self.pair_send(2)
            self.far(1)
        elif step == 1:
            self.pair_send(1)
            self.plain_plus(1)
        elif step == 2:
            self.pair_send(3)
            self.plain_minus(1)
            self.mid(1)
        elif step == 3:
            self.far(0)
            self.pair_add(2)
            self.far(2)
        elif step == 4:
            self.plain_plus(0)
            self.pair_add(1)
            self.plain_plus(2)
        elif step == 5:
            self.pair_send(0)
            self.end(1)
            self.pair_last()
        elif step == 6:
            self.plain_minus(0)
            self.pair_add(3)
            self.plain_minus(2)
            self.mid(0)

    def close(self):
        self.pair_add(0)
        self.end(0)
        self.pair_end()
        self.end(2)


def grads_kernel(inv, imgt_hbm, txt_hbm, e_hbm, a_ref, b_ref, part_ref, img_out, txt_out, part_out,
                 imgt, txt, erow, ecol, gb0, gb1, arow, stage, iacc, tacc, ibuf, tbuf, dbuf, pa, pb, psum,
                 local_sems, row_sems, col_sems, send_sems, recv_sems):
    g = Grid()
    n = iacc.shape[1]
    d = iacc.shape[2]
    m = imgt.shape[1]
    nt = txt.shape[0]
    img_offs = [(dy, dz) for dy in (0, 1) for dz in range(4) if (dy, dz) != (0, 0)]
    txt_offs = [(dc, dy, dx) for dc in (0, 1) for dy in (0, 1) for dx in range(4) if (dc, dy, dx) != (0, 0, 0)]

    def row_load(step):
        return pltpu.make_async_copy(e_hbm.at[POS[ORDER[step]]], erow.at[step % 2], row_sems.at[step % 2])

    def col_load(step, side):
        return pltpu.make_async_copy(e_hbm.at[:, side, POS[ORDER[step]]], ecol.at[side], col_sems.at[side])

    load_imgt = pltpu.make_async_copy(imgt_hbm, imgt, local_sems.at[0])
    load_txt = pltpu.make_async_copy(txt_hbm, txt, local_sems.at[1])
    cols = {}
    cols[0, 1] = col_load(0, 1)
    cols[0, 1].start()
    load_imgt.start()
    rows = {0: row_load(0)}
    rows[0].start()
    load_txt.start()
    cols[0, 0] = col_load(0, 0)
    cols[0, 0].start()
    for i in range(m // 128):
        arow[i * 128:(i + 1) * 128, :] = jnp.broadcast_to(a_ref[i:i + 1, :], (128, 128)).T
    greet([g.img_peer(*o) for o in img_offs] + [g.txt_peer(*o) for o in txt_offs])
    net = Net(send_sems, recv_sems)
    core = g.txt_peer(1, 0, 0)
    ia = g.z * 2 + g.y % 2
    ib = (g.x * 2 + g.y // 2) * 2 + g.c
    scal_a = [net.send(part_ref, pa.at[ia], g.img_peer(*o)) for o in img_offs]
    pa[ia] = part_ref[...]
    img = Ring(net, iacc, ibuf, ICUT, g.img_peer(0, 1), g.img_peer(0, 3), g.img_peer(1, 0))
    txr = Ring(net, tacc, tbuf, TCUT, g.txt_peer(0, 0, 1), g.txt_peer(0, 0, 3), g.txt_peer(0, 1, 0))

    def minus_diag(grad, q):
        r = lax.broadcasted_iota(jnp.int32, (n, 128), 0)
        c = lax.broadcasted_iota(jnp.int32, (n, 128), 1) + q * 128
        return grad - jnp.where(r == c, 2.0 * inv, 0.0)

    def col_slot(p, e_ref, out_ref):
        b = [b_ref[2 * p + q:2 * p + q + 1, :] for q in range(n // 128)]
        tiles = KC // n
        count = m // KC

        def grad(i, to, diag=False):
            for t in range(tiles):
                for q in range(n // 128):
                    lanes = slice(q * 128, (q + 1) * 128)
                    a = arow[pl.ds(pl.multiple_of(i * KC + t * n, n), n), :]
                    v = e_ref[i * tiles + t, :, lanes] * (a + b[q])
                    if diag and t == 0:
                        v = minus_diag(v, q)
                    to[t * n:(t + 1) * n, lanes] = v.astype(BF16)

        grad(0, gb0[0], diag=p == 0)
        out_ref[...] = jnp.zeros_like(out_ref)

        def body(it, carry):
            for half, (now, later) in enumerate(((gb0[0], gb0[1]), (gb0[1], gb0[0]))):
                i = 2 * it + half
                at = pl.ds(pl.multiple_of(i * KC, KC), KC)
                out_ref[...] += jnp.dot(imgt[:, at], now[...], preferred_element_type=F32)
                grad((i + 1) % count, later)
            return carry

        lax.fori_loop(0, count // 2, body, 0)

    def row_slot(p, e_ref, out_ref):
        tiles = KC // n
        count = nt // KC

        def grad(i, to, diag=False):
            for t in range(tiles):
                tile = i * tiles + t
                for q in range(n // 128):
                    lanes = slice(q * 128, (q + 1) * 128)
                    v = (e_ref[tile // 8, tile % 8, :, lanes]
                         * (arow[p * n:(p + 1) * n, :] + b_ref[pl.ds(2 * tile + q, 1), :]))
                    if diag and t == 0:
                        v = minus_diag(v, q)
                    to[:, t * n + q * 128:t * n + (q + 1) * 128] = v.astype(BF16)

        grad(0, gb1[0], diag=p == 0)
        out_ref[...] = jnp.zeros_like(out_ref)

        def body(it, carry):
            for half, (now, later) in enumerate(((gb1[0], gb1[1]), (gb1[1], gb1[0]))):
                i = 2 * it + half
                at = pl.ds(pl.multiple_of(i * KC, KC), KC)
                out_ref[...] += jnp.dot(now[...], txt[at, :], preferred_element_type=F32)
                grad((i + 1) % count, later)
            return carry

        lax.fori_loop(0, count // 2, body, 0)

    cross = {}
    for step, k in enumerate(ORDER):
        cols[step, 1].wait()
        if step == 0:
            load_imgt.wait()
        if step >= 2:
            cross[ORDER[step - 2]].wait_send()
        col_slot(8 + POS[k], ecol.at[1], stage.at[step % 2])
        cross[k] = net.send(stage.at[step % 2], dbuf.at[k], core)
        if step + 1 < len(ORDER):
            cols[step + 1, 1] = col_load(step + 1, 1)
            cols[step + 1, 1].start()
            rows[step + 1] = row_load(step + 1)
            rows[step + 1].start()
        rows[step].wait()
        if step == 0:
            load_txt.wait()
        row_slot(POS[k], erow.at[step % 2], iacc.at[k])
        img.ready(step)
        cols[step, 0].wait()
        col_slot(POS[k], ecol.at[0], tacc.at[k])
        if step + 1 < len(ORDER):
            cols[step + 1, 0] = col_load(step + 1, 0)
            cols[step + 1, 0].start()
        cross[k].wait_recv()
        tacc[k] += dbuf[k]
        txr.ready(step)
        if step == 1:
            for copy in scal_a:
                copy.wait_recv()
            total = pa[0]
            for q in range(1, 8):
                total += pa[q]
            psum[...] = total
            scal_b = [net.send(psum, pb.at[ib], g.txt_peer(*o)) for o in txt_offs]
            pb[ib] = total
    for r in (img, txr):
        r.mid(2)
    for copy in scal_b:
        copy.wait_recv()
    total = pb[0]
    for k in range(1, 16):
        total += pb[k]
    part_out[...] = total
    for r in (img, txr):
        r.close()
    img_out[...] = iacc[0]
    txt_out[...] = tacc[0]
    net.finish(skip=[cross[k] for k in ORDER[:-2]])


def grads(inv, imgt, txt_all, e, a, b, part):
    d, m = imgt.shape
    nt = txt_all.shape[0]
    n = m // 8
    vmem = pl.BlockSpec(memory_space=pltpu.VMEM)
    hbm = pl.BlockSpec(memory_space=pl.ANY)
    dma = pltpu.SemaphoreType.DMA
    return pl.pallas_call(
        functools.partial(grads_kernel, inv),
        out_shape=[jax.ShapeDtypeStruct((n, d), F32), jax.ShapeDtypeStruct((d, n), F32),
                   jax.ShapeDtypeStruct((8, 128), F32)],
        in_specs=[hbm, hbm, hbm, vmem, vmem, vmem],
        out_specs=[vmem] * 3,
        scratch_shapes=[pltpu.VMEM((d, m), BF16), pltpu.VMEM((nt, d), BF16), pltpu.VMEM((2, 2, 8, n, n), F32),
                        pltpu.VMEM((2, 8, n, n), F32), [pltpu.VMEM((KC, n), BF16)] * 2, [pltpu.VMEM((n, KC), BF16)] * 2,
                        pltpu.VMEM((m, 128), F32), pltpu.VMEM((2, d, n), F32), pltpu.VMEM((8, n, d), F32),
                        pltpu.VMEM((8, d, n), F32), pltpu.VMEM((8, n, d), F32), pltpu.VMEM((8, d, n), F32),
                        pltpu.VMEM((8, d, n), F32), pltpu.VMEM((8, 8, 128), F32), pltpu.VMEM((16, 8, 128), F32),
                        pltpu.VMEM((8, 128), F32), dma((2,)), dma((2,)), dma((2,)), dma((N_REDUCE,)),
                        dma((N_REDUCE,))],
        compiler_params=pltpu.CompilerParams(collective_id=2, has_side_effects=True, vmem_limit_bytes=VMEM_LIMIT),
        cost_estimate=pl.CostEstimate(flops=4 * m * nt * d, bytes_accessed=8 * m * nt, transcendentals=0),
        name="grads_reduce")(imgt, txt_all, e, a, b, part)


def solution(mesh):
    batch_spec = P(("row", "col"), None)
    shards = mesh.shape["row"] * mesh.shape["col"]

    def local_tile(img_loc, txt_loc, log_scale):
        n, d = img_loc.shape
        inv = 1.0 / (2 * n * shards)
        scale = jnp.exp(log_scale)
        e, imgt, txt_all, a, b, part = forward(inv, scale.reshape(1), img_loc, txt_loc)
        img_sum, txt_sum, tot = grads(inv, imgt, txt_all, e, a, b, part)
        d_img = (scale * img_sum).astype(BF16)
        d_txt = (scale * txt_sum).T.astype(BF16)
        tot = jnp.sum(tot[0:2], axis=1)
        return tot[0], d_img, d_txt, tot[1]

    return jax.shard_map(local_tile, mesh=mesh, in_specs=(batch_spec, batch_spec, P()),
                         out_specs=(P(), batch_spec, batch_spec, P()), check_vma=False)
```

```python
import functools

import jax
import jax.numpy as jnp
from jax import lax
from jax.experimental import pallas as pl
from jax.experimental.pallas import tpu as pltpu
from jax.sharding import PartitionSpec as P

MESH = pl.DeviceIdType.MESH
F32 = jnp.float32
BF16 = jnp.bfloat16
VMEM_LIMIT = 64_000_000


class Grid:
    def __init__(self):
        row = lax.axis_index("row")
        self.c = lax.axis_index("col")
        self.z = row // 16
        self.y = (row // 4) % 4
        self.x = row % 4

    def dev(self, z, y, x, c):
        return {"row": (z * 4 + y) * 4 + x, "col": c}

    def y_a(self):
        return self.y + 1 - 2 * (self.y % 2)

    def y_b(self):
        return 3 - self.y

    def img_peer(self, dy, dz):
        y = self.y_a() if dy else self.y
        return self.dev((self.z + dz) % 4, y, self.x, self.c)

    def txt_peer(self, dc, dy, dx):
        y = self.y_b() if dy else self.y
        c = 1 - self.c if dc else self.c
        return self.dev(self.z, y, (self.x + dx) % 4, c)


def view(ref):
    return ref[0].at[ref[1]] if isinstance(ref, tuple) else ref


class Copy:
    def __init__(self, net, i, src, dst, peer):
        self.net, self.i, self.src, self.dst, self.peer = net, i, src, dst, peer

    def make(self):
        return pltpu.make_async_remote_copy(
            src_ref=view(self.src), dst_ref=view(self.dst), send_sem=self.net.send_sems.at[self.i],
            recv_sem=self.net.recv_sems.at[self.i], device_id=self.peer, device_id_type=MESH)

    def wait_recv(self):
        self.make().wait_recv()

    def wait_send(self):
        self.make().wait_send()


class Net:
    def __init__(self, send_sems, recv_sems):
        self.send_sems, self.recv_sems, self.copies = send_sems, recv_sems, []

    def send(self, src, dst, peer):
        copy = Copy(self, len(self.copies), src, dst, peer)
        copy.make().start()
        self.copies.append(copy)
        return copy

    def finish(self):
        for copy in self.copies:
            copy.wait_send()


def greet(peers):
    barrier = pltpu.get_barrier_semaphore()
    for peer in peers:
        pl.semaphore_signal(barrier, inc=1, device_id=peer, device_id_type=MESH)
    pl.semaphore_wait(barrier, len(peers))


def neighbours(g):
    return [g.img_peer(0, 1), g.img_peer(0, 3), g.img_peer(1, 0), g.txt_peer(0, 0, 1), g.txt_peer(0, 0, 3),
            g.txt_peer(0, 1, 0), g.txt_peer(1, 0, 0)]


POS = {0: 0, 3: 1, 4: 2, 1: 3, 2: 4, 7: 5, 5: 6, 6: 7}
DEEP = 4
N_FORWARD = 2 * 18 + 9 + 22


class Gather:
    def __init__(self, net, own, dst, plus, minus, pair):
        self.net, self.own, self.dst = net, own, dst
        self.n = own.shape[0]
        self.plus, self.minus, self.pair = plus, minus, pair
        self.got = {}

    def half(self, k, side):
        h = self.n // 2
        return self.dst.at[POS[k], pl.ds(side * h, h)]

    def send(self, key, src, k, side, peer):
        self.got[key, side] = self.net.send(src, self.half(k, side), peer)

    def first(self):
        h = self.n // 2
        own = [self.own.at[pl.ds(side * h, h)] for side in (0, 1)]
        for side in (0, 1):
            self.send("p0", own[side], 3, side, self.plus)
            self.send("m0", own[1 - side], 1, 1 - side, self.minus)
            self.send("y0", own[side], 4, side, self.pair)

    def wait(self, *keys):
        for key in keys:
            self.got[key].wait_recv()

    def far(self, dy):
        self.wait(("p%d" % dy, 0))
        self.send("f%d" % dy, self.half(4 * dy + 3, 0), 4 * dy + 2, 0, self.plus)
        self.wait(("m%d" % dy, 1))
        self.send("f%d" % dy, self.half(4 * dy + 1, 1), 4 * dy + 2, 1, self.minus)

    def second(self):
        self.wait(("y0", 0), ("y0", 1))
        for side in (0, 1):
            self.send("p1", self.half(4, side), 7, side, self.plus)
            self.send("m1", self.half(4, 1 - side), 5, 1 - side, self.minus)


def forward_kernel(inv, scale_ref, img_ref, txt_ref, e_out, imgt_out, txt_out, a_ref, b_ref, part_ref,
                   img_all, txt_all, imgt, d0, d1, s0, s1, rs, rl, cs, cl, rsum, csum, rbuf, cbuf,
                   e_sems, t_sems, i_sems, own_sems, send_sems, recv_sems):
    g = Grid()
    n, d = img_ref.shape
    scale = scale_ref[0]
    img_offs = [(dy, dz) for dy in (0, 1) for dz in range(4) if (dy, dz) != (0, 0)]
    txt_offs = [(dc, dy, dx) for dc in (0, 1) for dy in (0, 1) for dx in range(4) if (dc, dy, dx) != (0, 0, 0)]
    own = [pltpu.make_async_copy(img_ref, img_all.at[0], own_sems.at[0]),
           pltpu.make_async_copy(txt_ref, txt_all.at[0], own_sems.at[1])]
    for copy in own:
        copy.start()
    greet([g.img_peer(*o) for o in img_offs] + [g.txt_peer(*o) for o in txt_offs])
    net = Net(send_sems, recv_sems)
    core = g.txt_peer(1, 0, 0)
    img = Gather(net, img_ref, img_all, g.img_peer(0, 1), g.img_peer(0, 3), g.img_peer(1, 0))
    txt = Gather(net, txt_ref, txt_all, g.txt_peer(0, 0, 1), g.txt_peer(0, 0, 3), g.txt_peer(0, 1, 0))
    img.first()
    txt.first()
    cross = {0: net.send(txt_ref, txt_all.at[8], core)}
    saves = []

    def save_txt(p):
        copy = pltpu.make_async_copy(txt_all.at[p], txt_out.at[pl.ds(p * n, n)], t_sems.at[p])
        copy.start()
        saves.append(copy)

    def got_txt(*slots):
        for k in slots:
            p = POS[k]
            cross[p] = net.send(txt_all.at[p], txt_all.at[8 + p], core)
            save_txt(p)

    def got_cross(*slots):
        for k in slots:
            cross[POS[k]].wait_recv()
            save_txt(8 + POS[k])

    def got_img(*slots):
        for k in slots:
            p = POS[k]
            imgt[p] = img_all[p].T
            copy = pltpu.make_async_copy(imgt.at[p], imgt_out.at[:, pl.ds(p * n, n)], i_sems.at[p])
            copy.start()
            saves.append(copy)

    dots, stage = (d0, d1), (s0, s1)

    def dot(i, k, buf):
        lhs = img_all[i]
        for side in (0, 1):
            dots[buf][side] = lax.dot_general(lhs, txt_all[8 * side + k], (((1,), (1,)), ((), ())),
                                              preferred_element_type=F32)

    def store(i, k, buf, slot):
        return pltpu.make_async_copy(stage[buf].at[slot], e_out.at[i, :, k], e_sems.at[buf * DEEP + slot])

    def free(buf, use):
        if isinstance(use, int):
            if use >= DEEP:
                store(0, 0, buf, use % DEEP).wait()
        else:
            @pl.when(use >= DEEP)
            def _():
                store(0, 0, buf, use % DEEP).wait()

    def finish_unit(i, k, buf, use):
        slot = use % DEEP
        for blk in range(n // 32):
            lo = blk * 32
            rows = pl.ds(i * n + lo, 32) if isinstance(i, int) else pl.ds(pl.multiple_of(i * n + lo, 32), 32)
            racc, lacc = rs[rows, :], rl[rows, :]
            for side in (0, 1):
                logits = scale * dots[buf][side, lo:lo + 32, :]
                e = jnp.exp(logits)
                el = e * logits
                stage[buf][slot, side, lo:lo + 32, :] = e
                for q in range(n // 128):
                    racc += e[:, q * 128:(q + 1) * 128]
                    lacc += el[:, q * 128:(q + 1) * 128]
                cs[8 * side + k] += jnp.sum(e.reshape(4, 8, n), axis=0)
                cl[8 * side + k] += jnp.sum(el.reshape(4, 8, n), axis=0)
            rs[rows, :] = racc
            rl[rows, :] = lacc
        store(i, k, buf, slot).start()

    state = {"buf": 0, "unit": (0, 0), "uses": [0, 0]}

    def last_unit():
        buf = state["buf"]
        free(buf, state["uses"][buf])
        finish_unit(*state["unit"], buf, state["uses"][buf])
        state["uses"][buf] += 1

    def one(i, k):
        buf = state["buf"]
        free(buf, state["uses"][buf])
        dot(i, k, 1 - buf)
        finish_unit(*state["unit"], buf, state["uses"][buf])
        state["uses"][buf] += 1
        state["buf"], state["unit"] = 1 - buf, (i, k)

    def run(i0, k0, width, start, count):
        buf = state["buf"]
        uses = list(state["uses"])

        def unit(u):
            return i0 + u // width, k0 + u % width

        def body(it, carry):
            u = start + 2 * it
            free(buf, uses[buf] + it)
            free(1 - buf, uses[1 - buf] + it)
            dot(*unit(u), 1 - buf)
            finish_unit(carry[0], carry[1], buf, uses[buf] + it)
            dot(*unit(u + 1), buf)
            finish_unit(*unit(u), 1 - buf, uses[1 - buf] + it)
            return unit(u + 1)

        last = tuple(jnp.int32(v) for v in state["unit"])
        state["unit"] = lax.fori_loop(0, count // 2, body, last)
        state["uses"] = [v + count // 2 for v in uses]
        if count % 2:
            one(*unit(jnp.int32(start + count - 1)))

    rs[...] = jnp.zeros_like(rs)
    rl[...] = jnp.zeros_like(rl)
    cs[...] = jnp.zeros_like(cs)
    cl[...] = jnp.zeros_like(cl)
    for copy in own:
        copy.wait()
    save_txt(0)
    got_img(0)
    img.far(0)
    txt.far(0)
    img.second()
    txt.second()
    got_txt(4)
    txt.wait(("p0", 1), ("m0", 0))
    got_txt(3, 1)
    got_cross(0)
    dot(0, 0, 0)
    img.wait(("p0", 1), ("m0", 0))
    got_cross(4, 3, 1)
    run(0, 0, 4, 1, 15)
    got_img(4, 3, 1)
    for r in (txt, img):
        r.wait(("f0", 0), ("f0", 1))
    got_txt(2)
    run(4, 0, 4, 0, 4)
    got_cross(2)
    run(0, 4, 1, 0, 5)
    got_img(2)
    for r in (txt, img):
        r.far(1)
    txt.wait(("p1", 1), ("m1", 0))
    got_txt(7, 5)
    img.wait(("p1", 1), ("m1", 0))
    run(5, 0, 5, 0, 10)
    got_cross(7, 5)
    run(0, 5, 2, 0, 6)
    txt.wait(("f1", 0), ("f1", 1))
    got_txt(6)
    run(3, 5, 2, 0, 8)
    got_img(7, 5)
    img.wait(("f1", 0), ("f1", 1))
    got_cross(6)
    run(7, 0, 8, 0, 8)
    run(0, 7, 1, 0, 7)
    last_unit()

    for p in range(16):
        for q in range(n // 128):
            csum[2 * p + q:2 * p + q + 1, :] = jnp.sum(cs[p, :, q * 128:(q + 1) * 128], axis=0, keepdims=True)
    sums = []
    for dc, dy, dx in txt_offs:
        sums.append(net.send(csum, cbuf.at[dc * 8 + dy * 4 + (4 - dx) % 4], g.txt_peer(dc, dy, dx)))
    for i in range(8 * n // 128):
        rsum[i:i + 1, :] = jnp.sum(rs[i * 128:(i + 1) * 128, :].T, axis=0, keepdims=True)
    for dy, dz in img_offs:
        sums.append(net.send(rsum, rbuf.at[dy * 4 + (4 - dz) % 4], g.img_peer(dy, dz)))
    got_img(6)
    pos = jnp.sum(img_ref[...].astype(F32) * txt_ref[...].astype(F32), axis=1, keepdims=True) * scale
    rlsum = [jnp.sum(rl[i * 128:(i + 1) * 128, :].T, axis=0, keepdims=True) for i in range(8 * n // 128)]
    clsum = [jnp.sum(cl[p, :, q * 128:(q + 1) * 128], axis=0, keepdims=True) for p in range(16) for q in range(n // 128)]
    for copy in sums:
        copy.wait_recv()
    loss = jnp.zeros((2, 128), F32)
    dt = jnp.zeros((1, 128), F32)
    for dy, dz in [(0, 0)] + img_offs:
        k = 2 * POS[dy * 4 + dz]
        tot = rsum[k:k + 2, :]
        for oy, oz in img_offs:
            q = 2 * POS[(dy ^ oy) * 4 + (dz - oz) % 4]
            tot += rbuf[oy * 4 + oz, q:q + 2, :]
        a = 1.0 / tot
        a_ref[k:k + 2, :] = a * inv
        dt += a[0:1] * rlsum[k] + a[1:2] * rlsum[k + 1]
        if k == 0:
            loss += jnp.log(tot)
    for dc, dy, dx in [(0, 0, 0)] + txt_offs:
        k = 2 * (dc * 8 + POS[dy * 4 + dx])
        tot = csum[k:k + 2, :]
        for oc, oy, ox in txt_offs:
            q = 2 * ((dc ^ oc) * 8 + POS[(dy ^ oy) * 4 + (dx - ox) % 4])
            tot += cbuf[oc * 8 + oy * 4 + ox, q:q + 2, :]
        b = 1.0 / tot
        b_ref[k:k + 2, :] = b * inv
        dt += b[0:1] * clsum[k] + b[1:2] * clsum[k + 1]
        if k == 0:
            loss += jnp.log(tot)
    diag = jnp.sum(pos, axis=0, keepdims=True)
    first_lane = lax.broadcasted_iota(jnp.int32, (1, 128), 1) == 0
    diag = jnp.where(first_lane, 2.0 * diag, 0.0)
    part_ref[...] = jnp.zeros_like(part_ref)
    part_ref[0:1, :] = (jnp.sum(loss, axis=0, keepdims=True) - diag) * inv
    part_ref[1:2, :] = (dt - diag) * inv
    for buf in (0, 1):
        for slot in range(DEEP):
            store(0, 0, buf, slot).wait()
    for copy in saves:
        copy.wait()
    net.finish()


def forward(inv, scale, img, txt):
    n, d = img.shape
    vmem = pl.BlockSpec(memory_space=pltpu.VMEM)
    hbm = pl.BlockSpec(memory_space=pl.ANY)
    dma = pltpu.SemaphoreType.DMA
    return pl.pallas_call(
        functools.partial(forward_kernel, inv),
        out_shape=[jax.ShapeDtypeStruct((8, 2, 8, n, n), F32), jax.ShapeDtypeStruct((d, 8 * n), BF16),
                   jax.ShapeDtypeStruct((16 * n, d), BF16), jax.ShapeDtypeStruct((16, 128), F32),
                   jax.ShapeDtypeStruct((32, 128), F32), jax.ShapeDtypeStruct((8, 128), F32)],
        in_specs=[pl.BlockSpec(memory_space=pltpu.SMEM), vmem, vmem],
        out_specs=[hbm, hbm, hbm, vmem, vmem, vmem],
        scratch_shapes=[pltpu.VMEM((8, n, d), BF16), pltpu.VMEM((16, n, d), BF16), pltpu.VMEM((8, d, n), BF16),
                        pltpu.VMEM((2, n, n), F32), pltpu.VMEM((2, n, n), F32), pltpu.VMEM((DEEP, 2, n, n), F32),
                        pltpu.VMEM((DEEP, 2, n, n), F32), pltpu.VMEM((8 * n, 128), F32), pltpu.VMEM((8 * n, 128), F32),
                        pltpu.VMEM((16, 8, n), F32), pltpu.VMEM((16, 8, n), F32), pltpu.VMEM((16, 128), F32),
                        pltpu.VMEM((32, 128), F32), pltpu.VMEM((8, 16, 128), F32), pltpu.VMEM((16, 32, 128), F32),
                        dma((2 * DEEP,)), dma((16,)), dma((8,)), dma((2,)), dma((N_FORWARD,)), dma((N_FORWARD,))],
        compiler_params=pltpu.CompilerParams(collective_id=0, has_side_effects=True, vmem_limit_bytes=VMEM_LIMIT),
        name="forward_sums")(scale, img, txt)


ICUT = 144
TCUT = 432
ORDER = (6, 5, 7, 2, 1, 4, 3, 0)
N_REDUCE = 2 * (4 + 18 + 1) + 22


class Ring:
    def __init__(self, net, acc, buf, cut, plus, minus, pair):
        self.net, self.acc, self.buf = net, acc, buf
        self.cut, self.rows = cut, acc.shape[1]
        self.plus, self.minus, self.pair = plus, minus, pair
        self.early, self.streams = {}, {}

    def pair_send(self, d):
        at = pl.ds(self.cut, self.rows - self.cut)
        self.early[d] = self.net.send((self.acc, (POS[4 + d], at)), (self.buf, (4 + d, at)), self.pair)

    def pair_add(self, d):
        self.early[d].wait_recv()
        self.acc[POS[d], self.cut:] += self.buf[4 + d, self.cut:]

    def where(self, name):
        if name == 2:
            return 0, self.cut, (self.rows - self.cut) // 2
        return 4 * name, 0, self.cut // 2

    def send(self, name, key, slot, half, to_slot, peer):
        _, lo, h = self.where(name)
        at = pl.ds(lo + half * h, h)
        self.streams[name, key] = self.net.send((self.acc, (POS[slot], at)), (self.buf, (to_slot, at)), peer)

    def far(self, name):
        b, _, _ = self.where(name)
        self.send(name, "a+", b + 2, 0, b + 2, self.plus)
        self.send(name, "a-", b + 2, 1, b + 2, self.minus)

    def plain_plus(self, name):
        b, _, _ = self.where(name)
        self.send(name, "b+1", b + 1, 1, b + 3, self.plus)

    def plain_minus(self, name):
        b, _, _ = self.where(name)
        self.send(name, "b-0", b + 3, 0, b + 1, self.minus)

    def mid(self, name):
        b, lo, h = self.where(name)
        self.streams[name, "a+"].wait_recv()
        self.acc[POS[b + 1], lo:lo + h] += self.buf[b + 2, lo:lo + h]
        self.send(name, "b+0", b + 1, 0, b + 3, self.plus)
        self.streams[name, "a-"].wait_recv()
        self.acc[POS[b + 3], lo + h:lo + 2 * h] += self.buf[b + 2, lo + h:lo + 2 * h]
        self.send(name, "b-1", b + 3, 1, b + 1, self.minus)

    def end(self, name):
        b, lo, h = self.where(name)
        for key in ("b+1", "b-0", "b+0", "b-1"):
            self.streams[name, key].wait_recv()
        self.acc[POS[b], lo:lo + 2 * h] += self.buf[b + 1, lo:lo + 2 * h] + self.buf[b + 3, lo:lo + 2 * h]

    def pair_last(self):
        at = pl.ds(0, self.cut)
        self.late = self.net.send((self.acc, (POS[4], at)), (self.buf, (0, at)), self.pair)

    def pair_end(self):
        self.late.wait_recv()
        self.acc[0, 0:self.cut] += self.buf[0, 0:self.cut]

    def ready(self, step):
        if step == 0:
            self.pair_send(2)
            self.far(1)
        elif step == 1:
            self.pair_send(1)
            self.plain_plus(1)
        elif step == 2:
            self.pair_send(3)
            self.plain_minus(1)
            self.mid(1)
        elif step == 3:
            self.far(0)
            self.pair_add(2)
            self.far(2)
        elif step == 4:
            self.plain_plus(0)
            self.pair_add(1)
            self.plain_plus(2)
        elif step == 5:
            self.pair_send(0)
            self.end(1)
            self.pair_last()
        elif step == 6:
            self.plain_minus(0)
            self.pair_add(3)
            self.plain_minus(2)
            self.mid(0)

    def close(self):
        self.pair_add(0)
        self.end(0)
        self.pair_end()
        self.end(2)


def grads_kernel(inv, imgt_hbm, txt_hbm, e_hbm, a_ref, b_ref, part_ref, img_out, txt_out, part_out,
                 imgt, txt, erow, ecol, gb_row, gb_near, gb_far, arow, stage, iacc, tacc, ibuf, tbuf, dbuf, pa, pb,
                 psum, local_sems, e_sems, send_sems, recv_sems, cross_send, cross_recv):
    g = Grid()
    n = iacc.shape[1]
    m = imgt.shape[1]
    img_offs = [(dy, dz) for dy in (0, 1) for dz in range(4) if (dy, dz) != (0, 0)]
    txt_offs = [(dc, dy, dx) for dc in (0, 1) for dy in (0, 1) for dx in range(4) if (dc, dy, dx) != (0, 0, 0)]
    last = len(ORDER) - 1

    def row_load(p):
        return pltpu.make_async_copy(e_hbm.at[p], erow, e_sems.at[2])

    def col_load(p, side):
        return pltpu.make_async_copy(e_hbm.at[:, side, p], ecol.at[side], e_sems.at[side])

    load_imgt = pltpu.make_async_copy(imgt_hbm, imgt, local_sems.at[0])
    load_txt = pltpu.make_async_copy(txt_hbm, txt, local_sems.at[1])
    col_load(last, 1).start()
    load_imgt.start()
    row_load(last).start()
    load_txt.start()
    col_load(last, 0).start()
    for i in range(m // 128):
        arow[i * 128:(i + 1) * 128, :] = jnp.broadcast_to(a_ref[i:i + 1, :], (128, 128)).T
    greet([g.img_peer(*o) for o in img_offs] + [g.txt_peer(*o) for o in txt_offs])
    net = Net(send_sems, recv_sems)
    core = g.txt_peer(1, 0, 0)
    img_peers = [g.img_peer(*o) for o in img_offs]
    txt_peers = [g.txt_peer(*o) for o in txt_offs]
    ia = g.z * 2 + g.y % 2
    ib = (g.x * 2 + g.y // 2) * 2 + g.c
    scal_a = [net.send(part_ref, (pa, ia), peer) for peer in img_peers]
    scal_b = []
    pa[ia] = part_ref[...]
    img = Ring(net, iacc, ibuf, ICUT, g.img_peer(0, 1), g.img_peer(0, 3), g.img_peer(1, 0))
    txr = Ring(net, tacc, tbuf, TCUT, g.txt_peer(0, 0, 1), g.txt_peer(0, 0, 3), g.txt_peer(0, 1, 0))

    def minus_diag(grad, q, p):
        r = lax.broadcasted_iota(jnp.int32, (n, 128), 0)
        c = lax.broadcasted_iota(jnp.int32, (n, 128), 1) + q * 128
        return grad - jnp.where(r == c, jnp.where(p == 0, 2.0 * inv, 0.0), 0.0)

    def col_grad(p, side, to):
        for t in range(m // n):
            a = arow[t * n:(t + 1) * n, :]
            for q in range(n // 128):
                lanes = slice(q * 128, (q + 1) * 128)
                v = ecol[side, t, :, lanes] * (a + b_ref[pl.ds(2 * (p + 8 * side) + q, 1), :])
                if side == 0 and t == 0:
                    v = minus_diag(v, q, p)
                to[t * n:(t + 1) * n, lanes] = v.astype(BF16)

    def row_grad(p):
        a = arow[pl.ds(pl.multiple_of(p * n, n), n), :]
        for t in range(16):
            for q in range(n // 128):
                lanes = slice(q * 128, (q + 1) * 128)
                v = erow[t // 8, t % 8, :, lanes] * (a + b_ref[2 * t + q:2 * t + q + 1, :])
                if t == 0:
                    v = minus_diag(v, q, p)
                gb_row[:, t * n + q * 128:t * n + (q + 1) * 128] = v.astype(BF16)

    def crossing(s):
        return pltpu.make_async_remote_copy(
            src_ref=stage.at[s % 2], dst_ref=dbuf.at[last - s], send_sem=cross_send.at[s], recv_sem=cross_recv.at[s],
            device_id=core, device_id_type=MESH)

    col_load(last, 1).wait()
    col_grad(last, 1, gb_far)
    load_imgt.wait()
    load_txt.wait()

    def step(s, carry):
        p = last - s
        row_load(p).wait()

        @pl.when(s >= 2)
        def _():
            crossing(s - 2).wait_send()

        stage[s % 2] = jnp.dot(imgt[...], gb_far[...], preferred_element_type=F32)
        row_grad(p)
        crossing(s).start()

        @pl.when(s < last)
        def _():
            row_load(p - 1).start()
            col_load(p - 1, 1).start()

        col_load(p, 0).wait()
        iacc[p] = jnp.dot(gb_row[...], txt[...], preferred_element_type=F32)
        col_grad(p, 0, gb_near)

        @pl.when(s < last)
        def _():
            col_load(p - 1, 0).start()
            col_load(p - 1, 1).wait()

        for i in range(last + 1):
            @pl.when(s == i)
            def _():
                img.ready(i)

        tacc[p] = jnp.dot(imgt[...], gb_near[...], preferred_element_type=F32)
        col_grad(p - 1 + (s // last), 1, gb_far)
        crossing(s).wait_recv()
        tacc[p] += dbuf[p]
        for i in range(last + 1):
            @pl.when(s == i)
            def _():
                txr.ready(i)
                if i == 1:
                    for copy in scal_a:
                        copy.wait_recv()
                    total = pa[0]
                    for q in range(1, 8):
                        total += pa[q]
                    psum[...] = total
                    scal_b.extend(net.send(psum, (pb, ib), peer) for peer in txt_peers)
                    pb[ib] = total
        return carry

    lax.fori_loop(0, last + 1, step, 0)
    for r in (img, txr):
        r.mid(2)
    for copy in scal_b:
        copy.wait_recv()
    total = pb[0]
    for k in range(1, 16):
        total += pb[k]
    part_out[...] = total
    for r in (img, txr):
        r.close()
    img_out[...] = iacc[0]
    txt_out[...] = tacc[0]
    crossing(last - 1).wait_send()
    crossing(last).wait_send()
    net.finish()


def grads(inv, imgt, txt_all, e, a, b, part):
    d, m = imgt.shape
    nt = txt_all.shape[0]
    n = m // 8
    vmem = pl.BlockSpec(memory_space=pltpu.VMEM)
    hbm = pl.BlockSpec(memory_space=pl.ANY)
    dma = pltpu.SemaphoreType.DMA
    return pl.pallas_call(
        functools.partial(grads_kernel, inv),
        out_shape=[jax.ShapeDtypeStruct((n, d), F32), jax.ShapeDtypeStruct((d, n), F32),
                   jax.ShapeDtypeStruct((8, 128), F32)],
        in_specs=[hbm, hbm, hbm, vmem, vmem, vmem],
        out_specs=[vmem] * 3,
        scratch_shapes=[pltpu.VMEM((d, m), BF16), pltpu.VMEM((nt, d), BF16), pltpu.VMEM((2, 8, n, n), F32),
                        pltpu.VMEM((2, 8, n, n), F32), pltpu.VMEM((n, nt), BF16), pltpu.VMEM((m, n), BF16),
                        pltpu.VMEM((m, n), BF16), pltpu.VMEM((m, 128), F32), pltpu.VMEM((2, d, n), F32),
                        pltpu.VMEM((8, n, d), F32), pltpu.VMEM((8, d, n), F32), pltpu.VMEM((8, n, d), F32),
                        pltpu.VMEM((8, d, n), F32), pltpu.VMEM((8, d, n), F32), pltpu.VMEM((8, 8, 128), F32),
                        pltpu.VMEM((16, 8, 128), F32), pltpu.VMEM((8, 128), F32), dma((2,)), dma((3,)),
                        dma((N_REDUCE,)), dma((N_REDUCE,)), dma((8,)), dma((8,))],
        compiler_params=pltpu.CompilerParams(collective_id=2, has_side_effects=True, vmem_limit_bytes=VMEM_LIMIT),
        cost_estimate=pl.CostEstimate(flops=4 * m * nt * d, bytes_accessed=8 * m * nt, transcendentals=0),
        name="grads_reduce")(imgt, txt_all, e, a, b, part)


def solution(mesh):
    batch_spec = P(("row", "col"), None)
    shards = mesh.shape["row"] * mesh.shape["col"]

    def local_tile(img_loc, txt_loc, log_scale):
        n, d = img_loc.shape
        inv = 1.0 / (2 * n * shards)
        scale = jnp.exp(log_scale)
        e, imgt, txt_all, a, b, part = forward(inv, scale.reshape(1), img_loc, txt_loc)
        img_sum, txt_sum, tot = grads(inv, imgt, txt_all, e, a, b, part)
        d_img = (scale * img_sum).astype(BF16)
        d_txt = (scale * txt_sum).T.astype(BF16)
        tot = jnp.sum(tot[0:2], axis=1)
        return tot[0], d_img, d_txt, tot[1]

    return jax.shard_map(local_tile, mesh=mesh, in_specs=(batch_spec, batch_spec, P()),
                         out_specs=(P(), batch_spec, batch_spec, P()), check_vma=False)
```

```python
import functools

import jax
import jax.numpy as jnp
from jax import lax
from jax.experimental import pallas as pl
from jax.experimental.pallas import tpu as pltpu
from jax.sharding import PartitionSpec as P

MESH = pl.DeviceIdType.MESH
F32 = jnp.float32
BF16 = jnp.bfloat16
VMEM_LIMIT = 67_043_328


class Grid:
    def __init__(self):
        row = lax.axis_index("row")
        self.c = lax.axis_index("col")
        self.z = row // 16
        self.y = (row // 4) % 4
        self.x = row % 4

    def dev(self, z, y, x, c):
        return {"row": (z * 4 + y) * 4 + x, "col": c}

    def y_a(self):
        return self.y + 1 - 2 * (self.y % 2)

    def y_b(self):
        return 3 - self.y

    def img_peer(self, dy, dz):
        y = self.y_a() if dy else self.y
        return self.dev((self.z + dz) % 4, y, self.x, self.c)

    def txt_peer(self, dc, dy, dx):
        y = self.y_b() if dy else self.y
        c = 1 - self.c if dc else self.c
        return self.dev(self.z, y, (self.x + dx) % 4, c)


def view(ref):
    return ref[0].at[ref[1]] if isinstance(ref, tuple) else ref


class Copy:
    def __init__(self, net, i, src, dst, peer):
        self.net, self.i, self.src, self.dst, self.peer = net, i, src, dst, peer

    def make(self):
        return pltpu.make_async_remote_copy(
            src_ref=view(self.src), dst_ref=view(self.dst), send_sem=self.net.send_sems.at[self.i],
            recv_sem=self.net.recv_sems.at[self.i], device_id=self.peer, device_id_type=MESH)

    def wait_recv(self):
        self.make().wait_recv()

    def wait_send(self):
        self.make().wait_send()


class Net:
    def __init__(self, send_sems, recv_sems):
        self.send_sems, self.recv_sems, self.copies = send_sems, recv_sems, []

    def send(self, src, dst, peer):
        copy = Copy(self, len(self.copies), src, dst, peer)
        copy.make().start()
        self.copies.append(copy)
        return copy

    def finish(self, skip=()):
        for copy in self.copies:
            if not any(copy is other for other in skip):
                copy.wait_send()


def greet(peers):
    barrier = pltpu.get_barrier_semaphore()
    for peer in peers:
        pl.semaphore_signal(barrier, inc=1, device_id=peer, device_id_type=MESH)
    pl.semaphore_wait(barrier, len(peers))


def neighbours(g):
    return [g.img_peer(0, 1), g.img_peer(0, 3), g.img_peer(1, 0), g.txt_peer(0, 0, 1), g.txt_peer(0, 0, 3),
            g.txt_peer(0, 1, 0), g.txt_peer(1, 0, 0)]


POS = {0: 0, 3: 1, 4: 2, 1: 3, 2: 4, 7: 5, 5: 6, 6: 7}
DEEP = 4
N_FORWARD = 2 * 18 + 9 + 22


class Gather:
    def __init__(self, net, own, dst, plus, minus, pair):
        self.net, self.own, self.dst = net, own, dst
        self.n = own.shape[0]
        self.plus, self.minus, self.pair = plus, minus, pair
        self.got = {}

    def half(self, k, side):
        h = self.n // 2
        return self.dst.at[POS[k], pl.ds(side * h, h)]

    def send(self, key, src, k, side, peer):
        self.got[key, side] = self.net.send(src, self.half(k, side), peer)

    def first(self):
        h = self.n // 2
        own = [self.own.at[pl.ds(side * h, h)] for side in (0, 1)]
        for side in (0, 1):
            self.send("p0", own[side], 3, side, self.plus)
            self.send("m0", own[1 - side], 1, 1 - side, self.minus)
            self.send("y0", own[side], 4, side, self.pair)

    def wait(self, *keys):
        for key in keys:
            self.got[key].wait_recv()

    def far(self, dy):
        self.wait(("p%d" % dy, 0))
        self.send("f%d" % dy, self.half(4 * dy + 3, 0), 4 * dy + 2, 0, self.plus)
        self.wait(("m%d" % dy, 1))
        self.send("f%d" % dy, self.half(4 * dy + 1, 1), 4 * dy + 2, 1, self.minus)

    def second(self):
        self.wait(("y0", 0), ("y0", 1))
        for side in (0, 1):
            self.send("p1", self.half(4, side), 7, side, self.plus)
            self.send("m1", self.half(4, 1 - side), 5, 1 - side, self.minus)


def forward_kernel(inv, scale_ref, img_ref, txt_ref, e_out, imgt_out, txt_out, a_ref, b_ref, part_ref,
                   img_all, txt_all, imgt, d0, d1, s0, s1, rs, rl, cs, cl, rsum, csum, rbuf, cbuf,
                   e_sems, t_sems, i_sems, own_sems, send_sems, recv_sems):
    g = Grid()
    n, d = img_ref.shape
    scale = scale_ref[0]
    img_offs = [(dy, dz) for dy in (0, 1) for dz in range(4) if (dy, dz) != (0, 0)]
    txt_offs = [(dc, dy, dx) for dc in (0, 1) for dy in (0, 1) for dx in range(4) if (dc, dy, dx) != (0, 0, 0)]
    own = [pltpu.make_async_copy(img_ref, img_all.at[0], own_sems.at[0]),
           pltpu.make_async_copy(txt_ref, txt_all.at[0], own_sems.at[1])]
    for copy in own:
        copy.start()
    greet([g.img_peer(*o) for o in img_offs] + [g.txt_peer(*o) for o in txt_offs])
    net = Net(send_sems, recv_sems)
    core = g.txt_peer(1, 0, 0)
    img = Gather(net, img_ref, img_all, g.img_peer(0, 1), g.img_peer(0, 3), g.img_peer(1, 0))
    txt = Gather(net, txt_ref, txt_all, g.txt_peer(0, 0, 1), g.txt_peer(0, 0, 3), g.txt_peer(0, 1, 0))
    img.first()
    txt.first()
    cross = {0: net.send(txt_ref, txt_all.at[8], core)}
    saves = []

    def save_txt(p):
        copy = pltpu.make_async_copy(txt_all.at[p], txt_out.at[pl.ds(p * n, n)], t_sems.at[p])
        copy.start()
        saves.append(copy)

    def got_txt(*slots):
        for k in slots:
            p = POS[k]
            cross[p] = net.send(txt_all.at[p], txt_all.at[8 + p], core)
            save_txt(p)

    def got_cross(*slots):
        for k in slots:
            cross[POS[k]].wait_recv()
            save_txt(8 + POS[k])

    def got_img(*slots):
        for k in slots:
            p = POS[k]
            imgt[p] = img_all[p].T
            copy = pltpu.make_async_copy(imgt.at[p], imgt_out.at[:, pl.ds(p * n, n)], i_sems.at[p])
            copy.start()
            saves.append(copy)

    dots, stage = (d0, d1), (s0, s1)

    def dot(i, k, buf):
        lhs = img_all[i]
        for side in (0, 1):
            dots[buf][side] = lax.dot_general(lhs, txt_all[8 * side + k], (((1,), (1,)), ((), ())),
                                              preferred_element_type=F32)

    def store(i, k, buf, slot):
        return pltpu.make_async_copy(stage[buf].at[slot], e_out.at[i, :, k], e_sems.at[buf * DEEP + slot])

    def free(buf, use):
        if isinstance(use, int):
            if use >= DEEP:
                store(0, 0, buf, use % DEEP).wait()
        else:
            @pl.when(use >= DEEP)
            def _():
                store(0, 0, buf, use % DEEP).wait()

    def finish_unit(i, k, buf, use):
        slot = use % DEEP
        for blk in range(n // 32):
            lo = blk * 32
            rows = pl.ds(i * n + lo, 32) if isinstance(i, int) else pl.ds(pl.multiple_of(i * n + lo, 32), 32)
            racc, lacc = rs[rows, :], rl[rows, :]
            for side in (0, 1):
                logits = scale * dots[buf][side, lo:lo + 32, :]
                e = jnp.exp(logits)
                el = e * logits
                stage[buf][slot, side, lo:lo + 32, :] = e
                for q in range(n // 128):
                    racc += e[:, q * 128:(q + 1) * 128]
                    lacc += el[:, q * 128:(q + 1) * 128]
                cs[8 * side + k] += jnp.sum(e.reshape(4, 8, n), axis=0)
                cl[8 * side + k] += jnp.sum(el.reshape(4, 8, n), axis=0)
            rs[rows, :] = racc
            rl[rows, :] = lacc
        store(i, k, buf, slot).start()

    state = {"buf": 0, "unit": (0, 0), "uses": [0, 0]}

    def last_unit():
        buf = state["buf"]
        free(buf, state["uses"][buf])
        finish_unit(*state["unit"], buf, state["uses"][buf])
        state["uses"][buf] += 1

    def one(i, k):
        buf = state["buf"]
        free(buf, state["uses"][buf])
        dot(i, k, 1 - buf)
        finish_unit(*state["unit"], buf, state["uses"][buf])
        state["uses"][buf] += 1
        state["buf"], state["unit"] = 1 - buf, (i, k)

    def run(i0, k0, width, start, count):
        buf = state["buf"]
        uses = list(state["uses"])

        def unit(u):
            return i0 + u // width, k0 + u % width

        def body(it, carry):
            u = start + 2 * it
            free(buf, uses[buf] + it)
            free(1 - buf, uses[1 - buf] + it)
            dot(*unit(u), 1 - buf)
            finish_unit(carry[0], carry[1], buf, uses[buf] + it)
            dot(*unit(u + 1), buf)
            finish_unit(*unit(u), 1 - buf, uses[1 - buf] + it)
            return unit(u + 1)

        last = tuple(jnp.int32(v) for v in state["unit"])
        state["unit"] = lax.fori_loop(0, count // 2, body, last)
        state["uses"] = [v + count // 2 for v in uses]
        if count % 2:
            one(*unit(jnp.int32(start + count - 1)))

    rs[...] = jnp.zeros_like(rs)
    rl[...] = jnp.zeros_like(rl)
    cs[...] = jnp.zeros_like(cs)
    cl[...] = jnp.zeros_like(cl)
    for copy in own:
        copy.wait()
    save_txt(0)
    got_img(0)
    img.far(0)
    txt.far(0)
    img.second()
    txt.second()
    got_txt(4)
    txt.wait(("p0", 1), ("m0", 0))
    got_txt(3, 1)
    got_cross(0)
    dot(0, 0, 0)
    img.wait(("p0", 1), ("m0", 0))
    got_cross(4, 3, 1)
    run(0, 0, 4, 1, 15)
    got_img(4, 3, 1)
    for r in (txt, img):
        r.wait(("f0", 0), ("f0", 1))
    got_txt(2)
    run(4, 0, 4, 0, 4)
    got_cross(2)
    run(0, 4, 1, 0, 5)
    got_img(2)
    for r in (txt, img):
        r.far(1)
    txt.wait(("p1", 1), ("m1", 0))
    got_txt(7, 5)
    img.wait(("p1", 1), ("m1", 0))
    run(5, 0, 5, 0, 10)
    got_cross(7, 5)
    run(0, 5, 2, 0, 6)
    txt.wait(("f1", 0), ("f1", 1))
    got_txt(6)
    run(3, 5, 2, 0, 8)
    got_img(7, 5)
    img.wait(("f1", 0), ("f1", 1))
    got_cross(6)
    run(7, 0, 8, 0, 8)
    run(0, 7, 1, 0, 7)
    last_unit()

    for p in range(16):
        for q in range(n // 128):
            csum[2 * p + q:2 * p + q + 1, :] = jnp.sum(cs[p, :, q * 128:(q + 1) * 128], axis=0, keepdims=True)
    sums = []
    for dc, dy, dx in txt_offs:
        sums.append(net.send(csum, cbuf.at[dc * 8 + dy * 4 + (4 - dx) % 4], g.txt_peer(dc, dy, dx)))
    for i in range(8 * n // 128):
        rsum[i:i + 1, :] = jnp.sum(rs[i * 128:(i + 1) * 128, :].T, axis=0, keepdims=True)
    for dy, dz in img_offs:
        sums.append(net.send(rsum, rbuf.at[dy * 4 + (4 - dz) % 4], g.img_peer(dy, dz)))
    got_img(6)
    pos = jnp.sum(img_ref[...].astype(F32) * txt_ref[...].astype(F32), axis=1, keepdims=True) * scale
    rlsum = [jnp.sum(rl[i * 128:(i + 1) * 128, :].T, axis=0, keepdims=True) for i in range(8 * n // 128)]
    clsum = [jnp.sum(cl[p, :, q * 128:(q + 1) * 128], axis=0, keepdims=True) for p in range(16) for q in range(n // 128)]
    for copy in sums:
        copy.wait_recv()
    loss = jnp.zeros((2, 128), F32)
    dt = jnp.zeros((1, 128), F32)
    for dy, dz in [(0, 0)] + img_offs:
        k = 2 * POS[dy * 4 + dz]
        tot = rsum[k:k + 2, :]
        for oy, oz in img_offs:
            q = 2 * POS[(dy ^ oy) * 4 + (dz - oz) % 4]
            tot += rbuf[oy * 4 + oz, q:q + 2, :]
        a = 1.0 / tot
        a_ref[k:k + 2, :] = a * inv
        dt += a[0:1] * rlsum[k] + a[1:2] * rlsum[k + 1]
        if k == 0:
            loss += jnp.log(tot)
    for dc, dy, dx in [(0, 0, 0)] + txt_offs:
        k = 2 * (dc * 8 + POS[dy * 4 + dx])
        tot = csum[k:k + 2, :]
        for oc, oy, ox in txt_offs:
            q = 2 * ((dc ^ oc) * 8 + POS[(dy ^ oy) * 4 + (dx - ox) % 4])
            tot += cbuf[oc * 8 + oy * 4 + ox, q:q + 2, :]
        b = 1.0 / tot
        b_ref[k:k + 2, :] = b * inv
        dt += b[0:1] * clsum[k] + b[1:2] * clsum[k + 1]
        if k == 0:
            loss += jnp.log(tot)
    diag = jnp.sum(pos, axis=0, keepdims=True)
    first_lane = lax.broadcasted_iota(jnp.int32, (1, 128), 1) == 0
    diag = jnp.where(first_lane, 2.0 * diag, 0.0)
    part_ref[...] = jnp.zeros_like(part_ref)
    part_ref[0:1, :] = (jnp.sum(loss, axis=0, keepdims=True) - diag) * inv
    part_ref[1:2, :] = (dt - diag) * inv
    for buf in (0, 1):
        for slot in range(DEEP):
            store(0, 0, buf, slot).wait()
    for copy in saves:
        copy.wait()
    net.finish()


def forward(inv, scale, img, txt):
    n, d = img.shape
    vmem = pl.BlockSpec(memory_space=pltpu.VMEM)
    hbm = pl.BlockSpec(memory_space=pl.ANY)
    dma = pltpu.SemaphoreType.DMA
    return pl.pallas_call(
        functools.partial(forward_kernel, inv),
        out_shape=[jax.ShapeDtypeStruct((8, 2, 8, n, n), F32), jax.ShapeDtypeStruct((d, 8 * n), BF16),
                   jax.ShapeDtypeStruct((16 * n, d), BF16), jax.ShapeDtypeStruct((16, 128), F32),
                   jax.ShapeDtypeStruct((32, 128), F32), jax.ShapeDtypeStruct((8, 128), F32)],
        in_specs=[pl.BlockSpec(memory_space=pltpu.SMEM), vmem, vmem],
        out_specs=[hbm, hbm, hbm, vmem, vmem, vmem],
        scratch_shapes=[pltpu.VMEM((8, n, d), BF16), pltpu.VMEM((16, n, d), BF16), pltpu.VMEM((8, d, n), BF16),
                        pltpu.VMEM((2, n, n), F32), pltpu.VMEM((2, n, n), F32), pltpu.VMEM((DEEP, 2, n, n), F32),
                        pltpu.VMEM((DEEP, 2, n, n), F32), pltpu.VMEM((8 * n, 128), F32), pltpu.VMEM((8 * n, 128), F32),
                        pltpu.VMEM((16, 8, n), F32), pltpu.VMEM((16, 8, n), F32), pltpu.VMEM((16, 128), F32),
                        pltpu.VMEM((32, 128), F32), pltpu.VMEM((8, 16, 128), F32), pltpu.VMEM((16, 32, 128), F32),
                        dma((2 * DEEP,)), dma((16,)), dma((8,)), dma((2,)), dma((N_FORWARD,)), dma((N_FORWARD,))],
        compiler_params=pltpu.CompilerParams(collective_id=0, has_side_effects=True, vmem_limit_bytes=VMEM_LIMIT),
        name="forward_sums")(scale, img, txt)


ICUT = 144
TCUT = 432
ORDER = (6, 5, 7, 2, 1, 4, 3, 0)
N_REDUCE = 8 + 2 * (4 + 18 + 1) + 22


class Ring:
    def __init__(self, net, acc, buf, cut, plus, minus, pair):
        self.net, self.acc, self.buf = net, acc, buf
        self.cut, self.rows = cut, acc.shape[1]
        self.plus, self.minus, self.pair = plus, minus, pair
        self.early, self.streams = {}, {}

    def pair_send(self, d):
        at = pl.ds(self.cut, self.rows - self.cut)
        self.early[d] = self.net.send((self.acc, (POS[4 + d], at)), (self.buf, (4 + d, at)), self.pair)

    def pair_add(self, d):
        self.early[d].wait_recv()
        self.acc[POS[d], self.cut:] += self.buf[4 + d, self.cut:]

    def where(self, name):
        if name == 2:
            return 0, self.cut, (self.rows - self.cut) // 2
        return 4 * name, 0, self.cut // 2

    def send(self, name, key, slot, half, to_slot, peer):
        _, lo, h = self.where(name)
        at = pl.ds(lo + half * h, h)
        self.streams[name, key] = self.net.send((self.acc, (POS[slot], at)), (self.buf, (to_slot, at)), peer)

    def far(self, name):
        b, _, _ = self.where(name)
        self.send(name, "a+", b + 2, 0, b + 2, self.plus)
        self.send(name, "a-", b + 2, 1, b + 2, self.minus)

    def plain_plus(self, name):
        b, _, _ = self.where(name)
        self.send(name, "b+1", b + 1, 1, b + 3, self.plus)

    def plain_minus(self, name):
        b, _, _ = self.where(name)
        self.send(name, "b-0", b + 3, 0, b + 1, self.minus)

    def mid(self, name):
        b, lo, h = self.where(name)
        self.streams[name, "a+"].wait_recv()
        self.acc[POS[b + 1], lo:lo + h] += self.buf[b + 2, lo:lo + h]
        self.send(name, "b+0", b + 1, 0, b + 3, self.plus)
        self.streams[name, "a-"].wait_recv()
        self.acc[POS[b + 3], lo + h:lo + 2 * h] += self.buf[b + 2, lo + h:lo + 2 * h]
        self.send(name, "b-1", b + 3, 1, b + 1, self.minus)

    def end(self, name):
        b, lo, h = self.where(name)
        for key in ("b+1", "b-0", "b+0", "b-1"):
            self.streams[name, key].wait_recv()
        self.acc[POS[b], lo:lo + 2 * h] += self.buf[b + 1, lo:lo + 2 * h] + self.buf[b + 3, lo:lo + 2 * h]

    def pair_last(self):
        at = pl.ds(0, self.cut)
        self.late = self.net.send((self.acc, (POS[4], at)), (self.buf, (0, at)), self.pair)

    def pair_end(self):
        self.late.wait_recv()
        self.acc[0, 0:self.cut] += self.buf[0, 0:self.cut]

    def ready(self, step):
        if step == 0:
            self.pair_send(2)
            self.far(1)
        elif step == 1:
            self.pair_send(1)
            self.plain_plus(1)
        elif step == 2:
            self.pair_send(3)
            self.plain_minus(1)
            self.mid(1)
        elif step == 3:
            self.far(0)
            self.pair_add(2)
            self.far(2)
        elif step == 4:
            self.plain_plus(0)
            self.pair_add(1)
            self.plain_plus(2)
        elif step == 5:
            self.pair_send(0)
            self.end(1)
            self.pair_last()
        elif step == 6:
            self.plain_minus(0)
            self.pair_add(3)
            self.plain_minus(2)
            self.mid(0)
            self.mid(2)

    def close(self):
        self.pair_add(0)
        self.end(0)
        self.pair_end()
        self.end(2)


KC = 512


def grads_kernel(inv, scale_ref, imgt_hbm, txt_hbm, e_hbm, a_ref, b_ref, part_ref, img_out, txt_out, part_out,
                 imgt, txt, erow, ecol, gb0, gb1, arow, stage, iacc, tacc, ibuf, tbuf, dbuf, pa, pb, psum,
                 local_sems, row_sems, col_sems, send_sems, recv_sems):
    g = Grid()
    n = iacc.shape[1]
    d = iacc.shape[2]
    m = imgt.shape[1]
    nt = txt.shape[0]
    img_offs = [(dy, dz) for dy in (0, 1) for dz in range(4) if (dy, dz) != (0, 0)]
    txt_offs = [(dc, dy, dx) for dc in (0, 1) for dy in (0, 1) for dx in range(4) if (dc, dy, dx) != (0, 0, 0)]

    def row_load(step):
        return pltpu.make_async_copy(e_hbm.at[POS[ORDER[step]]], erow.at[step % 2], row_sems.at[step % 2])

    def col_load(step, side):
        return pltpu.make_async_copy(e_hbm.at[:, side, POS[ORDER[step]]], ecol.at[side], col_sems.at[side])

    load_imgt = pltpu.make_async_copy(imgt_hbm, imgt, local_sems.at[0])
    load_txt = pltpu.make_async_copy(txt_hbm, txt, local_sems.at[1])
    cols = {}
    cols[0, 1] = col_load(0, 1)
    cols[0, 1].start()
    load_imgt.start()
    rows = {0: row_load(0)}
    rows[0].start()
    load_txt.start()
    cols[0, 0] = col_load(0, 0)
    cols[0, 0].start()
    for i in range(m // 128):
        arow[i * 128:(i + 1) * 128, :] = jnp.broadcast_to(a_ref[i:i + 1, :], (128, 128)).T
    greet([g.img_peer(*o) for o in img_offs] + [g.txt_peer(*o) for o in txt_offs])
    net = Net(send_sems, recv_sems)
    core = g.txt_peer(1, 0, 0)
    ia = g.z * 2 + g.y % 2
    ib = (g.x * 2 + g.y // 2) * 2 + g.c
    scal_a = [net.send(part_ref, pa.at[ia], g.img_peer(*o)) for o in img_offs]
    pa[ia] = part_ref[...]
    img = Ring(net, iacc, ibuf, ICUT, g.img_peer(0, 1), g.img_peer(0, 3), g.img_peer(1, 0))
    txr = Ring(net, tacc, tbuf, TCUT, g.txt_peer(0, 0, 1), g.txt_peer(0, 0, 3), g.txt_peer(0, 1, 0))

    def minus_diag(grad, q):
        r = lax.broadcasted_iota(jnp.int32, (n, 128), 0)
        c = lax.broadcasted_iota(jnp.int32, (n, 128), 1) + q * 128
        return grad - jnp.where(r == c, 2.0 * inv, 0.0)

    def add(out_ref, part, may_start, it):
        old = out_ref[...]
        out_ref[...] = part + (jnp.where(it > 0, old, 0.0) if may_start else old)

    def col_slot(p, e_ref, out_ref):
        b = [b_ref[2 * p + q:2 * p + q + 1, :] for q in range(n // 128)]
        tiles = KC // n
        count = m // KC

        def grad(i, to, diag=False):
            for t in range(tiles):
                for q in range(n // 128):
                    lanes = slice(q * 128, (q + 1) * 128)
                    a = arow[pl.ds(pl.multiple_of(i * KC + t * n, n), n), :]
                    v = e_ref[i * tiles + t, :, lanes] * (a + b[q])
                    if diag and t == 0:
                        v = minus_diag(v, q)
                    to[t * n:(t + 1) * n, lanes] = v.astype(BF16)

        grad(0, gb0[0], diag=p == 0)
        def body(it, carry):
            for half, (now, later) in enumerate(((gb0[0], gb0[1]), (gb0[1], gb0[0]))):
                i = 2 * it + half
                at = pl.ds(pl.multiple_of(i * KC, KC), KC)
                add(out_ref, jnp.dot(imgt[:, at], now[...], preferred_element_type=F32), half == 0, it)
                grad((i + 1) % count, later)
            return carry

        lax.fori_loop(0, count // 2, body, 0)

    def row_slot(p, e_ref, out_ref):
        tiles = KC // n
        count = nt // KC

        def grad(i, to, diag=False):
            for t in range(tiles):
                tile = i * tiles + t
                for q in range(n // 128):
                    lanes = slice(q * 128, (q + 1) * 128)
                    v = (e_ref[tile // 8, tile % 8, :, lanes]
                         * (arow[p * n:(p + 1) * n, :] + b_ref[pl.ds(2 * tile + q, 1), :]))
                    if diag and t == 0:
                        v = minus_diag(v, q)
                    to[:, t * n + q * 128:t * n + (q + 1) * 128] = v.astype(BF16)

        grad(0, gb1[0], diag=p == 0)
        def body(it, carry):
            for half, (now, later) in enumerate(((gb1[0], gb1[1]), (gb1[1], gb1[0]))):
                i = 2 * it + half
                at = pl.ds(pl.multiple_of(i * KC, KC), KC)
                add(out_ref, jnp.dot(now[...], txt[at, :], preferred_element_type=F32), half == 0, it)
                grad((i + 1) % count, later)
            return carry

        lax.fori_loop(0, count // 2, body, 0)

    cross = {}
    for step, k in enumerate(ORDER):
        cols[step, 1].wait()
        if step == 0:
            load_imgt.wait()
        if step >= 2:
            cross[ORDER[step - 2]].wait_send()
        col_slot(8 + POS[k], ecol.at[1], stage.at[step % 2])
        cross[k] = net.send(stage.at[step % 2], dbuf.at[k], core)
        if step + 1 < len(ORDER):
            cols[step + 1, 1] = col_load(step + 1, 1)
            cols[step + 1, 1].start()
            rows[step + 1] = row_load(step + 1)
            rows[step + 1].start()
        rows[step].wait()
        if step == 0:
            load_txt.wait()
        row_slot(POS[k], erow.at[step % 2], iacc.at[POS[k]])
        img.ready(step)
        cols[step, 0].wait()
        col_slot(POS[k], ecol.at[0], tacc.at[POS[k]])
        if step + 1 < len(ORDER):
            cols[step + 1, 0] = col_load(step + 1, 0)
            cols[step + 1, 0].start()
        cross[k].wait_recv()
        tacc[POS[k]] += dbuf[k]
        txr.ready(step)
        if step == 1:
            for copy in scal_a:
                copy.wait_recv()
            total = pa[0]
            for q in range(1, 8):
                total += pa[q]
            psum[...] = total
            scal_b = [net.send(psum, pb.at[ib], g.txt_peer(*o)) for o in txt_offs]
            pb[ib] = total
    for copy in scal_b:
        copy.wait_recv()
    total = pb[0]
    for k in range(1, 16):
        total += pb[k]
    part_out[...] = total
    for r in (img, txr):
        r.close()
    scale = scale_ref[0]
    img_out[...] = (scale * iacc[0]).astype(BF16)
    txt_out[...] = (scale * tacc[0]).T.astype(BF16)
    net.finish(skip=[cross[k] for k in ORDER[:-2]])


def grads(inv, scale, imgt, txt_all, e, a, b, part):
    d, m = imgt.shape
    nt = txt_all.shape[0]
    n = m // 8
    vmem = pl.BlockSpec(memory_space=pltpu.VMEM)
    hbm = pl.BlockSpec(memory_space=pl.ANY)
    dma = pltpu.SemaphoreType.DMA
    return pl.pallas_call(
        functools.partial(grads_kernel, inv),
        out_shape=[jax.ShapeDtypeStruct((n, d), BF16), jax.ShapeDtypeStruct((n, d), BF16),
                   jax.ShapeDtypeStruct((8, 128), F32)],
        in_specs=[pl.BlockSpec(memory_space=pltpu.SMEM), hbm, hbm, hbm, vmem, vmem, vmem],
        out_specs=[vmem] * 3,
        scratch_shapes=[pltpu.VMEM((d, m), BF16), pltpu.VMEM((nt, d), BF16), pltpu.VMEM((2, 2, 8, n, n), F32),
                        pltpu.VMEM((2, 8, n, n), F32), [pltpu.VMEM((KC, n), BF16)] * 2, [pltpu.VMEM((n, KC), BF16)] * 2,
                        pltpu.VMEM((m, 128), F32), pltpu.VMEM((2, d, n), F32), pltpu.VMEM((8, n, d), F32),
                        pltpu.VMEM((8, d, n), F32), pltpu.VMEM((8, n, d), F32), pltpu.VMEM((8, d, n), F32),
                        pltpu.VMEM((8, d, n), F32), pltpu.VMEM((8, 8, 128), F32), pltpu.VMEM((16, 8, 128), F32),
                        pltpu.VMEM((8, 128), F32), dma((2,)), dma((2,)), dma((2,)), dma((N_REDUCE,)),
                        dma((N_REDUCE,))],
        compiler_params=pltpu.CompilerParams(collective_id=2, has_side_effects=True, vmem_limit_bytes=VMEM_LIMIT),
        cost_estimate=pl.CostEstimate(flops=4 * m * nt * d, bytes_accessed=8 * m * nt, transcendentals=0),
        name="grads_reduce")(scale, imgt, txt_all, e, a, b, part)


def solution(mesh):
    batch_spec = P(("row", "col"), None)
    shards = mesh.shape["row"] * mesh.shape["col"]

    def local_tile(img_loc, txt_loc, log_scale):
        n, d = img_loc.shape
        inv = 1.0 / (2 * n * shards)
        scale = jnp.exp(log_scale)
        e, imgt, txt_all, a, b, part = forward(inv, scale.reshape(1), img_loc, txt_loc)
        d_img, d_txt, tot = grads(inv, scale.reshape(1), imgt, txt_all, e, a, b, part)
        tot = jnp.sum(tot[0:2], axis=1)
        return tot[0], d_img, d_txt, tot[1]

    return jax.shard_map(local_tile, mesh=mesh, in_specs=(batch_spec, batch_spec, P()),
                         out_specs=(P(), batch_spec, batch_spec, P()), check_vma=False)
```

```python
import functools

import jax
import jax.numpy as jnp
from jax import lax
from jax.experimental import pallas as pl
from jax.experimental.pallas import tpu as pltpu
from jax.sharding import PartitionSpec as P

MESH = pl.DeviceIdType.MESH
F32 = jnp.float32
BF16 = jnp.bfloat16
VMEM_LIMIT = 67_043_328


class Grid:
    def __init__(self):
        row = lax.axis_index("row")
        self.c = lax.axis_index("col")
        self.z = row // 16
        self.y = (row // 4) % 4
        self.x = row % 4

    def dev(self, z, y, x, c):
        return {"row": (z * 4 + y) * 4 + x, "col": c}

    def y_a(self):
        return self.y + 1 - 2 * (self.y % 2)

    def y_b(self):
        return 3 - self.y

    def img_peer(self, dy, dz):
        y = self.y_a() if dy else self.y
        return self.dev((self.z + dz) % 4, y, self.x, self.c)

    def txt_peer(self, dc, dy, dx):
        y = self.y_b() if dy else self.y
        c = 1 - self.c if dc else self.c
        return self.dev(self.z, y, (self.x + dx) % 4, c)


def view(ref):
    return ref[0].at[ref[1]] if isinstance(ref, tuple) else ref


class Copy:
    def __init__(self, net, i, src, dst, peer):
        self.net, self.i, self.src, self.dst, self.peer = net, i, src, dst, peer

    def make(self):
        return pltpu.make_async_remote_copy(
            src_ref=view(self.src), dst_ref=view(self.dst), send_sem=self.net.send_sems.at[self.i],
            recv_sem=self.net.recv_sems.at[self.i], device_id=self.peer, device_id_type=MESH)

    def wait_recv(self):
        self.make().wait_recv()

    def wait_send(self):
        self.make().wait_send()


class Net:
    def __init__(self, send_sems, recv_sems):
        self.send_sems, self.recv_sems, self.copies = send_sems, recv_sems, []

    def send(self, src, dst, peer):
        copy = Copy(self, len(self.copies), src, dst, peer)
        copy.make().start()
        self.copies.append(copy)
        return copy

    def finish(self, skip=()):
        for copy in self.copies:
            if not any(copy is other for other in skip):
                copy.wait_send()


def greet(peers):
    barrier = pltpu.get_barrier_semaphore()
    for peer in peers:
        pl.semaphore_signal(barrier, inc=1, device_id=peer, device_id_type=MESH)
    pl.semaphore_wait(barrier, len(peers))


def neighbours(g):
    return [g.img_peer(0, 1), g.img_peer(0, 3), g.img_peer(1, 0), g.txt_peer(0, 0, 1), g.txt_peer(0, 0, 3),
            g.txt_peer(0, 1, 0), g.txt_peer(1, 0, 0)]


POS = {0: 0, 3: 1, 4: 2, 1: 3, 2: 4, 7: 5, 5: 6, 6: 7}
DEEP = 4
N_FORWARD = 2 * 18 + 9 + 22


class Gather:
    def __init__(self, net, own, dst, plus, minus, pair):
        self.net, self.own, self.dst = net, own, dst
        self.n = own.shape[0]
        self.plus, self.minus, self.pair = plus, minus, pair
        self.got = {}

    def half(self, k, side):
        h = self.n // 2
        return self.dst.at[POS[k], pl.ds(side * h, h)]

    def send(self, key, src, k, side, peer):
        self.got[key, side] = self.net.send(src, self.half(k, side), peer)

    def first(self):
        h = self.n // 2
        own = [self.own.at[pl.ds(side * h, h)] for side in (0, 1)]
        for side in (0, 1):
            self.send("p0", own[side], 3, side, self.plus)
            self.send("m0", own[1 - side], 1, 1 - side, self.minus)
            self.send("y0", own[side], 4, side, self.pair)

    def wait(self, *keys):
        for key in keys:
            self.got[key].wait_recv()

    def far(self, dy):
        self.wait(("p%d" % dy, 0))
        self.send("f%d" % dy, self.half(4 * dy + 3, 0), 4 * dy + 2, 0, self.plus)
        self.wait(("m%d" % dy, 1))
        self.send("f%d" % dy, self.half(4 * dy + 1, 1), 4 * dy + 2, 1, self.minus)

    def second(self):
        self.wait(("y0", 0), ("y0", 1))
        for side in (0, 1):
            self.send("p1", self.half(4, side), 7, side, self.plus)
            self.send("m1", self.half(4, 1 - side), 5, 1 - side, self.minus)


def forward_kernel(inv, scale_ref, img_ref, txt_ref, e_out, imgt_out, txt_out, a_ref, b_ref, part_ref,
                   img_all, txt_all, imgt, d0, d1, s0, s1, rs, rl, cs, cl, rsum, csum, rbuf, cbuf,
                   e_sems, t_sems, i_sems, own_sems, send_sems, recv_sems):
    g = Grid()
    n, d = img_ref.shape
    scale = scale_ref[0]
    img_offs = [(dy, dz) for dy in (0, 1) for dz in range(4) if (dy, dz) != (0, 0)]
    txt_offs = [(dc, dy, dx) for dc in (0, 1) for dy in (0, 1) for dx in range(4) if (dc, dy, dx) != (0, 0, 0)]
    own = [pltpu.make_async_copy(img_ref, img_all.at[0], own_sems.at[0]),
           pltpu.make_async_copy(txt_ref, txt_all.at[0], own_sems.at[1])]
    for copy in own:
        copy.start()
    greet([g.img_peer(*o) for o in img_offs] + [g.txt_peer(*o) for o in txt_offs])
    net = Net(send_sems, recv_sems)
    core = g.txt_peer(1, 0, 0)
    img = Gather(net, img_ref, img_all, g.img_peer(0, 1), g.img_peer(0, 3), g.img_peer(1, 0))
    txt = Gather(net, txt_ref, txt_all, g.txt_peer(0, 0, 1), g.txt_peer(0, 0, 3), g.txt_peer(0, 1, 0))
    img.first()
    txt.first()
    cross = {0: net.send(txt_ref, txt_all.at[8], core)}
    saves = []

    def save_txt(p):
        copy = pltpu.make_async_copy(txt_all.at[p], txt_out.at[pl.ds(p * n, n)], t_sems.at[p])
        copy.start()
        saves.append(copy)

    def got_txt(*slots):
        for k in slots:
            p = POS[k]
            cross[p] = net.send(txt_all.at[p], txt_all.at[8 + p], core)
            save_txt(p)

    def got_cross(*slots):
        for k in slots:
            cross[POS[k]].wait_recv()
            save_txt(8 + POS[k])

    def got_img(*slots):
        for k in slots:
            p = POS[k]
            imgt[p] = img_all[p].T
            copy = pltpu.make_async_copy(imgt.at[p], imgt_out.at[:, pl.ds(p * n, n)], i_sems.at[p])
            copy.start()
            saves.append(copy)

    dots, stage = (d0, d1), (s0, s1)

    def dot(i, k, buf):
        lhs = img_all[i]
        for side in (0, 1):
            dots[buf][side] = lax.dot_general(lhs, txt_all[8 * side + k], (((1,), (1,)), ((), ())),
                                              preferred_element_type=F32)

    def store(i, k, buf, slot):
        return pltpu.make_async_copy(stage[buf].at[slot], e_out.at[i, :, k], e_sems.at[buf * DEEP + slot])

    def free(buf, use):
        if isinstance(use, int):
            if use >= DEEP:
                store(0, 0, buf, use % DEEP).wait()
        else:
            @pl.when(use >= DEEP)
            def _():
                store(0, 0, buf, use % DEEP).wait()

    def finish_unit(i, k, buf, use):
        slot = use % DEEP
        for blk in range(n // 32):
            lo = blk * 32
            rows = pl.ds(i * n + lo, 32) if isinstance(i, int) else pl.ds(pl.multiple_of(i * n + lo, 32), 32)
            racc, lacc = rs[rows, :], rl[rows, :]
            for side in (0, 1):
                logits = scale * dots[buf][side, lo:lo + 32, :]
                e = jnp.exp(logits)
                el = e * logits
                stage[buf][slot, side, lo:lo + 32, :] = e
                for q in range(n // 128):
                    racc += e[:, q * 128:(q + 1) * 128]
                    lacc += el[:, q * 128:(q + 1) * 128]
                cs[8 * side + k] += jnp.sum(e.reshape(4, 8, n), axis=0)
                cl[8 * side + k] += jnp.sum(el.reshape(4, 8, n), axis=0)
            rs[rows, :] = racc
            rl[rows, :] = lacc
        store(i, k, buf, slot).start()

    state = {"buf": 0, "unit": (0, 0), "uses": [0, 0]}

    def last_unit():
        buf = state["buf"]
        free(buf, state["uses"][buf])
        finish_unit(*state["unit"], buf, state["uses"][buf])
        state["uses"][buf] += 1

    def one(i, k):
        buf = state["buf"]
        free(buf, state["uses"][buf])
        dot(i, k, 1 - buf)
        finish_unit(*state["unit"], buf, state["uses"][buf])
        state["uses"][buf] += 1
        state["buf"], state["unit"] = 1 - buf, (i, k)

    def run(i0, k0, width, start, count):
        buf = state["buf"]
        uses = list(state["uses"])

        def unit(u):
            return i0 + u // width, k0 + u % width

        def body(it, carry):
            u = start + 2 * it
            free(buf, uses[buf] + it)
            free(1 - buf, uses[1 - buf] + it)
            dot(*unit(u), 1 - buf)
            finish_unit(carry[0], carry[1], buf, uses[buf] + it)
            dot(*unit(u + 1), buf)
            finish_unit(*unit(u), 1 - buf, uses[1 - buf] + it)
            return unit(u + 1)

        last = tuple(jnp.int32(v) for v in state["unit"])
        state["unit"] = lax.fori_loop(0, count // 2, body, last)
        state["uses"] = [v + count // 2 for v in uses]
        if count % 2:
            one(*unit(jnp.int32(start + count - 1)))

    rs[...] = jnp.zeros_like(rs)
    rl[...] = jnp.zeros_like(rl)
    cs[...] = jnp.zeros_like(cs)
    cl[...] = jnp.zeros_like(cl)
    for copy in own:
        copy.wait()
    save_txt(0)
    got_img(0)
    img.far(0)
    txt.far(0)
    img.second()
    txt.second()
    got_txt(4)
    txt.wait(("p0", 1), ("m0", 0))
    got_txt(3, 1)
    got_cross(0)
    dot(0, 0, 0)
    img.wait(("p0", 1), ("m0", 0))
    got_cross(4, 3, 1)
    run(0, 0, 4, 1, 15)
    got_img(4, 3, 1)
    for r in (txt, img):
        r.wait(("f0", 0), ("f0", 1))
    got_txt(2)
    run(4, 0, 4, 0, 4)
    got_cross(2)
    run(0, 4, 1, 0, 5)
    got_img(2)
    for r in (txt, img):
        r.far(1)
    txt.wait(("p1", 1), ("m1", 0))
    got_txt(7, 5)
    img.wait(("p1", 1), ("m1", 0))
    run(5, 0, 5, 0, 10)
    got_cross(7, 5)
    run(0, 5, 2, 0, 6)
    txt.wait(("f1", 0), ("f1", 1))
    got_txt(6)
    run(3, 5, 2, 0, 8)
    got_img(7, 5)
    img.wait(("f1", 0), ("f1", 1))
    got_cross(6)
    run(7, 0, 8, 0, 8)
    run(0, 7, 1, 0, 7)
    last_unit()

    for p in range(16):
        for q in range(n // 128):
            csum[2 * p + q:2 * p + q + 1, :] = jnp.sum(cs[p, :, q * 128:(q + 1) * 128], axis=0, keepdims=True)
    sums = []
    for dc, dy, dx in txt_offs:
        sums.append(net.send(csum, cbuf.at[dc * 8 + dy * 4 + (4 - dx) % 4], g.txt_peer(dc, dy, dx)))
    for i in range(8 * n // 128):
        rsum[i:i + 1, :] = jnp.sum(rs[i * 128:(i + 1) * 128, :].T, axis=0, keepdims=True)
    for dy, dz in img_offs:
        sums.append(net.send(rsum, rbuf.at[dy * 4 + (4 - dz) % 4], g.img_peer(dy, dz)))
    got_img(6)
    pos = jnp.sum(img_ref[...].astype(F32) * txt_ref[...].astype(F32), axis=1, keepdims=True) * scale
    rlsum = [jnp.sum(rl[i * 128:(i + 1) * 128, :].T, axis=0, keepdims=True) for i in range(8 * n // 128)]
    clsum = [jnp.sum(cl[p, :, q * 128:(q + 1) * 128], axis=0, keepdims=True) for p in range(16) for q in range(n // 128)]
    for copy in sums:
        copy.wait_recv()
    loss = jnp.zeros((2, 128), F32)
    dt = jnp.zeros((1, 128), F32)
    for dy, dz in [(0, 0)] + img_offs:
        k = 2 * POS[dy * 4 + dz]
        tot = rsum[k:k + 2, :]
        for oy, oz in img_offs:
            q = 2 * POS[(dy ^ oy) * 4 + (dz - oz) % 4]
            tot += rbuf[oy * 4 + oz, q:q + 2, :]
        a = 1.0 / tot
        a_ref[k:k + 2, :] = a * inv
        dt += a[0:1] * rlsum[k] + a[1:2] * rlsum[k + 1]
        if k == 0:
            loss += jnp.log(tot)
    for dc, dy, dx in [(0, 0, 0)] + txt_offs:
        k = 2 * (dc * 8 + POS[dy * 4 + dx])
        tot = csum[k:k + 2, :]
        for oc, oy, ox in txt_offs:
            q = 2 * ((dc ^ oc) * 8 + POS[(dy ^ oy) * 4 + (dx - ox) % 4])
            tot += cbuf[oc * 8 + oy * 4 + ox, q:q + 2, :]
        b = 1.0 / tot
        b_ref[k:k + 2, :] = b * inv
        dt += b[0:1] * clsum[k] + b[1:2] * clsum[k + 1]
        if k == 0:
            loss += jnp.log(tot)
    diag = jnp.sum(pos, axis=0, keepdims=True)
    first_lane = lax.broadcasted_iota(jnp.int32, (1, 128), 1) == 0
    diag = jnp.where(first_lane, 2.0 * diag, 0.0)
    part_ref[...] = jnp.zeros_like(part_ref)
    part_ref[0:1, :] = (jnp.sum(loss, axis=0, keepdims=True) - diag) * inv
    part_ref[1:2, :] = (dt - diag) * inv
    for buf in (0, 1):
        for slot in range(DEEP):
            store(0, 0, buf, slot).wait()
    for copy in saves:
        copy.wait()
    net.finish()


def forward(inv, scale, img, txt):
    n, d = img.shape
    vmem = pl.BlockSpec(memory_space=pltpu.VMEM)
    hbm = pl.BlockSpec(memory_space=pl.ANY)
    dma = pltpu.SemaphoreType.DMA
    return pl.pallas_call(
        functools.partial(forward_kernel, inv),
        out_shape=[jax.ShapeDtypeStruct((8, 2, 8, n, n), F32), jax.ShapeDtypeStruct((d, 8 * n), BF16),
                   jax.ShapeDtypeStruct((16 * n, d), BF16), jax.ShapeDtypeStruct((16, 128), F32),
                   jax.ShapeDtypeStruct((32, 128), F32), jax.ShapeDtypeStruct((8, 128), F32)],
        in_specs=[pl.BlockSpec(memory_space=pltpu.SMEM), vmem, vmem],
        out_specs=[hbm, hbm, hbm, vmem, vmem, vmem],
        scratch_shapes=[pltpu.VMEM((8, n, d), BF16), pltpu.VMEM((16, n, d), BF16), pltpu.VMEM((8, d, n), BF16),
                        pltpu.VMEM((2, n, n), F32), pltpu.VMEM((2, n, n), F32), pltpu.VMEM((DEEP, 2, n, n), F32),
                        pltpu.VMEM((DEEP, 2, n, n), F32), pltpu.VMEM((8 * n, 128), F32), pltpu.VMEM((8 * n, 128), F32),
                        pltpu.VMEM((16, 8, n), F32), pltpu.VMEM((16, 8, n), F32), pltpu.VMEM((16, 128), F32),
                        pltpu.VMEM((32, 128), F32), pltpu.VMEM((8, 16, 128), F32), pltpu.VMEM((16, 32, 128), F32),
                        dma((2 * DEEP,)), dma((16,)), dma((8,)), dma((2,)), dma((N_FORWARD,)), dma((N_FORWARD,))],
        compiler_params=pltpu.CompilerParams(collective_id=0, has_side_effects=True, vmem_limit_bytes=VMEM_LIMIT),
        name="forward_sums")(scale, img, txt)


ICUT = 144
TCUT = 432
ORDER = (6, 5, 7, 2, 1, 4, 3, 0)
N_REDUCE = 8 + 2 * (4 + 18 + 1) + 22


class Ring:
    def __init__(self, net, acc, buf, cut, plus, minus, pair):
        self.net, self.acc, self.buf = net, acc, buf
        self.cut, self.rows = cut, acc.shape[1]
        self.plus, self.minus, self.pair = plus, minus, pair
        self.early, self.streams = {}, {}

    def pair_send(self, d):
        at = pl.ds(self.cut, self.rows - self.cut)
        self.early[d] = self.net.send((self.acc, (POS[4 + d], at)), (self.buf, (4 + d, at)), self.pair)

    def pair_add(self, d):
        self.early[d].wait_recv()
        self.acc[POS[d], self.cut:] += self.buf[4 + d, self.cut:]

    def where(self, name):
        if name == 2:
            return 0, self.cut, (self.rows - self.cut) // 2
        return 4 * name, 0, self.cut // 2

    def send(self, name, key, slot, half, to_slot, peer):
        _, lo, h = self.where(name)
        at = pl.ds(lo + half * h, h)
        self.streams[name, key] = self.net.send((self.acc, (POS[slot], at)), (self.buf, (to_slot, at)), peer)

    def far(self, name):
        b, _, _ = self.where(name)
        self.send(name, "a+", b + 2, 0, b + 2, self.plus)
        self.send(name, "a-", b + 2, 1, b + 2, self.minus)

    def plain_plus(self, name):
        b, _, _ = self.where(name)
        self.send(name, "b+1", b + 1, 1, b + 3, self.plus)

    def plain_minus(self, name):
        b, _, _ = self.where(name)
        self.send(name, "b-0", b + 3, 0, b + 1, self.minus)

    def mid(self, name):
        b, lo, h = self.where(name)
        self.streams[name, "a+"].wait_recv()
        self.acc[POS[b + 1], lo:lo + h] += self.buf[b + 2, lo:lo + h]
        self.send(name, "b+0", b + 1, 0, b + 3, self.plus)
        self.streams[name, "a-"].wait_recv()
        self.acc[POS[b + 3], lo + h:lo + 2 * h] += self.buf[b + 2, lo + h:lo + 2 * h]
        self.send(name, "b-1", b + 3, 1, b + 1, self.minus)

    def end(self, name):
        b, lo, h = self.where(name)
        for key in ("b+1", "b-0", "b+0", "b-1"):
            self.streams[name, key].wait_recv()
        self.acc[POS[b], lo:lo + 2 * h] += self.buf[b + 1, lo:lo + 2 * h] + self.buf[b + 3, lo:lo + 2 * h]

    def pair_last(self):
        at = pl.ds(0, self.cut)
        self.late = self.net.send((self.acc, (POS[4], at)), (self.buf, (0, at)), self.pair)

    def pair_end(self):
        self.late.wait_recv()
        self.acc[0, 0:self.cut] += self.buf[0, 0:self.cut]

    def ready(self, step):
        if step == 0:
            self.pair_send(2)
            self.far(1)
        elif step == 1:
            self.pair_send(1)
            self.plain_plus(1)
        elif step == 2:
            self.pair_send(3)
            self.plain_minus(1)
            self.mid(1)
        elif step == 3:
            self.far(0)
            self.pair_add(2)
            self.far(2)
        elif step == 4:
            self.plain_plus(0)
            self.pair_add(1)
            self.plain_plus(2)
        elif step == 5:
            self.pair_send(0)
            self.end(1)
            self.pair_last()
        elif step == 6:
            self.plain_minus(0)
            self.pair_add(3)
            self.plain_minus(2)
            self.mid(0)
            self.mid(2)

    def close(self):
        self.pair_add(0)
        self.end(0)
        self.pair_end()
        self.end(2)


KC = 512


def grads_kernel(inv, imgt_hbm, txt_hbm, e_hbm, a_ref, b_ref, part_ref, img_out, txt_out, part_out,
                 imgt, txt, erow, ecol, gb0, gb1, arow, stage, iacc, tacc, ibuf, tbuf, dbuf, pa, pb, psum,
                 local_sems, row_sems, col_sems, send_sems, recv_sems):
    g = Grid()
    n = iacc.shape[1]
    d = iacc.shape[2]
    m = imgt.shape[1]
    nt = txt.shape[0]
    img_offs = [(dy, dz) for dy in (0, 1) for dz in range(4) if (dy, dz) != (0, 0)]
    txt_offs = [(dc, dy, dx) for dc in (0, 1) for dy in (0, 1) for dx in range(4) if (dc, dy, dx) != (0, 0, 0)]

    def row_load(step):
        return pltpu.make_async_copy(e_hbm.at[POS[ORDER[step]]], erow.at[step % 2], row_sems.at[step % 2])

    def col_load(step, side):
        return pltpu.make_async_copy(e_hbm.at[:, side, POS[ORDER[step]]], ecol.at[side], col_sems.at[side])

    load_imgt = pltpu.make_async_copy(imgt_hbm, imgt, local_sems.at[0])
    load_txt = pltpu.make_async_copy(txt_hbm, txt, local_sems.at[1])
    cols = {}
    for side in (1, 0):
        cols[0, side] = col_load(0, side)
        cols[0, side].start()
    load_imgt.start()
    rows = {0: row_load(0)}
    rows[0].start()
    load_txt.start()
    for i in range(m // 128):
        arow[i * 128:(i + 1) * 128, :] = jnp.broadcast_to(a_ref[i:i + 1, :], (128, 128)).T
    greet([g.img_peer(*o) for o in img_offs] + [g.txt_peer(*o) for o in txt_offs])
    net = Net(send_sems, recv_sems)
    core = g.txt_peer(1, 0, 0)
    ia = g.z * 2 + g.y % 2
    ib = (g.x * 2 + g.y // 2) * 2 + g.c
    scal_a = [net.send(part_ref, pa.at[ia], g.img_peer(*o)) for o in img_offs]
    pa[ia] = part_ref[...]
    img = Ring(net, iacc, ibuf, ICUT, g.img_peer(0, 1), g.img_peer(0, 3), g.img_peer(1, 0))
    txr = Ring(net, tacc, tbuf, TCUT, g.txt_peer(0, 0, 1), g.txt_peer(0, 0, 3), g.txt_peer(0, 1, 0))

    def minus_diag(grad, q):
        r = lax.broadcasted_iota(jnp.int32, (n, 128), 0)
        c = lax.broadcasted_iota(jnp.int32, (n, 128), 1) + q * 128
        return grad - jnp.where(r == c, 2.0 * inv, 0.0)

    def add(out_ref, part, may_start, it):
        old = out_ref[...]
        out_ref[...] = part + (jnp.where(it > 0, old, 0.0) if may_start else old)

    def col_slots(p, outs):
        tiles = KC // n
        count = m // KC

        def grad(i, to, diag=False):
            for t in range(tiles):
                a = arow[pl.ds(pl.multiple_of(i * KC + t * n, n), n), :]
                for side in (0, 1):
                    for q in range(n // 128):
                        lanes = slice(q * 128, (q + 1) * 128)
                        at = 2 * (p + 8 * side) + q
                        v = ecol[side, i * tiles + t, :, lanes] * (a + b_ref[at:at + 1, :])
                        if diag and t == 0 and side == 0:
                            v = minus_diag(v, q)
                        to[t * n:(t + 1) * n, side * n + q * 128:side * n + (q + 1) * 128] = v.astype(BF16)

        grad(0, gb0[0], diag=p == 0)

        def body(it, carry):
            for half, (now, later) in enumerate(((gb0[0], gb0[1]), (gb0[1], gb0[0]))):
                i = 2 * it + half
                at = pl.ds(pl.multiple_of(i * KC, KC), KC)
                part = jnp.dot(imgt[:, at], now[...], preferred_element_type=F32)
                for side in (0, 1):
                    add(outs[side], part[:, side * n:(side + 1) * n], half == 0, it)
                grad((i + 1) % count, later)
            return carry

        lax.fori_loop(0, count // 2, body, 0)

    def row_slot(p, e_ref, out_ref):
        tiles = KC // n
        count = nt // KC

        def grad(i, to, diag=False):
            for t in range(tiles):
                tile = i * tiles + t
                for q in range(n // 128):
                    lanes = slice(q * 128, (q + 1) * 128)
                    v = (e_ref[tile // 8, tile % 8, :, lanes]
                         * (arow[p * n:(p + 1) * n, :] + b_ref[pl.ds(2 * tile + q, 1), :]))
                    if diag and t == 0:
                        v = minus_diag(v, q)
                    to[:, t * n + q * 128:t * n + (q + 1) * 128] = v.astype(BF16)

        grad(0, gb1[0], diag=p == 0)
        def body(it, carry):
            for half, (now, later) in enumerate(((gb1[0], gb1[1]), (gb1[1], gb1[0]))):
                i = 2 * it + half
                at = pl.ds(pl.multiple_of(i * KC, KC), KC)
                add(out_ref, jnp.dot(now[...], txt[at, :], preferred_element_type=F32), half == 0, it)
                grad((i + 1) % count, later)
            return carry

        lax.fori_loop(0, count // 2, body, 0)

    cross = {}
    for step, k in enumerate(ORDER):
        cols[step, 1].wait()
        cols[step, 0].wait()
        if step == 0:
            load_imgt.wait()
        if step >= 2:
            cross[ORDER[step - 2]].wait_send()
        col_slots(POS[k], (tacc.at[POS[k]], stage.at[step % 2]))
        cross[k] = net.send(stage.at[step % 2], dbuf.at[k], core)
        if step + 1 < len(ORDER):
            rows[step + 1] = row_load(step + 1)
            rows[step + 1].start()
            for side in (1, 0):
                cols[step + 1, side] = col_load(step + 1, side)
                cols[step + 1, side].start()
        rows[step].wait()
        if step == 0:
            load_txt.wait()
        row_slot(POS[k], erow.at[step % 2], iacc.at[POS[k]])
        cross[k].wait_recv()
        tacc[POS[k]] += dbuf[k]
        txr.ready(step)
        img.ready(step)
        if step == 1:
            for copy in scal_a:
                copy.wait_recv()
            total = pa[0]
            for q in range(1, 8):
                total += pa[q]
            psum[...] = total
            scal_b = [net.send(psum, pb.at[ib], g.txt_peer(*o)) for o in txt_offs]
            pb[ib] = total
    for copy in scal_b:
        copy.wait_recv()
    total = pb[0]
    for k in range(1, 16):
        total += pb[k]
    part_out[...] = total
    for r in (img, txr):
        r.close()
    img_out[...] = iacc[0]
    txt_out[...] = tacc[0].T
    net.finish(skip=[cross[k] for k in ORDER[:-2]])


def grads(inv, imgt, txt_all, e, a, b, part):
    d, m = imgt.shape
    nt = txt_all.shape[0]
    n = m // 8
    vmem = pl.BlockSpec(memory_space=pltpu.VMEM)
    hbm = pl.BlockSpec(memory_space=pl.ANY)
    dma = pltpu.SemaphoreType.DMA
    return pl.pallas_call(
        functools.partial(grads_kernel, inv),
        out_shape=[jax.ShapeDtypeStruct((n, d), F32), jax.ShapeDtypeStruct((n, d), F32),
                   jax.ShapeDtypeStruct((8, 128), F32)],
        in_specs=[hbm, hbm, hbm, vmem, vmem, vmem],
        out_specs=[vmem] * 3,
        scratch_shapes=[pltpu.VMEM((d, m), BF16), pltpu.VMEM((nt, d), BF16), pltpu.VMEM((2, 2, 8, n, n), F32),
                        pltpu.VMEM((2, 8, n, n), F32), [pltpu.VMEM((KC, 2 * n), BF16)] * 2, [pltpu.VMEM((n, KC), BF16)] * 2,
                        pltpu.VMEM((m, 128), F32), pltpu.VMEM((2, d, n), F32), pltpu.VMEM((8, n, d), F32),
                        pltpu.VMEM((8, d, n), F32), pltpu.VMEM((8, n, d), F32), pltpu.VMEM((8, d, n), F32),
                        pltpu.VMEM((8, d, n), F32), pltpu.VMEM((8, 8, 128), F32), pltpu.VMEM((16, 8, 128), F32),
                        pltpu.VMEM((8, 128), F32), dma((2,)), dma((2,)), dma((2,)), dma((N_REDUCE,)),
                        dma((N_REDUCE,))],
        compiler_params=pltpu.CompilerParams(collective_id=2, has_side_effects=True, vmem_limit_bytes=VMEM_LIMIT),
        cost_estimate=pl.CostEstimate(flops=4 * m * nt * d, bytes_accessed=8 * m * nt, transcendentals=0),
        name="grads_reduce")(imgt, txt_all, e, a, b, part)


def solution(mesh):
    batch_spec = P(("row", "col"), None)
    shards = mesh.shape["row"] * mesh.shape["col"]

    def local_tile(img_loc, txt_loc, log_scale):
        n, d = img_loc.shape
        inv = 1.0 / (2 * n * shards)
        scale = jnp.exp(log_scale)
        e, imgt, txt_all, a, b, part = forward(inv, scale.reshape(1), img_loc, txt_loc)
        img_sum, txt_sum, tot = grads(inv, imgt, txt_all, e, a, b, part)
        d_img = (scale * img_sum).astype(BF16)
        d_txt = (scale * txt_sum).astype(BF16)
        tot = jnp.sum(tot[0:2], axis=1)
        return tot[0], d_img, d_txt, tot[1]

    return jax.shard_map(local_tile, mesh=mesh, in_specs=(batch_spec, batch_spec, P()),
                         out_specs=(P(), batch_spec, batch_spec, P()), check_vma=False)
```

```python
import functools

import jax
import jax.numpy as jnp
from jax import lax
from jax.experimental import pallas as pl
from jax.experimental.pallas import tpu as pltpu
from jax.sharding import PartitionSpec as P

MESH = pl.DeviceIdType.MESH
F32 = jnp.float32
BF16 = jnp.bfloat16
VMEM_LIMIT = 67_043_328


class Grid:
    def __init__(self):
        row = lax.axis_index("row")
        self.c = lax.axis_index("col")
        self.z = row // 16
        self.y = (row // 4) % 4
        self.x = row % 4
        self.turn = 1 - 2 * self.c

    def dev(self, z, y, x, c):
        return {"row": (z * 4 + y) * 4 + x, "col": c}

    def y_a(self):
        return self.y + 1 - 2 * (self.y % 2)

    def y_b(self):
        return 3 - self.y

    def img_peer(self, dy, dz):
        y = self.y_a() if dy else self.y
        return self.dev((self.z + 4 + self.turn * dz) % 4, y, self.x, self.c)

    def txt_peer(self, dc, dy, dx):
        y = self.y_b() if dy else self.y
        c = 1 - self.c if dc else self.c
        return self.dev(self.z, y, (self.x + 4 + self.turn * dx) % 4, c)


def view(ref):
    return ref[0].at[ref[1]] if isinstance(ref, tuple) else ref


class Copy:
    def __init__(self, net, i, src, dst, peer):
        self.net, self.i, self.src, self.dst, self.peer = net, i, src, dst, peer

    def make(self):
        return pltpu.make_async_remote_copy(
            src_ref=view(self.src), dst_ref=view(self.dst), send_sem=self.net.send_sems.at[self.i],
            recv_sem=self.net.recv_sems.at[self.i], device_id=self.peer, device_id_type=MESH)

    def wait_recv(self):
        self.make().wait_recv()

    def wait_send(self):
        self.make().wait_send()


class Net:
    def __init__(self, send_sems, recv_sems):
        self.send_sems, self.recv_sems, self.copies = send_sems, recv_sems, []

    def send(self, src, dst, peer):
        copy = Copy(self, len(self.copies), src, dst, peer)
        copy.make().start()
        self.copies.append(copy)
        return copy

    def finish(self, skip=()):
        for copy in self.copies:
            if not any(copy is other for other in skip):
                copy.wait_send()


def greet(peers):
    barrier = pltpu.get_barrier_semaphore()
    for peer in peers:
        pl.semaphore_signal(barrier, inc=1, device_id=peer, device_id_type=MESH)
    pl.semaphore_wait(barrier, len(peers))


def neighbours(g):
    return [g.img_peer(0, 1), g.img_peer(0, 3), g.img_peer(1, 0), g.txt_peer(0, 0, 1), g.txt_peer(0, 0, 3),
            g.txt_peer(0, 1, 0), g.txt_peer(1, 0, 0)]


POS = {0: 0, 3: 1, 4: 2, 1: 3, 2: 4, 7: 5, 5: 6, 6: 7}
DEEP = 4
N_FORWARD = 2 * 18 + 9 + 22


def mirror(k):
    return 4 * (k // 4) + (4 - k % 4) % 4


class Gather:
    def __init__(self, net, own, dst, plus, minus, pair):
        self.net, self.own, self.dst = net, own, dst
        self.n = own.shape[0]
        self.plus, self.minus, self.pair = plus, minus, pair
        self.got = {}

    def half(self, k, side):
        h = self.n // 2
        return self.dst.at[POS[k], pl.ds(side * h, h)]

    def send(self, key, src, k, side, peer):
        self.got[key, side] = self.net.send(src, self.half(k, side), peer)

    def first(self):
        h = self.n // 2
        own = [self.own.at[pl.ds(side * h, h)] for side in (0, 1)]
        for side in (0, 1):
            self.send("p0", own[side], 3, side, self.plus)
            self.send("m0", own[1 - side], 1, 1 - side, self.minus)
            self.send("y0", own[side], 4, side, self.pair)

    def wait(self, *keys):
        for key in keys:
            self.got[key].wait_recv()

    def far(self, dy):
        self.wait(("p%d" % dy, 0))
        self.send("f%d" % dy, self.half(4 * dy + 3, 0), 4 * dy + 2, 0, self.plus)
        self.wait(("m%d" % dy, 1))
        self.send("f%d" % dy, self.half(4 * dy + 1, 1), 4 * dy + 2, 1, self.minus)

    def second(self):
        self.wait(("y0", 0), ("y0", 1))
        for side in (0, 1):
            self.send("p1", self.half(4, side), 7, side, self.plus)
            self.send("m1", self.half(4, 1 - side), 5, 1 - side, self.minus)


def forward_kernel(inv, scale_ref, img_ref, txt_ref, e_out, imgt_out, txt_out, a_ref, b_ref, part_ref,
                   img_all, txt_all, imgt, d0, d1, s0, s1, rs, rl, cs, cl, rsum, csum, rbuf, cbuf,
                   e_sems, t_sems, i_sems, own_sems, send_sems, recv_sems):
    g = Grid()
    n, d = img_ref.shape
    scale = scale_ref[0]
    img_offs = [(dy, dz) for dy in (0, 1) for dz in range(4) if (dy, dz) != (0, 0)]
    txt_offs = [(dc, dy, dx) for dc in (0, 1) for dy in (0, 1) for dx in range(4) if (dc, dy, dx) != (0, 0, 0)]
    own = [pltpu.make_async_copy(img_ref, img_all.at[0], own_sems.at[0]),
           pltpu.make_async_copy(txt_ref, txt_all.at[0], own_sems.at[1])]
    for copy in own:
        copy.start()
    greet([g.img_peer(*o) for o in img_offs] + [g.txt_peer(*o) for o in txt_offs])
    net = Net(send_sems, recv_sems)
    core = g.txt_peer(1, 0, 0)
    img = Gather(net, img_ref, img_all, g.img_peer(0, 1), g.img_peer(0, 3), g.img_peer(1, 0))
    txt = Gather(net, txt_ref, txt_all, g.txt_peer(0, 0, 1), g.txt_peer(0, 0, 3), g.txt_peer(0, 1, 0))
    img.first()
    txt.first()
    cross = {0: net.send(txt_ref, txt_all.at[8], core)}
    saves = []

    def save_txt(p):
        copy = pltpu.make_async_copy(txt_all.at[p], txt_out.at[pl.ds(p * n, n)], t_sems.at[p])
        copy.start()
        saves.append(copy)

    def got_txt(*slots):
        for k in slots:
            p = POS[k]
            cross[k] = net.send(txt_all.at[p], txt_all.at[8 + POS[mirror(k)]], core)
            save_txt(p)

    def got_cross(*slots):
        for k in slots:
            cross[mirror(k)].wait_recv()
            save_txt(8 + POS[k])

    def got_img(*slots):
        for k in slots:
            p = POS[k]
            imgt[p] = img_all[p].T
            copy = pltpu.make_async_copy(imgt.at[p], imgt_out.at[:, pl.ds(p * n, n)], i_sems.at[p])
            copy.start()
            saves.append(copy)

    dots, stage = (d0, d1), (s0, s1)

    def dot(i, k, buf):
        lhs = img_all[i]
        for side in (0, 1):
            dots[buf][side] = lax.dot_general(lhs, txt_all[8 * side + k], (((1,), (1,)), ((), ())),
                                              preferred_element_type=F32)

    def store(i, k, buf, slot):
        return pltpu.make_async_copy(stage[buf].at[slot], e_out.at[i, :, k], e_sems.at[buf * DEEP + slot])

    def free(buf, use):
        if isinstance(use, int):
            if use >= DEEP:
                store(0, 0, buf, use % DEEP).wait()
        else:
            @pl.when(use >= DEEP)
            def _():
                store(0, 0, buf, use % DEEP).wait()

    def finish_unit(i, k, buf, use):
        slot = use % DEEP
        for blk in range(n // 32):
            lo = blk * 32
            rows = pl.ds(i * n + lo, 32) if isinstance(i, int) else pl.ds(pl.multiple_of(i * n + lo, 32), 32)
            racc, lacc = rs[rows, :], rl[rows, :]
            for side in (0, 1):
                logits = scale * dots[buf][side, lo:lo + 32, :]
                e = jnp.exp(logits)
                el = e * logits
                stage[buf][slot, side, lo:lo + 32, :] = e
                for q in range(n // 128):
                    racc += e[:, q * 128:(q + 1) * 128]
                    lacc += el[:, q * 128:(q + 1) * 128]
                cs[8 * side + k] += jnp.sum(e.reshape(4, 8, n), axis=0)
                cl[8 * side + k] += jnp.sum(el.reshape(4, 8, n), axis=0)
            rs[rows, :] = racc
            rl[rows, :] = lacc
        store(i, k, buf, slot).start()

    state = {"buf": 0, "unit": (0, 0), "uses": [0, 0]}

    def last_unit():
        buf = state["buf"]
        free(buf, state["uses"][buf])
        finish_unit(*state["unit"], buf, state["uses"][buf])
        state["uses"][buf] += 1

    def one(i, k):
        buf = state["buf"]
        free(buf, state["uses"][buf])
        dot(i, k, 1 - buf)
        finish_unit(*state["unit"], buf, state["uses"][buf])
        state["uses"][buf] += 1
        state["buf"], state["unit"] = 1 - buf, (i, k)

    def run(i0, k0, width, start, count):
        buf = state["buf"]
        uses = list(state["uses"])

        def unit(u):
            return i0 + u // width, k0 + u % width

        def body(it, carry):
            u = start + 2 * it
            free(buf, uses[buf] + it)
            free(1 - buf, uses[1 - buf] + it)
            dot(*unit(u), 1 - buf)
            finish_unit(carry[0], carry[1], buf, uses[buf] + it)
            dot(*unit(u + 1), buf)
            finish_unit(*unit(u), 1 - buf, uses[1 - buf] + it)
            return unit(u + 1)

        last = tuple(jnp.int32(v) for v in state["unit"])
        state["unit"] = lax.fori_loop(0, count // 2, body, last)
        state["uses"] = [v + count // 2 for v in uses]
        if count % 2:
            one(*unit(jnp.int32(start + count - 1)))

    rs[...] = jnp.zeros_like(rs)
    rl[...] = jnp.zeros_like(rl)
    cs[...] = jnp.zeros_like(cs)
    cl[...] = jnp.zeros_like(cl)
    for copy in own:
        copy.wait()
    save_txt(0)
    got_img(0)
    img.far(0)
    txt.far(0)
    img.second()
    txt.second()
    got_txt(4)
    txt.wait(("p0", 1), ("m0", 0))
    got_txt(3, 1)
    got_cross(0)
    dot(0, 0, 0)
    img.wait(("p0", 1), ("m0", 0))
    got_cross(4, 3, 1)
    run(0, 0, 4, 1, 15)
    got_img(4, 3, 1)
    for r in (txt, img):
        r.wait(("f0", 0), ("f0", 1))
    got_txt(2)
    run(4, 0, 4, 0, 4)
    got_cross(2)
    run(0, 4, 1, 0, 5)
    got_img(2)
    for r in (txt, img):
        r.far(1)
    txt.wait(("p1", 1), ("m1", 0))
    got_txt(7, 5)
    img.wait(("p1", 1), ("m1", 0))
    run(5, 0, 5, 0, 10)
    got_cross(7, 5)
    run(0, 5, 2, 0, 6)
    txt.wait(("f1", 0), ("f1", 1))
    got_txt(6)
    run(3, 5, 2, 0, 8)
    got_img(7, 5)
    img.wait(("f1", 0), ("f1", 1))
    got_cross(6)
    run(7, 0, 8, 0, 8)
    run(0, 7, 1, 0, 7)
    last_unit()

    for p in range(16):
        for q in range(n // 128):
            csum[2 * p + q:2 * p + q + 1, :] = jnp.sum(cs[p, :, q * 128:(q + 1) * 128], axis=0, keepdims=True)
    sums = []
    for dc, dy, dx in txt_offs:
        sums.append(net.send(csum, cbuf.at[dc * 8 + dy * 4 + (dx if dc else (4 - dx) % 4)], g.txt_peer(dc, dy, dx)))
    for i in range(8 * n // 128):
        rsum[i:i + 1, :] = jnp.sum(rs[i * 128:(i + 1) * 128, :].T, axis=0, keepdims=True)
    for dy, dz in img_offs:
        sums.append(net.send(rsum, rbuf.at[dy * 4 + (4 - dz) % 4], g.img_peer(dy, dz)))
    got_img(6)
    pos = jnp.sum(img_ref[...].astype(F32) * txt_ref[...].astype(F32), axis=1, keepdims=True) * scale
    rlsum = [jnp.sum(rl[i * 128:(i + 1) * 128, :].T, axis=0, keepdims=True) for i in range(8 * n // 128)]
    clsum = [jnp.sum(cl[p, :, q * 128:(q + 1) * 128], axis=0, keepdims=True) for p in range(16) for q in range(n // 128)]
    for copy in sums:
        copy.wait_recv()
    loss = jnp.zeros((2, 128), F32)
    dt = jnp.zeros((1, 128), F32)
    for dy, dz in [(0, 0)] + img_offs:
        k = 2 * POS[dy * 4 + dz]
        tot = rsum[k:k + 2, :]
        for oy, oz in img_offs:
            q = 2 * POS[(dy ^ oy) * 4 + (dz - oz) % 4]
            tot += rbuf[oy * 4 + oz, q:q + 2, :]
        a = 1.0 / tot
        a_ref[k:k + 2, :] = a * inv
        dt += a[0:1] * rlsum[k] + a[1:2] * rlsum[k + 1]
        if k == 0:
            loss += jnp.log(tot)
    for dc, dy, dx in [(0, 0, 0)] + txt_offs:
        k = 2 * (dc * 8 + POS[dy * 4 + dx])
        tot = csum[k:k + 2, :]
        for oc, oy, ox in txt_offs:
            q = 2 * ((dc ^ oc) * 8 + POS[(dy ^ oy) * 4 + ((ox - dx) if oc else (dx - ox)) % 4])
            tot += cbuf[oc * 8 + oy * 4 + ox, q:q + 2, :]
        b = 1.0 / tot
        b_ref[k:k + 2, :] = b * inv
        dt += b[0:1] * clsum[k] + b[1:2] * clsum[k + 1]
        if k == 0:
            loss += jnp.log(tot)
    diag = jnp.sum(pos, axis=0, keepdims=True)
    first_lane = lax.broadcasted_iota(jnp.int32, (1, 128), 1) == 0
    diag = jnp.where(first_lane, 2.0 * diag, 0.0)
    part_ref[...] = jnp.zeros_like(part_ref)
    part_ref[0:1, :] = (jnp.sum(loss, axis=0, keepdims=True) - diag) * inv
    part_ref[1:2, :] = (dt - diag) * inv
    for buf in (0, 1):
        for slot in range(DEEP):
            store(0, 0, buf, slot).wait()
    for copy in saves:
        copy.wait()
    net.finish()


def forward(inv, scale, img, txt):
    n, d = img.shape
    vmem = pl.BlockSpec(memory_space=pltpu.VMEM)
    hbm = pl.BlockSpec(memory_space=pl.ANY)
    dma = pltpu.SemaphoreType.DMA
    return pl.pallas_call(
        functools.partial(forward_kernel, inv),
        out_shape=[jax.ShapeDtypeStruct((8, 2, 8, n, n), F32), jax.ShapeDtypeStruct((d, 8 * n), BF16),
                   jax.ShapeDtypeStruct((16 * n, d), BF16), jax.ShapeDtypeStruct((16, 128), F32),
                   jax.ShapeDtypeStruct((32, 128), F32), jax.ShapeDtypeStruct((8, 128), F32)],
        in_specs=[pl.BlockSpec(memory_space=pltpu.SMEM), vmem, vmem],
        out_specs=[hbm, hbm, hbm, vmem, vmem, vmem],
        scratch_shapes=[pltpu.VMEM((8, n, d), BF16), pltpu.VMEM((16, n, d), BF16), pltpu.VMEM((8, d, n), BF16),
                        pltpu.VMEM((2, n, n), F32), pltpu.VMEM((2, n, n), F32), pltpu.VMEM((DEEP, 2, n, n), F32),
                        pltpu.VMEM((DEEP, 2, n, n), F32), pltpu.VMEM((8 * n, 128), F32), pltpu.VMEM((8 * n, 128), F32),
                        pltpu.VMEM((16, 8, n), F32), pltpu.VMEM((16, 8, n), F32), pltpu.VMEM((16, 128), F32),
                        pltpu.VMEM((32, 128), F32), pltpu.VMEM((8, 16, 128), F32), pltpu.VMEM((16, 32, 128), F32),
                        dma((2 * DEEP,)), dma((16,)), dma((8,)), dma((2,)), dma((N_FORWARD,)), dma((N_FORWARD,))],
        compiler_params=pltpu.CompilerParams(collective_id=0, has_side_effects=True, vmem_limit_bytes=VMEM_LIMIT),
        name="forward_sums")(scale, img, txt)


ICUT = 144
TCUT = 432
ORDER = (6, 5, 7, 2, 1, 4, 3, 0)
N_REDUCE = 8 + 2 * (4 + 18 + 1) + 22


class Ring:
    def __init__(self, net, acc, buf, cut, plus, minus, pair):
        self.net, self.acc, self.buf = net, acc, buf
        self.cut, self.rows = cut, acc.shape[1]
        self.plus, self.minus, self.pair = plus, minus, pair
        self.early, self.streams = {}, {}

    def pair_send(self, d):
        at = pl.ds(self.cut, self.rows - self.cut)
        self.early[d] = self.net.send((self.acc, (POS[4 + d], at)), (self.buf, (4 + d, at)), self.pair)

    def pair_add(self, d):
        self.early[d].wait_recv()
        self.acc[POS[d], self.cut:] += self.buf[4 + d, self.cut:]

    def where(self, name):
        if name == 2:
            return 0, self.cut, (self.rows - self.cut) // 2
        return 4 * name, 0, self.cut // 2

    def send(self, name, key, slot, half, to_slot, peer):
        _, lo, h = self.where(name)
        at = pl.ds(lo + half * h, h)
        self.streams[name, key] = self.net.send((self.acc, (POS[slot], at)), (self.buf, (to_slot, at)), peer)

    def far(self, name):
        b, _, _ = self.where(name)
        self.send(name, "a+", b + 2, 0, b + 2, self.plus)
        self.send(name, "a-", b + 2, 1, b + 2, self.minus)

    def plain_plus(self, name):
        b, _, _ = self.where(name)
        self.send(name, "b+1", b + 1, 1, b + 3, self.plus)

    def plain_minus(self, name):
        b, _, _ = self.where(name)
        self.send(name, "b-0", b + 3, 0, b + 1, self.minus)

    def mid(self, name):
        b, lo, h = self.where(name)
        self.streams[name, "a+"].wait_recv()
        self.acc[POS[b + 1], lo:lo + h] += self.buf[b + 2, lo:lo + h]
        self.send(name, "b+0", b + 1, 0, b + 3, self.plus)
        self.streams[name, "a-"].wait_recv()
        self.acc[POS[b + 3], lo + h:lo + 2 * h] += self.buf[b + 2, lo + h:lo + 2 * h]
        self.send(name, "b-1", b + 3, 1, b + 1, self.minus)

    def end(self, name):
        b, lo, h = self.where(name)
        for key in ("b+1", "b-0", "b+0", "b-1"):
            self.streams[name, key].wait_recv()
        self.acc[POS[b], lo:lo + 2 * h] += self.buf[b + 1, lo:lo + 2 * h] + self.buf[b + 3, lo:lo + 2 * h]

    def pair_last(self):
        at = pl.ds(0, self.cut)
        self.late = self.net.send((self.acc, (POS[4], at)), (self.buf, (0, at)), self.pair)

    def pair_end(self):
        self.late.wait_recv()
        self.acc[0, 0:self.cut] += self.buf[0, 0:self.cut]

    def ready(self, step):
        if step == 0:
            self.pair_send(2)
            self.far(1)
        elif step == 1:
            self.pair_send(1)
            self.plain_plus(1)
        elif step == 2:
            self.pair_send(3)
            self.plain_minus(1)
            self.mid(1)
        elif step == 3:
            self.far(0)
            self.pair_add(2)
            self.far(2)
        elif step == 4:
            self.plain_plus(0)
            self.pair_add(1)
            self.plain_plus(2)
        elif step == 5:
            self.pair_send(0)
            self.end(1)
            self.pair_last()
        elif step == 6:
            self.plain_minus(0)
            self.pair_add(3)
            self.plain_minus(2)
            self.mid(0)
            self.mid(2)

    def close(self):
        self.pair_add(0)
        self.end(0)
        self.pair_end()
        self.end(2)


KC = 512


def grads_kernel(inv, imgt_hbm, txt_hbm, e_hbm, a_ref, b_ref, part_ref, img_out, txt_out, part_out,
                 imgt, txt, erow, ecol, gb0, gb1, arow, stage, iacc, tacc, ibuf, tbuf, dbuf, pa, pb, psum,
                 local_sems, row_sems, col_sems, send_sems, recv_sems):
    g = Grid()
    n = iacc.shape[1]
    d = iacc.shape[2]
    m = imgt.shape[1]
    nt = txt.shape[0]
    img_offs = [(dy, dz) for dy in (0, 1) for dz in range(4) if (dy, dz) != (0, 0)]
    txt_offs = [(dc, dy, dx) for dc in (0, 1) for dy in (0, 1) for dx in range(4) if (dc, dy, dx) != (0, 0, 0)]

    def row_load(step):
        return pltpu.make_async_copy(e_hbm.at[POS[ORDER[step]]], erow.at[step % 2], row_sems.at[step % 2])

    def col_load(step, side):
        k = mirror(ORDER[step]) if side else ORDER[step]
        return pltpu.make_async_copy(e_hbm.at[:, side, POS[k]], ecol.at[side], col_sems.at[side])

    load_imgt = pltpu.make_async_copy(imgt_hbm, imgt, local_sems.at[0])
    load_txt = pltpu.make_async_copy(txt_hbm, txt, local_sems.at[1])
    cols = {}
    cols[0, 1] = col_load(0, 1)
    cols[0, 1].start()
    load_imgt.start()
    rows = {0: row_load(0)}
    rows[0].start()
    load_txt.start()
    cols[0, 0] = col_load(0, 0)
    cols[0, 0].start()
    for i in range(m // 128):
        arow[i * 128:(i + 1) * 128, :] = jnp.broadcast_to(a_ref[i:i + 1, :], (128, 128)).T
    greet([g.img_peer(*o) for o in img_offs] + [g.txt_peer(*o) for o in txt_offs])
    net = Net(send_sems, recv_sems)
    core = g.txt_peer(1, 0, 0)
    ia = g.z * 2 + g.y % 2
    ib = (g.x * 2 + g.y // 2) * 2 + g.c
    scal_a = [net.send(part_ref, pa.at[ia], g.img_peer(*o)) for o in img_offs]
    pa[ia] = part_ref[...]
    img = Ring(net, iacc, ibuf, ICUT, g.img_peer(0, 1), g.img_peer(0, 3), g.img_peer(1, 0))
    txr = Ring(net, tacc, tbuf, TCUT, g.txt_peer(0, 0, 1), g.txt_peer(0, 0, 3), g.txt_peer(0, 1, 0))

    def minus_diag(grad, q):
        r = lax.broadcasted_iota(jnp.int32, (n, 128), 0)
        c = lax.broadcasted_iota(jnp.int32, (n, 128), 1) + q * 128
        return grad - jnp.where(r == c, 2.0 * inv, 0.0)

    def add(out_ref, part, may_start, it):
        old = out_ref[...]
        out_ref[...] = part + (jnp.where(it > 0, old, 0.0) if may_start else old)

    def col_slot(p, e_ref, out_ref):
        b = [b_ref[2 * p + q:2 * p + q + 1, :] for q in range(n // 128)]
        tiles = KC // n
        count = m // KC

        def grad(i, to, diag=False):
            for t in range(tiles):
                for q in range(n // 128):
                    lanes = slice(q * 128, (q + 1) * 128)
                    a = arow[pl.ds(pl.multiple_of(i * KC + t * n, n), n), :]
                    v = e_ref[i * tiles + t, :, lanes] * (a + b[q])
                    if diag and t == 0:
                        v = minus_diag(v, q)
                    to[t * n:(t + 1) * n, lanes] = v.astype(BF16)

        grad(0, gb0[0], diag=p == 0)
        def body(it, carry):
            for half, (now, later) in enumerate(((gb0[0], gb0[1]), (gb0[1], gb0[0]))):
                i = 2 * it + half
                at = pl.ds(pl.multiple_of(i * KC, KC), KC)
                add(out_ref, jnp.dot(imgt[:, at], now[...], preferred_element_type=F32), half == 0, it)
                grad((i + 1) % count, later)
            return carry

        lax.fori_loop(0, count // 2, body, 0)

    def row_slot(p, e_ref, out_ref):
        tiles = KC // n
        count = nt // KC

        def grad(i, to, diag=False):
            for t in range(tiles):
                tile = i * tiles + t
                for q in range(n // 128):
                    lanes = slice(q * 128, (q + 1) * 128)
                    v = (e_ref[tile // 8, tile % 8, :, lanes]
                         * (arow[p * n:(p + 1) * n, :] + b_ref[pl.ds(2 * tile + q, 1), :]))
                    if diag and t == 0:
                        v = minus_diag(v, q)
                    to[:, t * n + q * 128:t * n + (q + 1) * 128] = v.astype(BF16)

        grad(0, gb1[0], diag=p == 0)
        def body(it, carry):
            for half, (now, later) in enumerate(((gb1[0], gb1[1]), (gb1[1], gb1[0]))):
                i = 2 * it + half
                at = pl.ds(pl.multiple_of(i * KC, KC), KC)
                add(out_ref, jnp.dot(now[...], txt[at, :], preferred_element_type=F32), half == 0, it)
                grad((i + 1) % count, later)
            return carry

        lax.fori_loop(0, count // 2, body, 0)

    cross = {}
    for step, k in enumerate(ORDER):
        cols[step, 1].wait()
        if step == 0:
            load_imgt.wait()
        if step >= 2:
            cross[ORDER[step - 2]].wait_send()
        col_slot(8 + POS[mirror(k)], ecol.at[1], stage.at[step % 2])
        cross[k] = net.send(stage.at[step % 2], dbuf.at[k], core)
        if step + 1 < len(ORDER):
            cols[step + 1, 1] = col_load(step + 1, 1)
            cols[step + 1, 1].start()
            rows[step + 1] = row_load(step + 1)
            rows[step + 1].start()
        rows[step].wait()
        if step == 0:
            load_txt.wait()
        row_slot(POS[k], erow.at[step % 2], iacc.at[POS[k]])
        img.ready(step)
        cols[step, 0].wait()
        col_slot(POS[k], ecol.at[0], tacc.at[POS[k]])
        if step + 1 < len(ORDER):
            cols[step + 1, 0] = col_load(step + 1, 0)
            cols[step + 1, 0].start()
        cross[k].wait_recv()
        tacc[POS[k]] += dbuf[k]
        txr.ready(step)
        if step == 1:
            for copy in scal_a:
                copy.wait_recv()
            total = pa[0]
            for q in range(1, 8):
                total += pa[q]
            psum[...] = total
            scal_b = [net.send(psum, pb.at[ib], g.txt_peer(*o)) for o in txt_offs]
            pb[ib] = total
    for copy in scal_b:
        copy.wait_recv()
    total = pb[0]
    for k in range(1, 16):
        total += pb[k]
    part_out[...] = total
    for r in (img, txr):
        r.close()
    img_out[...] = iacc[0]
    txt_out[...] = tacc[0].T
    net.finish(skip=[cross[k] for k in ORDER[:-2]])


def grads(inv, imgt, txt_all, e, a, b, part):
    d, m = imgt.shape
    nt = txt_all.shape[0]
    n = m // 8
    vmem = pl.BlockSpec(memory_space=pltpu.VMEM)
    hbm = pl.BlockSpec(memory_space=pl.ANY)
    dma = pltpu.SemaphoreType.DMA
    return pl.pallas_call(
        functools.partial(grads_kernel, inv),
        out_shape=[jax.ShapeDtypeStruct((n, d), F32), jax.ShapeDtypeStruct((n, d), F32),
                   jax.ShapeDtypeStruct((8, 128), F32)],
        in_specs=[hbm, hbm, hbm, vmem, vmem, vmem],
        out_specs=[vmem] * 3,
        scratch_shapes=[pltpu.VMEM((d, m), BF16), pltpu.VMEM((nt, d), BF16), pltpu.VMEM((2, 2, 8, n, n), F32),
                        pltpu.VMEM((2, 8, n, n), F32), [pltpu.VMEM((KC, n), BF16)] * 2, [pltpu.VMEM((n, KC), BF16)] * 2,
                        pltpu.VMEM((m, 128), F32), pltpu.VMEM((2, d, n), F32), pltpu.VMEM((8, n, d), F32),
                        pltpu.VMEM((8, d, n), F32), pltpu.VMEM((8, n, d), F32), pltpu.VMEM((8, d, n), F32),
                        pltpu.VMEM((8, d, n), F32), pltpu.VMEM((8, 8, 128), F32), pltpu.VMEM((16, 8, 128), F32),
                        pltpu.VMEM((8, 128), F32), dma((2,)), dma((2,)), dma((2,)), dma((N_REDUCE,)),
                        dma((N_REDUCE,))],
        compiler_params=pltpu.CompilerParams(collective_id=2, has_side_effects=True, vmem_limit_bytes=VMEM_LIMIT),
        cost_estimate=pl.CostEstimate(flops=4 * m * nt * d, bytes_accessed=8 * m * nt, transcendentals=0),
        name="grads_reduce")(imgt, txt_all, e, a, b, part)


def solution(mesh):
    batch_spec = P(("row", "col"), None)
    shards = mesh.shape["row"] * mesh.shape["col"]

    def local_tile(img_loc, txt_loc, log_scale):
        n, d = img_loc.shape
        inv = 1.0 / (2 * n * shards)
        scale = jnp.exp(log_scale)
        e, imgt, txt_all, a, b, part = forward(inv, scale.reshape(1), img_loc, txt_loc)
        img_sum, txt_sum, tot = grads(inv, imgt, txt_all, e, a, b, part)
        d_img = (scale * img_sum).astype(BF16)
        d_txt = (scale * txt_sum).astype(BF16)
        tot = jnp.sum(tot[0:2], axis=1)
        return tot[0], d_img, d_txt, tot[1]

    return jax.shard_map(local_tile, mesh=mesh, in_specs=(batch_spec, batch_spec, P()),
                         out_specs=(P(), batch_spec, batch_spec, P()), check_vma=False)
```

```python
import functools

import jax
import jax.numpy as jnp
from jax import lax
from jax.experimental import pallas as pl
from jax.experimental.pallas import tpu as pltpu
from jax.sharding import PartitionSpec as P

MESH = pl.DeviceIdType.MESH
F32 = jnp.float32
BF16 = jnp.bfloat16
VMEM_LIMIT = 67_043_328


class Grid:
    def __init__(self):
        row = lax.axis_index("row")
        self.c = lax.axis_index("col")
        self.z = row // 16
        self.y = (row // 4) % 4
        self.x = row % 4
        self.turn = 1 - 2 * self.c

    def dev(self, z, y, x, c):
        return {"row": (z * 4 + y) * 4 + x, "col": c}

    def y_a(self):
        return self.y + 1 - 2 * (self.y % 2)

    def y_b(self):
        return 3 - self.y

    def img_peer(self, dy, dz):
        y = self.y_a() if dy else self.y
        return self.dev((self.z + 4 + self.turn * dz) % 4, y, self.x, self.c)

    def txt_peer(self, dc, dy, dx):
        y = self.y_b() if dy else self.y
        c = 1 - self.c if dc else self.c
        return self.dev(self.z, y, (self.x + 4 + self.turn * dx) % 4, c)


def view(ref):
    return ref[0].at[ref[1]] if isinstance(ref, tuple) else ref


class Copy:
    def __init__(self, net, i, src, dst, peer):
        self.net, self.i, self.src, self.dst, self.peer = net, i, src, dst, peer

    def make(self):
        return pltpu.make_async_remote_copy(
            src_ref=view(self.src), dst_ref=view(self.dst), send_sem=self.net.send_sems.at[self.i],
            recv_sem=self.net.recv_sems.at[self.i], device_id=self.peer, device_id_type=MESH)

    def wait_recv(self):
        self.make().wait_recv()

    def wait_send(self):
        self.make().wait_send()


class Net:
    def __init__(self, send_sems, recv_sems):
        self.send_sems, self.recv_sems, self.copies = send_sems, recv_sems, []

    def send(self, src, dst, peer):
        copy = Copy(self, len(self.copies), src, dst, peer)
        copy.make().start()
        self.copies.append(copy)
        return copy

    def finish(self, skip=()):
        for copy in self.copies:
            if not any(copy is other for other in skip):
                copy.wait_send()


def greet(peers):
    barrier = pltpu.get_barrier_semaphore()
    for peer in peers:
        pl.semaphore_signal(barrier, inc=1, device_id=peer, device_id_type=MESH)
    pl.semaphore_wait(barrier, len(peers))


def neighbours(g):
    return [g.img_peer(0, 1), g.img_peer(0, 3), g.img_peer(1, 0), g.txt_peer(0, 0, 1), g.txt_peer(0, 0, 3),
            g.txt_peer(0, 1, 0), g.txt_peer(1, 0, 0)]


POS = {0: 0, 3: 1, 4: 2, 1: 3, 2: 4, 7: 5, 5: 6, 6: 7}
DEEP = 4
N_FORWARD = 2 * 18 + 9 + 22


def mirror(k):
    return 4 * (k // 4) + (4 - k % 4) % 4


class Gather:
    def __init__(self, net, own, dst, plus, minus, pair):
        self.net, self.own, self.dst = net, own, dst
        self.n = own.shape[0]
        self.plus, self.minus, self.pair = plus, minus, pair
        self.got = {}

    def half(self, k, side):
        h = self.n // 2
        return self.dst.at[POS[k], pl.ds(side * h, h)]

    def send(self, key, src, k, side, peer):
        self.got[key, side] = self.net.send(src, self.half(k, side), peer)

    def first(self):
        h = self.n // 2
        own = [self.own.at[pl.ds(side * h, h)] for side in (0, 1)]
        for side in (0, 1):
            self.send("p0", own[side], 3, side, self.plus)
            self.send("m0", own[1 - side], 1, 1 - side, self.minus)
            self.send("y0", own[side], 4, side, self.pair)

    def wait(self, *keys):
        for key in keys:
            self.got[key].wait_recv()

    def far(self, dy):
        self.wait(("p%d" % dy, 0))
        self.send("f%d" % dy, self.half(4 * dy + 3, 0), 4 * dy + 2, 0, self.plus)
        self.wait(("m%d" % dy, 1))
        self.send("f%d" % dy, self.half(4 * dy + 1, 1), 4 * dy + 2, 1, self.minus)

    def second(self):
        self.wait(("y0", 0), ("y0", 1))
        for side in (0, 1):
            self.send("p1", self.half(4, side), 7, side, self.plus)
            self.send("m1", self.half(4, 1 - side), 5, 1 - side, self.minus)


def forward_kernel(inv, scale_ref, img_ref, txt_ref, e_out, imgt_out, txt_out, a_ref, b_ref, part_ref,
                   img_all, txt_all, imgt, d0, d1, s0, s1, rs, rl, cs, cl, rsum, csum, rbuf, cbuf,
                   e_sems, t_sems, i_sems, own_sems, send_sems, recv_sems):
    g = Grid()
    n, d = img_ref.shape
    scale = scale_ref[0]
    img_offs = [(dy, dz) for dy in (0, 1) for dz in range(4) if (dy, dz) != (0, 0)]
    txt_offs = [(dc, dy, dx) for dc in (0, 1) for dy in (0, 1) for dx in range(4) if (dc, dy, dx) != (0, 0, 0)]
    own = [pltpu.make_async_copy(img_ref, img_all.at[0], own_sems.at[0]),
           pltpu.make_async_copy(txt_ref, txt_all.at[0], own_sems.at[1])]
    for copy in own:
        copy.start()
    greet([g.img_peer(*o) for o in img_offs] + [g.txt_peer(*o) for o in txt_offs])
    net = Net(send_sems, recv_sems)
    core = g.txt_peer(1, 0, 0)
    img = Gather(net, img_ref, img_all, g.img_peer(0, 1), g.img_peer(0, 3), g.img_peer(1, 0))
    txt = Gather(net, txt_ref, txt_all, g.txt_peer(0, 0, 1), g.txt_peer(0, 0, 3), g.txt_peer(0, 1, 0))
    img.first()
    txt.first()
    cross = {0: net.send(txt_ref, txt_all.at[8], core)}
    saves = []

    def save_txt(p):
        copy = pltpu.make_async_copy(txt_all.at[p], txt_out.at[pl.ds(p * n, n)], t_sems.at[p])
        copy.start()
        saves.append(copy)

    def got_txt(*slots):
        for k in slots:
            p = POS[k]
            cross[k] = net.send(txt_all.at[p], txt_all.at[8 + POS[mirror(k)]], core)
            save_txt(p)

    def got_cross(*slots):
        for k in slots:
            cross[mirror(k)].wait_recv()
            save_txt(8 + POS[k])

    def got_img(*slots):
        for k in slots:
            p = POS[k]
            imgt[p] = img_all[p].T
            copy = pltpu.make_async_copy(imgt.at[p], imgt_out.at[:, pl.ds(p * n, n)], i_sems.at[p])
            copy.start()
            saves.append(copy)

    dots, stage = (d0, d1), (s0, s1)

    def dot(i, k, buf):
        lhs = img_all[i]
        for side in (0, 1):
            dots[buf][side] = lax.dot_general(lhs, txt_all[8 * side + k], (((1,), (1,)), ((), ())),
                                              preferred_element_type=F32)

    def store(i, k, buf, slot):
        return pltpu.make_async_copy(stage[buf].at[slot], e_out.at[i, :, k], e_sems.at[buf * DEEP + slot])

    def free(buf, use):
        if isinstance(use, int):
            if use >= DEEP:
                store(0, 0, buf, use % DEEP).wait()
        else:
            @pl.when(use >= DEEP)
            def _():
                store(0, 0, buf, use % DEEP).wait()

    def finish_unit(i, k, buf, use):
        slot = use % DEEP
        for blk in range(n // 32):
            lo = blk * 32
            rows = pl.ds(i * n + lo, 32) if isinstance(i, int) else pl.ds(pl.multiple_of(i * n + lo, 32), 32)
            racc, lacc = rs[rows, :], rl[rows, :]
            for side in (0, 1):
                logits = scale * dots[buf][side, lo:lo + 32, :]
                e = jnp.exp(logits)
                el = e * logits
                stage[buf][slot, side, lo:lo + 32, :] = e
                for q in range(n // 128):
                    racc += e[:, q * 128:(q + 1) * 128]
                    lacc += el[:, q * 128:(q + 1) * 128]
                cs[8 * side + k] += jnp.sum(e.reshape(4, 8, n), axis=0)
                cl[8 * side + k] += jnp.sum(el.reshape(4, 8, n), axis=0)
            rs[rows, :] = racc
            rl[rows, :] = lacc
        store(i, k, buf, slot).start()

    state = {"buf": 0, "unit": (0, 0), "uses": [0, 0]}

    def last_unit():
        buf = state["buf"]
        free(buf, state["uses"][buf])
        finish_unit(*state["unit"], buf, state["uses"][buf])
        state["uses"][buf] += 1

    def one(i, k):
        buf = state["buf"]
        free(buf, state["uses"][buf])
        dot(i, k, 1 - buf)
        finish_unit(*state["unit"], buf, state["uses"][buf])
        state["uses"][buf] += 1
        state["buf"], state["unit"] = 1 - buf, (i, k)

    def run(i0, k0, width, start, count):
        buf = state["buf"]
        uses = list(state["uses"])

        def unit(u):
            return i0 + u // width, k0 + u % width

        def body(it, carry):
            u = start + 2 * it
            free(buf, uses[buf] + it)
            free(1 - buf, uses[1 - buf] + it)
            dot(*unit(u), 1 - buf)
            finish_unit(carry[0], carry[1], buf, uses[buf] + it)
            dot(*unit(u + 1), buf)
            finish_unit(*unit(u), 1 - buf, uses[1 - buf] + it)
            return unit(u + 1)

        last = tuple(jnp.int32(v) for v in state["unit"])
        state["unit"] = lax.fori_loop(0, count // 2, body, last)
        state["uses"] = [v + count // 2 for v in uses]
        if count % 2:
            one(*unit(jnp.int32(start + count - 1)))

    rs[...] = jnp.zeros_like(rs)
    rl[...] = jnp.zeros_like(rl)
    cs[...] = jnp.zeros_like(cs)
    cl[...] = jnp.zeros_like(cl)
    for copy in own:
        copy.wait()
    save_txt(0)
    got_img(0)
    img.far(0)
    txt.far(0)
    img.second()
    txt.second()
    got_txt(4)
    txt.wait(("p0", 1), ("m0", 0))
    got_txt(3, 1)
    got_cross(0)
    dot(0, 0, 0)
    img.wait(("p0", 1), ("m0", 0))
    got_cross(4, 3, 1)
    run(0, 0, 4, 1, 15)
    got_img(4, 3, 1)
    for r in (txt, img):
        r.wait(("f0", 0), ("f0", 1))
    got_txt(2)
    run(4, 0, 4, 0, 4)
    got_cross(2)
    run(0, 4, 1, 0, 5)
    got_img(2)
    for r in (txt, img):
        r.far(1)
    txt.wait(("p1", 1), ("m1", 0))
    got_txt(7, 5)
    img.wait(("p1", 1), ("m1", 0))
    run(5, 0, 5, 0, 10)
    got_cross(7, 5)
    run(0, 5, 2, 0, 6)
    txt.wait(("f1", 0), ("f1", 1))
    got_txt(6)
    run(3, 5, 2, 0, 8)
    got_img(7, 5)
    img.wait(("f1", 0), ("f1", 1))
    got_cross(6)
    run(7, 0, 8, 0, 8)
    run(0, 7, 1, 0, 7)
    last_unit()

    for p in range(16):
        for q in range(n // 128):
            csum[2 * p + q:2 * p + q + 1, :] = jnp.sum(cs[p, :, q * 128:(q + 1) * 128], axis=0, keepdims=True)
    sums = []
    for dc, dy, dx in txt_offs:
        sums.append(net.send(csum, cbuf.at[dc * 8 + dy * 4 + (dx if dc else (4 - dx) % 4)], g.txt_peer(dc, dy, dx)))
    for i in range(8 * n // 128):
        rsum[i:i + 1, :] = jnp.sum(rs[i * 128:(i + 1) * 128, :].T, axis=0, keepdims=True)
    for dy, dz in img_offs:
        sums.append(net.send(rsum, rbuf.at[dy * 4 + (4 - dz) % 4], g.img_peer(dy, dz)))
    got_img(6)
    pos = jnp.sum(img_ref[...].astype(F32) * txt_ref[...].astype(F32), axis=1, keepdims=True) * scale
    rlsum = [jnp.sum(rl[i * 128:(i + 1) * 128, :].T, axis=0, keepdims=True) for i in range(8 * n // 128)]
    clsum = [jnp.sum(cl[p, :, q * 128:(q + 1) * 128], axis=0, keepdims=True) for p in range(16) for q in range(n // 128)]
    for copy in sums:
        copy.wait_recv()
    loss = jnp.zeros((2, 128), F32)
    dt = jnp.zeros((1, 128), F32)
    for dy, dz in [(0, 0)] + img_offs:
        k = 2 * POS[dy * 4 + dz]
        tot = rsum[k:k + 2, :]
        for oy, oz in img_offs:
            q = 2 * POS[(dy ^ oy) * 4 + (dz - oz) % 4]
            tot += rbuf[oy * 4 + oz, q:q + 2, :]
        a = 1.0 / tot
        a_ref[k:k + 2, :] = a * inv
        dt += a[0:1] * rlsum[k] + a[1:2] * rlsum[k + 1]
        if k == 0:
            loss += jnp.log(tot)
    for dc, dy, dx in [(0, 0, 0)] + txt_offs:
        k = 2 * (dc * 8 + POS[dy * 4 + dx])
        tot = csum[k:k + 2, :]
        for oc, oy, ox in txt_offs:
            q = 2 * ((dc ^ oc) * 8 + POS[(dy ^ oy) * 4 + ((ox - dx) if oc else (dx - ox)) % 4])
            tot += cbuf[oc * 8 + oy * 4 + ox, q:q + 2, :]
        b = 1.0 / tot
        b_ref[k:k + 2, :] = b * inv
        dt += b[0:1] * clsum[k] + b[1:2] * clsum[k + 1]
        if k == 0:
            loss += jnp.log(tot)
    diag = jnp.sum(pos, axis=0, keepdims=True)
    first_lane = lax.broadcasted_iota(jnp.int32, (1, 128), 1) == 0
    diag = jnp.where(first_lane, 2.0 * diag, 0.0)
    part_ref[...] = jnp.zeros_like(part_ref)
    part_ref[0:1, :] = (jnp.sum(loss, axis=0, keepdims=True) - diag) * inv
    part_ref[1:2, :] = (dt - diag) * inv
    for buf in (0, 1):
        for slot in range(DEEP):
            store(0, 0, buf, slot).wait()
    for copy in saves:
        copy.wait()
    net.finish()


def forward(inv, scale, img, txt):
    n, d = img.shape
    vmem = pl.BlockSpec(memory_space=pltpu.VMEM)
    hbm = pl.BlockSpec(memory_space=pl.ANY)
    dma = pltpu.SemaphoreType.DMA
    return pl.pallas_call(
        functools.partial(forward_kernel, inv),
        out_shape=[jax.ShapeDtypeStruct((8, 2, 8, n, n), F32), jax.ShapeDtypeStruct((d, 8 * n), BF16),
                   jax.ShapeDtypeStruct((16 * n, d), BF16), jax.ShapeDtypeStruct((16, 128), F32),
                   jax.ShapeDtypeStruct((32, 128), F32), jax.ShapeDtypeStruct((8, 128), F32)],
        in_specs=[pl.BlockSpec(memory_space=pltpu.SMEM), vmem, vmem],
        out_specs=[hbm, hbm, hbm, vmem, vmem, vmem],
        scratch_shapes=[pltpu.VMEM((8, n, d), BF16), pltpu.VMEM((16, n, d), BF16), pltpu.VMEM((8, d, n), BF16),
                        pltpu.VMEM((2, n, n), F32), pltpu.VMEM((2, n, n), F32), pltpu.VMEM((DEEP, 2, n, n), F32),
                        pltpu.VMEM((DEEP, 2, n, n), F32), pltpu.VMEM((8 * n, 128), F32), pltpu.VMEM((8 * n, 128), F32),
                        pltpu.VMEM((16, 8, n), F32), pltpu.VMEM((16, 8, n), F32), pltpu.VMEM((16, 128), F32),
                        pltpu.VMEM((32, 128), F32), pltpu.VMEM((8, 16, 128), F32), pltpu.VMEM((16, 32, 128), F32),
                        dma((2 * DEEP,)), dma((16,)), dma((8,)), dma((2,)), dma((N_FORWARD,)), dma((N_FORWARD,))],
        compiler_params=pltpu.CompilerParams(collective_id=0, has_side_effects=True, vmem_limit_bytes=VMEM_LIMIT),
        name="forward_sums")(scale, img, txt)


ICUT = 144
TCUT = 432
ORDER = (6, 5, 7, 4, 2, 1, 3, 0)
N_REDUCE = 8 + 2 * (4 + 18 + 1) + 22


class Ring:
    def __init__(self, net, acc, buf, cut, plus, minus, pair):
        self.net, self.acc, self.buf = net, acc, buf
        self.cut, self.rows = cut, acc.shape[1]
        self.plus, self.minus, self.pair = plus, minus, pair
        self.early, self.streams = {}, {}

    def pair_send(self, d):
        at = pl.ds(self.cut, self.rows - self.cut)
        self.early[d] = self.net.send((self.acc, (POS[4 + d], at)), (self.buf, (4 + d, at)), self.pair)

    def pair_add(self, d):
        self.early[d].wait_recv()
        self.acc[POS[d], self.cut:] += self.buf[4 + d, self.cut:]

    def where(self, name):
        if name == 2:
            return 0, self.cut, (self.rows - self.cut) // 2
        return 4 * name, 0, self.cut // 2

    def send(self, name, key, slot, half, to_slot, peer):
        _, lo, h = self.where(name)
        at = pl.ds(lo + half * h, h)
        self.streams[name, key] = self.net.send((self.acc, (POS[slot], at)), (self.buf, (to_slot, at)), peer)

    def far(self, name):
        b, _, _ = self.where(name)
        self.send(name, "a+", b + 2, 0, b + 2, self.plus)
        self.send(name, "a-", b + 2, 1, b + 2, self.minus)

    def plain_plus(self, name):
        b, _, _ = self.where(name)
        self.send(name, "b+1", b + 1, 1, b + 3, self.plus)

    def plain_minus(self, name):
        b, _, _ = self.where(name)
        self.send(name, "b-0", b + 3, 0, b + 1, self.minus)

    def mid(self, name):
        b, lo, h = self.where(name)
        self.streams[name, "a+"].wait_recv()
        self.acc[POS[b + 1], lo:lo + h] += self.buf[b + 2, lo:lo + h]
        self.send(name, "b+0", b + 1, 0, b + 3, self.plus)
        self.streams[name, "a-"].wait_recv()
        self.acc[POS[b + 3], lo + h:lo + 2 * h] += self.buf[b + 2, lo + h:lo + 2 * h]
        self.send(name, "b-1", b + 3, 1, b + 1, self.minus)

    def end(self, name):
        b, lo, h = self.where(name)
        for key in ("b+1", "b-0", "b+0", "b-1"):
            self.streams[name, key].wait_recv()
        self.acc[POS[b], lo:lo + 2 * h] += self.buf[b + 1, lo:lo + 2 * h] + self.buf[b + 3, lo:lo + 2 * h]

    def pair_last(self):
        at = pl.ds(0, self.cut)
        self.late = self.net.send((self.acc, (POS[4], at)), (self.buf, (0, at)), self.pair)

    def pair_end(self):
        self.late.wait_recv()
        self.acc[0, 0:self.cut] += self.buf[0, 0:self.cut]

    def ready(self, step):
        if step == 0:
            self.pair_send(2)
            self.far(1)
        elif step == 1:
            self.pair_send(1)
            self.plain_plus(1)
        elif step == 2:
            self.pair_send(3)
            self.plain_minus(1)
            self.mid(1)
        elif step == 3:
            self.pair_send(0)
        elif step == 4:
            self.far(0)
            self.pair_add(2)
            self.far(2)
            self.end(1)
            self.pair_last()
        elif step == 5:
            self.plain_plus(0)
            self.pair_add(1)
            self.plain_plus(2)
        elif step == 6:
            self.plain_minus(0)
            self.pair_add(3)
            self.plain_minus(2)
            self.mid(0)
            self.mid(2)

    def close(self):
        self.pair_add(0)
        self.end(0)
        self.pair_end()
        self.end(2)


KC = 512


def grads_kernel(inv, imgt_hbm, txt_hbm, e_hbm, a_ref, b_ref, part_ref, img_out, txt_out, part_out,
                 imgt, txt, erow, ecol, gb0, gb1, arow, stage, iacc, tacc, ibuf, tbuf, dbuf, pa, pb, psum,
                 local_sems, row_sems, col_sems, send_sems, recv_sems):
    g = Grid()
    n = iacc.shape[1]
    d = iacc.shape[2]
    m = imgt.shape[1]
    nt = txt.shape[0]
    img_offs = [(dy, dz) for dy in (0, 1) for dz in range(4) if (dy, dz) != (0, 0)]
    txt_offs = [(dc, dy, dx) for dc in (0, 1) for dy in (0, 1) for dx in range(4) if (dc, dy, dx) != (0, 0, 0)]

    def row_load(step):
        return pltpu.make_async_copy(e_hbm.at[POS[ORDER[step]]], erow.at[step % 2], row_sems.at[step % 2])

    def col_load(step, side):
        k = mirror(ORDER[step]) if side else ORDER[step]
        return pltpu.make_async_copy(e_hbm.at[:, side, POS[k]], ecol.at[side], col_sems.at[side])

    load_imgt = pltpu.make_async_copy(imgt_hbm, imgt, local_sems.at[0])
    load_txt = pltpu.make_async_copy(txt_hbm, txt, local_sems.at[1])
    cols = {}
    cols[0, 1] = col_load(0, 1)
    cols[0, 1].start()
    load_imgt.start()
    rows = {0: row_load(0)}
    rows[0].start()
    load_txt.start()
    cols[0, 0] = col_load(0, 0)
    cols[0, 0].start()
    for i in range(m // 128):
        arow[i * 128:(i + 1) * 128, :] = jnp.broadcast_to(a_ref[i:i + 1, :], (128, 128)).T
    greet([g.img_peer(*o) for o in img_offs] + [g.txt_peer(*o) for o in txt_offs])
    net = Net(send_sems, recv_sems)
    core = g.txt_peer(1, 0, 0)
    ia = g.z * 2 + g.y % 2
    ib = (g.x * 2 + g.y // 2) * 2 + g.c
    scal_a = [net.send(part_ref, pa.at[ia], g.img_peer(*o)) for o in img_offs]
    pa[ia] = part_ref[...]
    img = Ring(net, iacc, ibuf, ICUT, g.img_peer(0, 1), g.img_peer(0, 3), g.img_peer(1, 0))
    txr = Ring(net, tacc, tbuf, TCUT, g.txt_peer(0, 0, 1), g.txt_peer(0, 0, 3), g.txt_peer(0, 1, 0))

    def minus_diag(grad, q):
        r = lax.broadcasted_iota(jnp.int32, (n, 128), 0)
        c = lax.broadcasted_iota(jnp.int32, (n, 128), 1) + q * 128
        return grad - jnp.where(r == c, 2.0 * inv, 0.0)

    def add(out_ref, part, may_start, it):
        old = out_ref[...]
        out_ref[...] = part + (jnp.where(it > 0, old, 0.0) if may_start else old)

    def col_slot(p, e_ref, out_ref):
        b = [b_ref[2 * p + q:2 * p + q + 1, :] for q in range(n // 128)]
        tiles = KC // n
        count = m // KC

        def grad(i, to, diag=False):
            for t in range(tiles):
                for q in range(n // 128):
                    lanes = slice(q * 128, (q + 1) * 128)
                    a = arow[pl.ds(pl.multiple_of(i * KC + t * n, n), n), :]
                    v = e_ref[i * tiles + t, :, lanes] * (a + b[q])
                    if diag and t == 0:
                        v = minus_diag(v, q)
                    to[t * n:(t + 1) * n, lanes] = v.astype(BF16)

        grad(0, gb0[0], diag=p == 0)
        def body(it, carry):
            for half, (now, later) in enumerate(((gb0[0], gb0[1]), (gb0[1], gb0[0]))):
                i = 2 * it + half
                at = pl.ds(pl.multiple_of(i * KC, KC), KC)
                add(out_ref, jnp.dot(imgt[:, at], now[...], preferred_element_type=F32), half == 0, it)
                grad((i + 1) % count, later)
            return carry

        lax.fori_loop(0, count // 2, body, 0)

    def row_slot(p, e_ref, out_ref):
        tiles = KC // n
        count = nt // KC

        def grad(i, to, diag=False):
            for t in range(tiles):
                tile = i * tiles + t
                for q in range(n // 128):
                    lanes = slice(q * 128, (q + 1) * 128)
                    v = (e_ref[tile // 8, tile % 8, :, lanes]
                         * (arow[p * n:(p + 1) * n, :] + b_ref[pl.ds(2 * tile + q, 1), :]))
                    if diag and t == 0:
                        v = minus_diag(v, q)
                    to[:, t * n + q * 128:t * n + (q + 1) * 128] = v.astype(BF16)

        grad(0, gb1[0], diag=p == 0)
        def body(it, carry):
            for half, (now, later) in enumerate(((gb1[0], gb1[1]), (gb1[1], gb1[0]))):
                i = 2 * it + half
                at = pl.ds(pl.multiple_of(i * KC, KC), KC)
                add(out_ref, jnp.dot(now[...], txt[at, :], preferred_element_type=F32), half == 0, it)
                grad((i + 1) % count, later)
            return carry

        lax.fori_loop(0, count // 2, body, 0)

    cross = {}
    for step, k in enumerate(ORDER):
        cols[step, 1].wait()
        if step == 0:
            load_imgt.wait()
        if step >= 2:
            cross[ORDER[step - 2]].wait_send()
        col_slot(8 + POS[mirror(k)], ecol.at[1], stage.at[step % 2])
        cross[k] = net.send(stage.at[step % 2], dbuf.at[k], core)
        if step + 1 < len(ORDER):
            cols[step + 1, 1] = col_load(step + 1, 1)
            cols[step + 1, 1].start()
            rows[step + 1] = row_load(step + 1)
            rows[step + 1].start()
        rows[step].wait()
        if step == 0:
            load_txt.wait()
        row_slot(POS[k], erow.at[step % 2], iacc.at[POS[k]])
        img.ready(step)
        cols[step, 0].wait()
        col_slot(POS[k], ecol.at[0], tacc.at[POS[k]])
        if step + 1 < len(ORDER):
            cols[step + 1, 0] = col_load(step + 1, 0)
            cols[step + 1, 0].start()
        cross[k].wait_recv()
        tacc[POS[k]] += dbuf[k]
        txr.ready(step)
        if step == 1:
            for copy in scal_a:
                copy.wait_recv()
            total = pa[0]
            for q in range(1, 8):
                total += pa[q]
            psum[...] = total
            scal_b = [net.send(psum, pb.at[ib], g.txt_peer(*o)) for o in txt_offs]
            pb[ib] = total
    for copy in scal_b:
        copy.wait_recv()
    total = pb[0]
    for k in range(1, 16):
        total += pb[k]
    part_out[...] = total
    for r in (img, txr):
        r.close()
    img_out[...] = iacc[0]
    txt_out[...] = tacc[0].T
    net.finish(skip=[cross[k] for k in ORDER[:-2]])


def grads(inv, imgt, txt_all, e, a, b, part):
    d, m = imgt.shape
    nt = txt_all.shape[0]
    n = m // 8
    vmem = pl.BlockSpec(memory_space=pltpu.VMEM)
    hbm = pl.BlockSpec(memory_space=pl.ANY)
    dma = pltpu.SemaphoreType.DMA
    return pl.pallas_call(
        functools.partial(grads_kernel, inv),
        out_shape=[jax.ShapeDtypeStruct((n, d), F32), jax.ShapeDtypeStruct((n, d), F32),
                   jax.ShapeDtypeStruct((8, 128), F32)],
        in_specs=[hbm, hbm, hbm, vmem, vmem, vmem],
        out_specs=[vmem] * 3,
        scratch_shapes=[pltpu.VMEM((d, m), BF16), pltpu.VMEM((nt, d), BF16), pltpu.VMEM((2, 2, 8, n, n), F32),
                        pltpu.VMEM((2, 8, n, n), F32), [pltpu.VMEM((KC, n), BF16)] * 2, [pltpu.VMEM((n, KC), BF16)] * 2,
                        pltpu.VMEM((m, 128), F32), pltpu.VMEM((2, d, n), F32), pltpu.VMEM((8, n, d), F32),
                        pltpu.VMEM((8, d, n), F32), pltpu.VMEM((8, n, d), F32), pltpu.VMEM((8, d, n), F32),
                        pltpu.VMEM((8, d, n), F32), pltpu.VMEM((8, 8, 128), F32), pltpu.VMEM((16, 8, 128), F32),
                        pltpu.VMEM((8, 128), F32), dma((2,)), dma((2,)), dma((2,)), dma((N_REDUCE,)),
                        dma((N_REDUCE,))],
        compiler_params=pltpu.CompilerParams(collective_id=2, has_side_effects=True, vmem_limit_bytes=VMEM_LIMIT),
        cost_estimate=pl.CostEstimate(flops=4 * m * nt * d, bytes_accessed=8 * m * nt, transcendentals=0),
        name="grads_reduce")(imgt, txt_all, e, a, b, part)


def solution(mesh):
    batch_spec = P(("row", "col"), None)
    shards = mesh.shape["row"] * mesh.shape["col"]

    def local_tile(img_loc, txt_loc, log_scale):
        n, d = img_loc.shape
        inv = 1.0 / (2 * n * shards)
        scale = jnp.exp(log_scale)
        e, imgt, txt_all, a, b, part = forward(inv, scale.reshape(1), img_loc, txt_loc)
        img_sum, txt_sum, tot = grads(inv, imgt, txt_all, e, a, b, part)
        d_img = (scale * img_sum).astype(BF16)
        d_txt = (scale * txt_sum).astype(BF16)
        tot = jnp.sum(tot[0:2], axis=1)
        return tot[0], d_img, d_txt, tot[1]

    return jax.shard_map(local_tile, mesh=mesh, in_specs=(batch_spec, batch_spec, P()),
                         out_specs=(P(), batch_spec, batch_spec, P()), check_vma=False)
```
